32 devices in a mesh: seq: 4 (over z), shard: 8 (over y, x, core).
Axes of the slice: x: 2, y: 2, z: 4, core: 2. Of those that a mesh axis runs over, the one named last changes fastest.
Arguments:
- tokens: bfloat16 [8, 2048, 1024], P('shard', 'seq'), may hold values from -6 to 6
- ln1_gain: bfloat16 [1024], P(('seq', 'shard')), may hold values from 0.5 to 1.5
- ln1_bias: bfloat16 [1024], P(('seq', 'shard')), may hold values from -3 to 3
- w_qkv: bfloat16 [1024, 3072], P(('seq', 'shard')), may hold values from -0.1875 to 0.1875
- bias_query: bfloat16 [1024], P(('seq', 'shard')), may hold values from -3 to 3
- bias_value: bfloat16 [1024], P(('seq', 'shard')), may hold values from -3 to 3
- w_out: bfloat16 [1024, 1024], P(('seq', 'shard')), may hold values from -1 to 1
- bias_out: bfloat16 [1024], P(('seq', 'shard')), may hold values from -3 to 3
- ln2_gain: bfloat16 [1024], P(('seq', 'shard')), may hold values from 0.5 to 1.5
- ln2_bias: bfloat16 [1024], P(('seq', 'shard')), may hold values from -3 to 3
- w_in: bfloat16 [1024, 4096], P(('seq', 'shard')), may hold values from -0.1875 to 0.1875
- bias_in: bfloat16 [4096], P(('seq', 'shard')), may hold values from -3 to 3
- w_back: bfloat16 [4096, 1024], P(('seq', 'shard')), may hold values from -0.09375 to 0.09375
- bias_back: bfloat16 [1024], P(('seq', 'shard')), may hold values from -3 to 3
- cotangent: bfloat16 [8, 2048, 1024], P('shard', 'seq'), may hold values from -6 to 6
Outputs:
- result: bfloat16 [8, 2048, 1024], P('shard', 'seq')
- grad_tokens: float32 [8, 2048, 1024], P('shard', 'seq')
- grad_ln1_gain: float32 [1024], P(('seq', 'shard'))
- grad_ln1_bias: float32 [1024], P(('seq', 'shard'))
- grad_w_qkv: float32 [1024, 3072], P(('seq', 'shard'))
- grad_bias_query: float32 [1024], P(('seq', 'shard'))
- grad_bias_value: float32 [1024], P(('seq', 'shard'))
- grad_w_out: float32 [1024, 1024], P(('seq', 'shard'))
- grad_bias_out: float32 [1024], P(('seq', 'shard'))
- grad_ln2_gain: float32 [1024], P(('seq', 'shard'))
- grad_ln2_bias: float32 [1024], P(('seq', 'shard'))
- grad_w_in: float32 [1024, 4096], P(('seq', 'shard'))
- grad_bias_in: float32 [4096], P(('seq', 'shard'))
- grad_w_back: float32 [4096, 1024], P(('seq', 'shard'))
- grad_bias_back: float32 [1024], P(('seq', 'shard'))
The draws below stay inside these ranges and needn't reach their ends.
All inputs are finite; a program needn't handle non-finite values.
Results may differ from the reference program's by a relative error of at most 0.014.
The reference program's roundings to bfloat16 on the way count: a program that leaves them out, or rounds other values in their place, can miss the bound.
Values may be sent and summed in bfloat16 or wider, within the bound.
A program may use at most 192 MiB of HBM per device.

```python
import math
import jax
import jax.numpy as jnp
from jax import lax

D = 1024
HEADS = 16
HEAD_DIM = 64
FF = 4096
LENGTH = 2048
SEQS = 8


def strengthened(values, key, source, target, parts, factor):
    def block_of(position):
        return (jnp.arange(values.shape[position]) // (values.shape[position] // parts)).reshape((-1,) + (1,) * (values.ndim - 1 - position))

    first = jax.random.permutation(key, parts)[block_of(target)]
    other_side = (block_of(target) + parts // 2) % parts
    return jnp.where((block_of(source) == first) | (block_of(source) == other_side), factor * values, values)


def block_scale(rng, extent, split, least, largest):
    factor_of, own = 1.0, jax.random.fold_in(rng, 6)
    for axis_at, parts in split:
        steps = jnp.exp(jax.random.uniform(jax.random.fold_in(own, axis_at), (parts,), jnp.float32, least / len(split), largest / len(split)))
        factor_of = factor_of * jnp.repeat(steps, extent[axis_at] // parts).reshape([-1 if axis == axis_at else 1 for axis in range(len(extent))])
    return factor_of


def gaussian(own_key, extent, scale, bound, pieces=(), kind=jnp.bfloat16):
    loudness = block_scale(own_key, extent, pieces, -0.22, 0.18) if pieces else 1.0
    values = jax.random.normal(own_key, extent, jnp.float32) * scale * loudness
    return jnp.minimum(jnp.maximum(values, -bound), bound).astype(kind)


def noise_with(own_key, dims, deviation, limit, pieces, heavy, held_as=jnp.bfloat16):
    values = deviation * jax.random.normal(own_key, dims, jnp.float32)
    if pieces:
        values = values * block_scale(own_key, dims, pieces, -0.22, 0.18)
    return jnp.clip(strengthened(values, jax.random.fold_in(own_key, 3), *heavy), -limit, limit).astype(held_as)


def setup_inputs(seed: int = 0) -> dict:
    key_list = jax.random.split(jax.random.key(seed), 16)
    return {
        "tokens": gaussian(key_list[0], (SEQS, LENGTH, D), 1.0, 6.0, ((0, 8), (1, 4))),
        "ln1_gain": jnp.clip(1.0 + 0.1 * jax.random.normal(key_list[1], (D,), jnp.float32), 0.5, 1.5).astype(jnp.bfloat16),
        "ln1_bias": gaussian(key_list[2], (D,), 0.5, 3.0, ((0, 32),)),
        "w_qkv": gaussian(key_list[3], (D, 3 * D), D ** -0.5, 0.1875, ((0, 32),)),
        "bias_query": gaussian(key_list[4], (D,), 0.5, 3.0, ((0, 32),)),
        "bias_value": gaussian(key_list[5], (D,), 0.5, 3.0, ((0, 32),)),
        "w_out": gaussian(key_list[6], (D, D), (max(D // 32, 1)) ** -0.5, 1.0, ((0, 32),)),
        "bias_out": gaussian(key_list[7], (D,), 0.5, 3.0, ((0, 32),)),
        "ln2_gain": jnp.clip(1.0 + 0.1 * jax.random.normal(key_list[8], (D,), jnp.float32), 0.5, 1.5).astype(jnp.bfloat16),
        "ln2_bias": gaussian(key_list[9], (D,), 0.5, 3.0, ((0, 32),)),
        "w_in": gaussian(key_list[10], (D, FF), D ** -0.5, 0.1875, ((0, 32),)),
        "bias_in": gaussian(key_list[11], (FF,), 0.5, 3.0, ((0, 32),)),
        "w_back": gaussian(key_list[12], (FF, D), FF ** -0.5, 0.09375, ((0, 32),)),
        "bias_back": gaussian(key_list[13], (D,), 0.5, 3.0, ((0, 32),)),
        "cotangent": noise_with(key_list[14], (SEQS, LENGTH, D), 1.0, 6.0, ((0, 8), (1, 4)), (1, 2, 4, 2.0)),
    }


norm_eps = 1e-05
gelu_c = math.sqrt(2.0 / math.pi)

def normalize(values):
    mean_row = lax.optimization_barrier(jnp.mean(values, axis=-1, keepdims=True))
    centred = values - mean_row
    var_row = lax.optimization_barrier(jnp.mean(centred * centred, axis=-1, keepdims=True))
    scale_row = lax.rsqrt(var_row + norm_eps)
    return (centred * scale_row, scale_row)

def norm_back(dnormed, normed, scale_row):
    return scale_row * (dnormed - lax.optimization_barrier(jnp.mean(dnormed, axis=-1, keepdims=True)) - normed * lax.optimization_barrier(jnp.mean(dnormed * normed, axis=-1, keepdims=True)))

def gelu_pair(inputs):
    inner = gelu_c * (inputs + 0.044715 * inputs * inputs * inputs)
    tanh_val = jnp.tanh(inner)
    value = 0.5 * inputs * (1.0 + tanh_val)
    slope = 0.5 * (1.0 + tanh_val) + 0.5 * inputs * (1.0 - tanh_val * tanh_val) * gelu_c * (1.0 + 3.0 * 0.044715 * inputs * inputs)
    return (value, slope)

def masked_scores(query_block, keys_f, start, scale):
    block = query_block.shape[0]
    length = keys_f.shape[0]
    scores = jnp.einsum('qgd,kgd->gqk', query_block, keys_f) * scale
    q_pos = start + jnp.arange(block, dtype=jnp.int32)
    k_pos = jnp.arange(length, dtype=jnp.int32)
    allowed = k_pos[None, None, :] <= q_pos[None, :, None]
    return jnp.where(allowed, scores, -1e+30)

def attend_forward(query, keys, values):
    length, groups, width = query.shape
    block = min(512, length)
    scale = 1.0 / math.sqrt(width)
    keys_f = keys.astype(jnp.float32)
    values_f = values.astype(jnp.float32)

    def one_block(index):
        start = index * block
        q_blk = lax.dynamic_slice_in_dim(query, start, block, 0).astype(jnp.float32)
        scores = masked_scores(q_blk, keys_f, start, scale)
        log_total = jnp.log(lax.optimization_barrier(jnp.sum(jnp.exp(scores), axis=-1)))
        probs = lax.optimization_barrier(jnp.exp(scores - log_total[:, :, None]).astype(jnp.bfloat16))
        attended = jnp.einsum('gqk,kgd->qgd', probs.astype(jnp.float32), values_f)
        return (attended.astype(jnp.bfloat16), log_total)
    outs, logs = lax.map(one_block, jnp.arange(length // block, dtype=jnp.int32))
    return (outs.reshape(length, groups, width), logs)

def attend_backward(query, keys, values, attended, logs, d_att):
    length, groups, width = query.shape
    block = min(512, length)
    scale = 1.0 / math.sqrt(width)
    keys_f = keys.astype(jnp.float32)
    values_f = values.astype(jnp.float32)

    def one_block(carry, index):
        d_keys, d_values = carry
        start = index * block
        q_blk = lax.dynamic_slice_in_dim(query, start, block, 0).astype(jnp.float32)
        o_blk = lax.dynamic_slice_in_dim(attended, start, block, 0).astype(jnp.float32)
        do_blk = lax.dynamic_slice_in_dim(d_att, start, block, 0).astype(jnp.float32)
        scores = masked_scores(q_blk, keys_f, start, scale)
        log_total = lax.dynamic_index_in_dim(logs, index, 0, keepdims=False)
        probs = jnp.exp(scores - log_total[:, :, None])
        probs_b = lax.optimization_barrier(probs.astype(jnp.bfloat16)).astype(jnp.float32)
        d_values = d_values + jnp.einsum('gqk,qgd->kgd', probs_b, do_blk)
        d_probs = jnp.einsum('qgd,kgd->gqk', do_blk, values_f)
        delta = jnp.swapaxes(lax.optimization_barrier(jnp.sum(do_blk * o_blk, axis=-1)), 0, 1)
        d_scores = lax.optimization_barrier((probs * (d_probs - delta[:, :, None]) * scale).astype(jnp.bfloat16)).astype(jnp.float32)
        d_query = jnp.einsum('gqk,kgd->qgd', d_scores, keys_f).astype(jnp.bfloat16)
        d_keys = d_keys + jnp.einsum('gqk,qgd->kgd', d_scores, q_blk)
        return ((d_keys, d_values), d_query)
    zeros = jnp.zeros((length, groups, width), jnp.float32)
    (d_keys, d_values), d_queries = lax.scan(one_block, (zeros, zeros), jnp.arange(length // block, dtype=jnp.int32))
    return (d_queries.reshape(length, groups, width), d_keys.astype(jnp.bfloat16), d_values.astype(jnp.bfloat16))

def col_dot(left, right):
    return lax.dot_general(left, right, (((0,), (0,)), ((), ())), preferred_element_type=jnp.float32)

def row_dot(left, right):
    return lax.dot_general(left, right, (((1,), (1,)), ((), ())), preferred_element_type=jnp.float32)

def reference(tokens, ln1_gain, ln1_bias, w_qkv, bias_query, bias_value, w_out, bias_out, ln2_gain, ln2_bias, w_in, bias_in, w_back, bias_back, cotangent):
    f32 = jnp.float32
    gain_one = ln1_gain.astype(f32)
    shift_one = ln1_bias.astype(f32)
    gain_two = ln2_gain.astype(f32)
    shift_two = ln2_bias.astype(f32)
    bias_qkv = jnp.concatenate([bias_query.astype(f32), jnp.zeros((D,), f32), bias_value.astype(f32)])

    def one_sequence(grads, pair):
        seq_tokens, seq_cot = pair
        rows = seq_tokens.shape[0]
        x_f = seq_tokens.astype(f32)
        normed1, scale1 = normalize(x_f)
        h_one = (normed1 * gain_one + shift_one).astype(jnp.bfloat16)
        qkv = (jnp.dot(h_one, w_qkv, preferred_element_type=f32) + bias_qkv).astype(jnp.bfloat16)
        qkv = qkv.reshape(rows, 3, HEADS, HEAD_DIM)
        query, keys, values = (qkv[:, 0], qkv[:, 1], qkv[:, 2])
        attended, logs = attend_forward(query, keys, values)
        att_flat = attended.reshape(rows, D)
        resid = x_f + jnp.dot(att_flat, w_out, preferred_element_type=f32) + bias_out.astype(f32)
        normed2, scale2 = normalize(resid)
        h_two = (normed2 * gain_two + shift_two).astype(jnp.bfloat16)
        pre = jnp.dot(h_two, w_in, preferred_element_type=f32) + bias_in.astype(f32)
        act_val, slope = gelu_pair(pre)
        act = act_val.astype(jnp.bfloat16)
        result = (resid + jnp.dot(act, w_back, preferred_element_type=f32) + bias_back.astype(f32)).astype(jnp.bfloat16)
        cot_f = seq_cot.astype(f32)
        g_w_back = col_dot(act, seq_cot)
        g_b_back = lax.optimization_barrier(jnp.sum(cot_f, axis=0))
        d_pre = (row_dot(seq_cot, w_back) * slope).astype(jnp.bfloat16)
        g_w_in = col_dot(h_two, d_pre)
        g_b_in = lax.optimization_barrier(jnp.sum(d_pre.astype(f32), axis=0))
        d_h2 = row_dot(d_pre, w_in)
        g_g2 = lax.optimization_barrier(jnp.sum(d_h2 * normed2, axis=0))
        g_s2 = lax.optimization_barrier(jnp.sum(d_h2, axis=0))
        d_resid = cot_f + norm_back(d_h2 * gain_two, normed2, scale2)
        d_resid_b = d_resid.astype(jnp.bfloat16)
        g_w_out = col_dot(att_flat, d_resid_b)
        g_b_out = lax.optimization_barrier(jnp.sum(d_resid, axis=0))
        d_att = row_dot(d_resid_b, w_out).astype(jnp.bfloat16).reshape(rows, HEADS, HEAD_DIM)
        d_query, d_keys, d_values = attend_backward(query, keys, values, attended, logs, d_att)
        d_qkv = jnp.stack([d_query.reshape(rows, D), d_keys.reshape(rows, D), d_values.reshape(rows, D)], axis=1).reshape(rows, 3 * D)
        g_w_qkv = col_dot(h_one, d_qkv)
        g_bq = lax.optimization_barrier(jnp.sum(d_query.reshape(rows, D).astype(f32), axis=0))
        g_bv = lax.optimization_barrier(jnp.sum(d_values.reshape(rows, D).astype(f32), axis=0))
        d_h1 = row_dot(d_qkv, w_qkv)
        g_g1 = lax.optimization_barrier(jnp.sum(d_h1 * normed1, axis=0))
        g_s1 = lax.optimization_barrier(jnp.sum(d_h1, axis=0))
        d_tokens = d_resid + norm_back(d_h1 * gain_one, normed1, scale1)
        terms = (g_g1, g_s1, g_w_qkv, g_bq, g_bv, g_w_out, g_b_out, g_g2, g_s2, g_w_in, g_b_in, g_w_back, g_b_back)
        grads = tuple((total + term for total, term in zip(grads, terms)))
        return (grads, (result, d_tokens))
    zero_grads = (jnp.zeros((D,), f32), jnp.zeros((D,), f32), jnp.zeros((D, 3 * D), f32), jnp.zeros((D,), f32), jnp.zeros((D,), f32), jnp.zeros((D, D), f32), jnp.zeros((D,), f32), jnp.zeros((D,), f32), jnp.zeros((D,), f32), jnp.zeros((D, FF), f32), jnp.zeros((FF,), f32), jnp.zeros((FF, D), f32), jnp.zeros((D,), f32))
    grads, (results, d_tokens) = lax.scan(one_sequence, zero_grads, (tokens, cotangent))
    return (results, d_tokens, grads[0], grads[1], grads[2], grads[3], grads[4], grads[5], grads[6], grads[7], grads[8], grads[9], grads[10], grads[11], grads[12])
```

```python
import math

import jax
import jax.numpy as jnp
from jax import lax
from jax.experimental import pallas as pl
from jax.experimental.pallas import tpu as pltpu
from jax.sharding import PartitionSpec as P

HEAD_DIM = 64
LANES = 128
MESH = pl.DeviceIdType.MESH
NT = (((1,), (1,)), ((), ()))
TN = (((0,), (0,)), ((), ()))
f32 = jnp.float32
bf16 = jnp.bfloat16

norm_eps = 1e-05
gelu_c = math.sqrt(2.0 / math.pi)
scale = 1.0 / math.sqrt(HEAD_DIM)

VM = pl.BlockSpec(memory_space=pltpu.VMEM)
HB = pl.BlockSpec(memory_space=pl.ANY)


def dot(a, b):
    return jnp.dot(a, b, preferred_element_type=f32)


def row_dot(a, b):
    return lax.dot_general(a, b, NT, preferred_element_type=f32)


def col_dot(a, b):
    return lax.dot_general(a, b, TN, preferred_element_type=f32)


def normalize(values):
    mean_row = jnp.mean(values, axis=-1, keepdims=True)
    centred = values - mean_row
    var_row = jnp.mean(centred * centred, axis=-1, keepdims=True)
    scale_row = lax.rsqrt(var_row + norm_eps)
    return (centred * scale_row, scale_row)


def norm_back(dnormed, normed, scale_row):
    return scale_row * (
        dnormed
        - jnp.mean(dnormed, axis=-1, keepdims=True)
        - normed * jnp.mean(dnormed * normed, axis=-1, keepdims=True)
    )


def gelu_pair(inputs):
    inner = gelu_c * (inputs + 0.044715 * inputs * inputs * inputs)
    tanh_val = jnp.tanh(inner)
    value = 0.5 * inputs * (1.0 + tanh_val)
    slope = 0.5 * (1.0 + tanh_val) + 0.5 * inputs * (1.0 - tanh_val * tanh_val) * gelu_c * (
        1.0 + 3.0 * 0.044715 * inputs * inputs
    )
    return (value, slope)


def block_rows(index, size, count=1):
    return pl.ds(pl.multiple_of(index * size, size), size * count)


def head_lanes(shape, head):
    return lax.broadcasted_iota(jnp.int32, shape, len(shape) - 1) // HEAD_DIM == head


def only_head(values, head):
    return jnp.where(head_lanes(values.shape, head), values, jnp.zeros_like(values))


def spread_heads(columns, rows, width):
    out = None
    for head in range(width // HEAD_DIM):
        one = jnp.broadcast_to(columns[:, head : head + 1], (rows, width))
        out = one if out is None else jnp.where(head_lanes((rows, width), head), one, out)
    return out


class Place:
    def __init__(self, n, m):
        self.n, self.m, self.half, self.planes = n, m, n // 2, m // 2
        self.s, self.k = lax.axis_index("seq"), lax.axis_index("shard")
        self.core, self.plane = lax.rem(self.k, 2), self.k // 2
        self.team, self.low = self.s // self.half, lax.rem(self.s, self.half)
        self.rank = self.low + self.half * self.core
        self.index = self.s * m + self.k

    def member(self, rank):
        return (self.team * self.half + lax.rem(rank, self.half), 2 * self.plane + rank // self.half)

    def across(self):
        return (lax.rem(self.s + self.half, self.n), self.k)

    def swap(self):
        return (lax.rem(self.s + self.half, self.n), 2 * self.plane + 1 - self.core)

    def partner(self):
        return (self.s, 2 * self.plane + 1 - self.core)

    def along(self, step):
        return lax.rem(self.s + step, self.n)

    def beside(self, step):
        return lax.rem(self.plane + step, self.planes)

    def greet(self):
        barrier = pltpu.get_barrier_semaphore()
        count = 0

        def signal(device):
            pl.semaphore_signal(barrier, inc=1, device_id=device, device_id_type=MESH)

        for step in range(1, self.n):
            signal((self.along(step), self.k))
            count += 1
        for step in range(self.n):
            signal((self.along(step), 2 * self.plane + 1 - self.core))
            count += 1
        for step in range(1, self.planes):
            signal((self.s, 2 * self.beside(step) + self.core))
            count += 1
        pl.semaphore_wait(barrier, count)


def send(src, dst, sems, at, device):
    pltpu.make_async_remote_copy(
        src_ref=src,
        dst_ref=dst,
        send_sem=sems[0].at[at],
        recv_sem=sems[1].at[at],
        device_id=device,
        device_id_type=MESH,
    ).start()


def settle(view, sem):
    pltpu.make_async_copy(view, view, sem).wait()


def attend_row(i, q_ref, k_ref, v_ref, o_ref, lse_ref, qm, m_s, l_s, acc, size):
    width = q_ref.shape[1]
    heads = width // HEAD_DIM
    rows = block_rows(i, size)
    q = q_ref[rows, :] * jnp.asarray(scale, bf16)
    for h in range(heads):
        qm[h] = only_head(q, h)

    def step(j, diagonal):
        at = block_rows(j, size)
        k = k_ref[at, :]
        v = v_ref[at, :]
        old = m_s[...]
        tops, sums, total = [], [], None
        for h in range(heads):
            s = row_dot(k, qm[h])
            if diagonal:
                k_pos = lax.broadcasted_iota(jnp.int32, (size, size), 0)
                q_pos = lax.broadcasted_iota(jnp.int32, (size, size), 1)
                s = jnp.where(k_pos <= q_pos, s, -1e30)
            top = jnp.max(s, axis=0, keepdims=True)
            if not diagonal:
                top = jnp.maximum(old[h : h + 1], top)
            p = jnp.exp(s - top)
            tops.append(top)
            sums.append(jnp.sum(p, axis=0, keepdims=True))
            part = col_dot(p.astype(bf16), only_head(v, h))
            total = part if total is None else total + part
        rest = [jnp.zeros((8 - heads, size), f32)] if heads < 8 else []
        top = jnp.concatenate(tops + rest, 0)
        add = jnp.concatenate(sums + rest, 0)
        if diagonal:
            l_s[...] = add
            acc[...] = total
        else:
            fade = jnp.exp(old - top)
            l_s[...] = l_s[...] * fade + add
            acc[...] = acc[...] * spread_heads(jnp.transpose(fade), size, width) + total
        m_s[...] = top

    step(i, True)

    def body(j, carry):
        step(j, False)
        return carry

    lax.fori_loop(0, i, body, 0)
    l = l_s[...]
    lse_ref[:, rows] = m_s[...] + jnp.log(l)
    o_ref[rows, :] = (acc[...] * spread_heads(jnp.transpose(1.0 / l), size, width)).astype(bf16)


def forward_call(n, m, tok, cot, wq_s, sm_s, wo_s, wi_s, wb_s):
    size, d = tok.shape
    nd = n * m
    length = n * size
    width = d // n
    rq = wq_s.shape[1]
    chunks = []
    chunks.append((0, wo_s.shape[0], 0, wo_s.shape[0], 0, wo_s.shape[1]))
    for part in range(2):
        columns = wi_s.shape[1] // 2
        chunks.append((1, wi_s.shape[0], 0, wi_s.shape[0], part * columns, columns))
    for part in range(2):
        rows = wb_s.shape[0] // 2
        chunks.append((2, wb_s.shape[0], part * rows, rows, 0, wb_s.shape[1]))
    nc = len(chunks)

    def kernel(
        tok_r, cot_r, wqs_r, sms_r, wos_r, wis_r, wbs_r,
        wo_r, wi_r, wb_r, q_r, k_r, v_r, o_r, lse_r, att_r, h1_r, wq_r, tb_r, cb_r, sv_r,
        tokf, sma, qm, m_s, l_s, acc, vec,
        t_send, t_recv, w_send, w_recv, a_send, a_recv, z_send, z_recv, p_send, p_recv, c_send, c_recv, loc,
    ):
        at = Place(n, m)
        half, planes, rank, core = at.half, at.planes, at.rank, at.core
        fulls, shards = (wo_r, wi_r, wb_r), (wos_r, wis_r, wbs_r)
        ts, ws, zs, ps, cs = (t_send, t_recv), (w_send, w_recv), (z_send, z_recv), (p_send, p_recv), (c_send, c_recv)
        at.greet()
        away = core != at.team

        own_w = pltpu.make_async_copy(wqs_r.at[rank], wq_r.at[block_rows(at.index, rq)], loc.at[0])
        own_s = pltpu.make_async_copy(sms_r, sma.at[at.index], loc.at[1])
        own_w.start()
        own_s.start()
        for step in range(1, n):
            other = lax.rem(rank + step, n)
            send(wqs_r.at[other], wq_r.at[block_rows(at.index, rq)], ws, 0, at.member(other))
            send(sms_r, sma.at[at.index], ws, 1, at.member(other))

        @pl.when(away)
        def _():
            send(tok_r, tokf.at[at.low + half * (1 - core)], ts, 0, at.swap())

        @pl.when(jnp.logical_not(away))
        def _():
            pltpu.make_async_copy(tok_r, tokf.at[rank], loc.at[2]).start()

        own_w.wait()
        own_s.wait()
        settle(wq_r.at[pl.ds(0, (n - 1) * rq)], w_recv.at[0])
        settle(sma.at[pl.ds(0, n - 1)], w_recv.at[1])
        for low in range(half):
            row = (at.team * half + low) * m + 2 * at.plane
            send(wq_r.at[block_rows(row, rq, 2)], wq_r.at[block_rows(row, rq, 2)], ws, 2, at.across())
            send(sma.at[pl.ds(row, 2)], sma.at[pl.ds(row, 2)], ws, 3, at.across())

        @pl.when(away)
        def _():
            settle(tokf.at[0], t_recv.at[0])

        @pl.when(jnp.logical_not(away))
        def _():
            settle(tokf.at[0], loc.at[2])

        for step in range(1, half):
            low = lax.rem(at.low + step, half)
            send(tokf.at[rank], tokf.at[rank], ts, 1, (at.team * half + low, at.k))
        send(tokf.at[rank], tokf.at[rank], ts, 2, at.partner())

        @pl.when(away)
        def _():
            send(cot_r, cb_r, ts, 4, at.swap())

        @pl.when(jnp.logical_not(away))
        def _():
            pltpu.make_async_copy(cot_r, cb_r, loc.at[3]).start()

        def piece(c, device):
            which, rs, r0, nr, c0, ncol = chunks[c]
            return fulls[which].at[pl.ds(pl.multiple_of(device * rs + r0, 8), nr), pl.ds(c0, ncol)]

        def some(c, count):
            which, rs, r0, nr, c0, ncol = chunks[c]
            return fulls[which].at[pl.ds(0, count * nr), pl.ds(c0, ncol)]

        def mine(c):
            which, rs, r0, nr, c0, ncol = chunks[c]
            return shards[which].at[pl.ds(r0, nr), pl.ds(c0, ncol)]

        for c in range(nc):
            pltpu.make_async_copy(mine(c), piece(c, at.index), loc.at[4 + c]).start()
            for step in range(1, n):
                send(mine(c), piece(c, at.index), zs, c, (at.along(step), at.k))

        settle(wq_r.at[pl.ds(0, half * 2 * rq)], w_recv.at[2])
        settle(sma.at[pl.ds(0, half * 2)], w_recv.at[3])
        for step in range(1, planes):
            there = (at.s, 2 * at.beside(step) + core)
            for other in range(n):
                row = other * m + 2 * at.plane
                send(wq_r.at[block_rows(row, rq, 2)], wq_r.at[block_rows(row, rq, 2)], ws, 4, there)
                send(sma.at[pl.ds(row, 2)], sma.at[pl.ds(row, 2)], ws, 5, there)

        def z_to_p(c):
            settle(some(c, 1), loc.at[4 + c])
            settle(some(c, n - 1), z_recv.at[c])
            for step in range(1, planes):
                there = (at.s, 2 * at.beside(step) + core)
                for other in range(n):
                    view = piece(c, other * m + at.k)
                    send(view, view, ps, c, there)

        def p_to_c(c):
            settle(some(c, (planes - 1) * n), p_recv.at[c])
            for other in range(n * planes):
                view = piece(c, other * 2 + core)
                send(view, view, cs, c, at.partner())

        settle(wq_r.at[pl.ds(0, (planes - 1) * n * 2 * rq)], w_recv.at[4])
        settle(sma.at[pl.ds(0, (planes - 1) * n * 2)], w_recv.at[5])
        per = LANES // (d // nd)
        for group in range(d // LANES):
            total = sma[group * per].astype(f32)
            for other in range(1, per):
                total = total + sma[group * per + other].astype(f32)
            sv_r[:, group * LANES : (group + 1) * LANES] = total
            vec[0, group : group + 1, :] = total[2:3]
            vec[1, group : group + 1, :] = total[3:4]

        def norm_block(b):
            def body(t, carry):
                part = pl.ds(pl.multiple_of(t * 128, 128), 128)
                x = tokf[b, part, :].astype(f32)
                normed, _ = normalize(x)
                h1_r[pl.ds(pl.multiple_of(b * size + t * 128, 128), 128), :] = (
                    normed * sv_r[0:1, :] + sv_r[1:2, :]
                ).astype(bf16)
                return carry

            lax.fori_loop(0, size // 128, body, 0)

        groups = width // LANES
        bias_q = jnp.concatenate([vec[0, pl.ds(rank * groups + g, 1), :] for g in range(groups)], 1)
        bias_v = jnp.concatenate([vec[1, pl.ds(rank * groups + g, 1), :] for g in range(groups)], 1)

        def project_block(b):
            def body(t, carry):
                part = pl.ds(pl.multiple_of(b * size + t * 256, 256), 256)
                h = h1_r[part, :]
                q_r[part, :] = (dot(h, wq_r[:, 0:width]) + bias_q).astype(bf16)
                k_r[part, :] = dot(h, wq_r[:, width : 2 * width]).astype(bf16)
                v_r[part, :] = (dot(h, wq_r[:, 2 * width : 3 * width]) + bias_v).astype(bf16)
                return carry

            lax.fori_loop(0, size // 256, body, 0)

        def take_block(b):
            norm_block(b)
            project_block(b)

        take_block(rank)
        settle(tokf.at[0], t_recv.at[2])
        take_block(lax.rem(rank + half, n))
        if half > 1:
            settle(tokf.at[pl.ds(0, half - 1)], t_recv.at[1])
            for step in range(1, half):
                b = lax.rem(at.low + step, half) + half * core
                send(tokf.at[b], tokf.at[b], ts, 3, at.partner())
        z_to_p(0)
        for step in range(1, half):
            take_block(lax.rem(at.low + step, half) + half * core)
        if half > 1:
            settle(tokf.at[pl.ds(0, half - 1)], t_recv.at[3])
            for step in range(1, half):
                take_block(lax.rem(at.low + step, half) + half * (1 - core))
        tb_r[...] = tokf[rank]
        z_to_p(1)

        def row(i, carry):
            attend_row(i, q_r, k_r, v_r, o_r, lse_r, qm, m_s, l_s, acc, size)
            src = o_r.at[block_rows(i, size)]
            dst = att_r.at[:, block_rows(rank, width)]

            @pl.when(i != rank)
            def _():
                send(src, dst, (a_send, a_recv), 0, at.member(i))

            @pl.when(i == rank)
            def _():
                pltpu.make_async_copy(src, dst, loc.at[2]).start()

            for c, when in ((2, 1), (3, 2), (4, n - 1)):

                @pl.when(i == when)
                def _(c=c):
                    z_to_p(c)
                    if c == 4:
                        p_to_c(0)

            return carry

        lax.fori_loop(0, n, row, 0)
        settle(tokf.at[0, :, pl.ds(0, width)], loc.at[2])
        others = tokf.at[0, :, pl.ds(0, (n - 1) * width)]
        settle(others, a_recv.at[0])
        for c in range(1, nc):
            p_to_c(c)
        for c in range(nc):
            settle(some(c, n * planes), c_recv.at[c])

        settle(others, a_send.at[0])
        for c in range(nc):
            settle(some(c, n - 1), z_send.at[c])
            settle(some(c, (planes - 1) * n), p_send.at[c])
            settle(some(c, n * planes), c_send.at[c])
        for at_sem, count in ((0, n - 1), (2, half * 2), (4, (planes - 1) * n * 2)):
            settle(wq_r.at[pl.ds(0, count * rq)], w_send.at[at_sem])
            settle(sma.at[pl.ds(0, count)], w_send.at[at_sem + 1])

        @pl.when(away)
        def _():
            settle(tokf.at[0], t_send.at[0])
            settle(cb_r, t_recv.at[4])
            settle(cb_r, t_send.at[4])

        @pl.when(jnp.logical_not(away))
        def _():
            settle(cb_r, loc.at[3])

        settle(tokf.at[0], t_send.at[2])
        if half > 1:
            settle(tokf.at[pl.ds(0, half - 1)], t_send.at[1])
            settle(tokf.at[pl.ds(0, half - 1)], t_send.at[3])

    def sds(shape, dtype=bf16):
        return jax.ShapeDtypeStruct(shape, dtype)

    sems = pltpu.SemaphoreType.DMA
    return pl.pallas_call(
        kernel,
        name="gather_attend",
        out_shape=(
            sds((nd * wo_s.shape[0], wo_s.shape[1])),
            sds((nd * wi_s.shape[0], wi_s.shape[1])),
            sds((nd * wb_s.shape[0], wb_s.shape[1])),
            sds((length, width)), sds((length, width)), sds((length, width)), sds((length, width)),
            sds((8, length), f32),
            sds((size, d)),
            sds((length, d)),
            sds((d, 3 * width)),
            sds((size, d)), sds((size, d)),
            sds((16, d), f32),
        ),
        in_specs=[HB] * 7,
        out_specs=(HB,) * 3 + (VM,) * 11,
        scratch_shapes=[
            pltpu.VMEM((n, size, d), bf16),
            pltpu.VMEM((nd, 16, LANES), bf16),
            pltpu.VMEM((width // HEAD_DIM, size, width), bf16),
            pltpu.VMEM((8, size), f32),
            pltpu.VMEM((8, size), f32),
            pltpu.VMEM((size, width), f32),
            pltpu.VMEM((2, max(8, d // LANES), LANES), f32),
            sems((5,)), sems((5,)),
            sems((6,)), sems((6,)),
            sems((1,)), sems((1,)),
            sems((nc,)), sems((nc,)),
            sems((nc,)), sems((nc,)),
            sems((nc,)), sems((nc,)),
            sems((4 + nc,)),
        ],
        compiler_params=pltpu.CompilerParams(
            collective_id=0, has_side_effects=True, vmem_limit_bytes=62 << 20
        ),
    )(tok, cot, wq_s, sm_s, wo_s, wi_s, wb_s)


def small_pack(index, vectors):
    per = vectors[0].shape[0]
    rows = [part for v in vectors for part in v.reshape(-1, per)]
    rows = jnp.stack(rows + [jnp.zeros_like(rows[0])] * (16 - len(rows)))
    lane = lax.broadcasted_iota(jnp.int32, (16, LANES), 1)
    spread = jnp.tile(rows, (1, LANES // per))
    return jnp.where(lane // per == lax.rem(index, LANES // per), spread, jnp.zeros_like(spread))


def backward_call(n, m, res, dat, dres, q, k, v, o, lse, h1, wq, tb, sv, gsm, gwo, gwi, gwb):
    size, d = res.shape
    nd = n * m
    length = n * size
    width = d // n
    heads = width // HEAD_DIM
    half, planes = n // 2, m // 2
    rq = d // nd
    ro, ri, rb = gwo.shape[0] // nd, gwi.shape[0] // nd, gwb.shape[0] // nd
    chunks = [(0, ro, 0, ro, 0, gwo.shape[1])]
    for part in range(2):
        columns = gwi.shape[1] // 2
        chunks.append((1, ri, 0, ri, part * columns, columns))
    for part in range(2):
        rows = rb // 2
        chunks.append((2, rb, part * rows, rows, 0, gwb.shape[1]))
    chunks = chunks[3:] + chunks[1:3] + chunks[:1]
    nc = len(chunks)
    lanes_s = d // n

    def kernel(*refs):
        (res_r, dat_r, dres_r, q_r, k_r, v_r, o_r, lse_r, h1_r, wq_r, tb_r, sv_r, gsm_r, gwo_r, gwi_r, gwb_r) = refs[:16]
        (reso_r, gt_r, gq_r, go_r, gi_r, gb_r, small_r) = refs[16:23]
        (do, delta, dqa, dka, dva, dqkv, gacc, rqp, rqh, pf, sd, rd, rzd, rg, sm, smz, smp, smc) = refs[23:41]
        rest = refs[41:]
        ga, rc, rp, rz = (rest[i * nc : (i + 1) * nc] for i in range(4))
        (d_s, d_r, x_s, x_r, y_s, y_r, e_s, e_r, c_s, c_r, p_s, p_r, z_s, z_r, m_s, m_r, loc) = rest[4 * nc :]
        gqb, hb, sg = rc[0].at[:, pl.ds(0, 3 * width)], rc[1], rc[4]
        tb_v, o_v = rc[2].at[:, pl.ds(0, d)], rc[3]
        at = Place(n, m)
        rank, core, low = at.rank, at.core, at.low
        grads = (gwo_r, gwi_r, gwb_r)
        outs = (go_r, gi_r, gb_r)
        at.greet()
        away = core != at.team

        for step in range(1, n):
            other = lax.rem(rank + step, n)
            send(dat_r.at[:, block_rows(other, width)], do.at[block_rows(rank, size)], (d_s, d_r), 0, at.member(other))
        own_do = pltpu.make_async_copy(dat_r.at[:, block_rows(rank, width)], do.at[block_rows(rank, size)], loc.at[0])
        own_do.start()

        def piece(c, device):
            which, rs, r0, nr, c0, ncol = chunks[c]
            return grads[which].at[pl.ds(pl.multiple_of(device * rs + r0, 8), nr), pl.ds(c0, ncol)]

        def cells(ref, c, index, count=1):
            nr = chunks[c][3]
            return ref.at[pl.ds(pl.multiple_of(index * nr, nr), count * nr)]

        for c in range(nc):
            for other in range(n * planes):
                send(piece(c, 2 * other + 1 - core), cells(rc[c], c, other), (c_s, c_r), c, at.partner())
                pltpu.make_async_copy(piece(c, 2 * other + core), cells(ga[c], c, other), loc.at[4 + c]).start()

        @pl.when(away)
        def _():
            send(res_r, reso_r, (x_s, x_r), 0, at.swap())

        @pl.when(jnp.logical_not(away))
        def _():
            pltpu.make_async_copy(res_r, reso_r, loc.at[1]).start()

        own_dres = pltpu.make_async_copy(dres_r, gt_r, loc.at[2])
        own_dres.start()

        def fetch_h1(b):
            return pltpu.make_async_copy(h1_r.at[block_rows(b, size)], hb.at[block_rows(lax.rem(b, 2), size)], loc.at[3])

        def c_to_p(c):
            nr = chunks[c][3]
            settle(ga[c], loc.at[4 + c])
            settle(rc[c], c_r.at[c])

            def add(t, carry):
                rows = block_rows(t, nr)
                ga[c][rows, :] = (ga[c][rows, :].astype(f32) + rc[c][rows, :].astype(f32)).astype(bf16)
                return carry

            lax.fori_loop(0, n * planes, add, 0)
            for step in range(1, planes):
                other = at.beside(step)
                for s in range(n):
                    send(
                        cells(ga[c], c, s * planes + other),
                        cells(rp[c], c, (step - 1) * n + s),
                        (p_s, p_r), c, (at.s, 2 * other + core),
                    )

        def p_to_z(c):
            nr = chunks[c][3]
            settle(rp[c], p_r.at[c])

            def add(s, carry):
                rows = block_rows(s * planes + at.plane, nr)
                total = ga[c][rows, :].astype(f32)
                for step in range(1, planes):
                    total = total + rp[c][block_rows((step - 1) * n + s, nr), :].astype(f32)
                ga[c][rows, :] = total.astype(bf16)
                return carry

            lax.fori_loop(0, n, add, 0)
            for step in range(1, n):
                s = at.along(step)
                send(cells(ga[c], c, s * planes + at.plane), cells(rz[c], c, step - 1), (z_s, z_r), c, (s, at.k))

        def z_to_out(c):
            which, rs, r0, nr, c0, ncol = chunks[c]
            settle(rz[c], z_r.at[c])
            total = ga[c][block_rows(at.s * planes + at.plane, nr), :].astype(f32)
            for step in range(1, n):
                total = total + rz[c][(step - 1) * nr : step * nr, :].astype(f32)
            outs[which][r0 : r0 + nr, c0 : c0 + ncol] = total

        for c in range(nc):
            c_to_p(c)
        fetch_h1(0).start()
        fetch_tb = pltpu.make_async_copy(tb_r, tb_v, loc.at[4])
        fetch_tb.start()
        for i in range(n):
            pltpu.make_async_copy(o_r.at[pl.ds(i * size, size)], o_v.at[:, pl.ds(i * width, width)], loc.at[5]).start()

        own_do.wait()
        settle(do.at[pl.ds(0, (n - 1) * size)], d_r.at[0])

        settle(o_v.at[:, pl.ds(0, n * width)], loc.at[5])
        pick = (
            lax.broadcasted_iota(jnp.int32, (8, width), 1) // HEAD_DIM
            == lax.broadcasted_iota(jnp.int32, (8, width), 0)
        ).astype(f32)

        def prepare(i, carry):
            rows = block_rows(i, size)
            product = do[rows, :].astype(f32) * o_v[:, block_rows(i, width)].astype(f32)
            delta[:, rows] = lax.dot_general(
                pick, product, NT, preferred_element_type=f32, precision=lax.Precision.HIGHEST
            )
            dqa[rows, :] = jnp.zeros((size, width), f32)
            return carry

        lax.fori_loop(0, n, prepare, 0)
        gacc[...] = jnp.zeros_like(gacc)
        sm[...] = jnp.zeros_like(sm)
        sm[4:12, :] = gsm_r[...]

        def pair(i, j, diagonal):
            rows, at_k = block_rows(i, size), block_rows(j, size)
            kk, vv = k_r[at_k, :], v_r[at_k, :]
            qs, dd = q_r[rows, :] * jnp.asarray(scale, bf16), do[rows, :]
            dq = dk = dv = None
            for h in range(heads):
                qh, dh_, kh = only_head(qs, h), only_head(dd, h), only_head(kk, h)
                p = jnp.exp(row_dot(kk, qh) - lse_r[h : h + 1, rows])
                if diagonal:
                    k_pos = lax.broadcasted_iota(jnp.int32, (size, size), 0)
                    q_pos = lax.broadcasted_iota(jnp.int32, (size, size), 1)
                    p = jnp.where(k_pos <= q_pos, p, 0.0)
                dp = row_dot(vv, dh_)
                ds = (p * (dp - delta[h : h + 1, rows])).astype(bf16)
                one, two, three = dot(p.astype(bf16), dh_), dot(ds, qh), col_dot(ds, kh)
                dv = one if dv is None else dv + one
                dk = two if dk is None else dk + two
                dq = three if dq is None else dq + three
            dva[...] += dv
            dka[...] += dk
            dqa[rows, :] += dq

        def owner(j):
            return j // half, lax.rem(j, half)

        def finish_block(j):
            core_j, low_j = owner(j)

            @pl.when(core_j == core)
            def _():
                settle(rd.at[0], y_r.at[low_j])

                def add(t, carry):
                    rows = pl.ds(pl.multiple_of(t * 128, 128), 128)
                    rd[low_j, rows, :] = (pf[rows, :] + rd[low_j, rows, :].astype(f32)).astype(bf16)
                    return carry

                lax.fori_loop(0, size // 128, add, 0)

                @pl.when(low_j != low)
                def _():
                    slot = lax.rem(low_j - low + half, half) - 1
                    send(rd.at[low_j], rzd.at[slot], (e_s, e_r), 0, (at.team * half + low_j, at.k))

        def column(j, carry):
            fetch_h1(j).wait()

            @pl.when(j + 1 < n)
            def _():
                fetch_h1(j + 1).start()

            dka[...] = jnp.zeros_like(dka)
            dva[...] = jnp.zeros_like(dva)
            pair(j, j, True)

            def inner(i, c2):
                pair(i, j, False)
                return c2

            lax.fori_loop(j + 1, n, inner, 0)
            dqb = (dqa[block_rows(j, size), :] * scale).astype(bf16)
            dkb, dvb = dka[...].astype(bf16), dva[...].astype(bf16)
            dqkv[:, 0:width] = dqb
            dqkv[:, width : 2 * width] = dkb
            dqkv[:, 2 * width : 3 * width] = dvb
            mine = block_rows(rank, width)
            sm[2:3, mine] += jnp.sum(dqb.astype(f32), axis=0, keepdims=True)
            sm[3:4, mine] += jnp.sum(dvb.astype(f32), axis=0, keepdims=True)

            @pl.when(j > 0)
            def _():
                finish_block(j - 1)

            core_j, low_j = owner(j)

            def project(t, c2):
                rows = pl.ds(pl.multiple_of(t * 256, 256), 256)
                part = row_dot(dqkv[rows, :], wq_r[...])

                @pl.when(core_j == core)
                def _():
                    pf[rows, :] = part

                @pl.when(core_j != core)
                def _():
                    sd[low_j, rows, :] = part.astype(bf16)

                return c2

            lax.fori_loop(0, size // 256, project, 0)

            @pl.when(core_j != core)
            def _():
                send(sd.at[low_j], rd.at[low_j], (y_s, y_r), low_j, at.partner())

            slot = lax.rem(j, 2)
            for t in range(3):
                cols = slice(t * width, (t + 1) * width)
                gacc[:, cols] += col_dot(hb[block_rows(slot, size), :], dqkv[:, cols])
            for c in range(nc):

                @pl.when(j == min(c + 1, n - 1))
                def _(c=c):
                    p_to_z(c)

            return carry

        lax.fori_loop(0, n, column, 0)
        gqb[...] = gacc[...].astype(bf16)
        for step in range(1, planes):
            other = at.beside(step)
            for s in range(n):
                send(
                    gqb.at[block_rows(s * m + 2 * other, rq, 2)],
                    rqp.at[block_rows((step - 1) * n + s, 2 * rq)],
                    (m_s, m_r), 0, (at.s, 2 * other + core),
                )
        finish_block(jnp.int32(n - 1))
        own_dres.wait()
        fetch_tb.wait()
        if half > 1:
            settle(rzd, e_r.at[0])

        def norm_step(t, carry):
            sum_g, sum_s = carry
            rows = pl.ds(pl.multiple_of(t * 128, 128), 128)
            dh1 = rd[low, rows, :].astype(f32)
            for slot in range(half - 1):
                dh1 = dh1 + rzd[slot, rows, :].astype(f32)
            normed, inv = normalize(tb_v[rows, :].astype(f32))
            grad = gt_r[rows, :] + norm_back(dh1 * sv_r[0:1, :], normed, inv)
            gt_r[rows, :] = grad
            sg[rows, :] = grad.astype(bf16)

            @pl.when(away)
            def _():
                send(sg.at[rows], rg.at[rows], (x_s, x_r), 1, at.swap())

            return (
                sum_g + jnp.sum(dh1 * normed, axis=0, keepdims=True),
                sum_s + jnp.sum(dh1, axis=0, keepdims=True),
            )

        zero = jnp.zeros((1, d), f32)
        sum_g, sum_s = lax.fori_loop(0, size // 128, norm_step, (zero, zero))
        sm[0:1, :] = sum_g
        sm[1:2, :] = sum_s

        for step in range(1, n):
            s = at.along(step)
            send(sm.at[:, block_rows(s, lanes_s)], smz.at[step - 1], (m_s, m_r), 1, (s, at.k))

        settle(rqp, m_r.at[0])

        def add_q(s, carry):
            rows = block_rows(s * m + 2 * at.plane, rq, 2)
            total = gqb[rows, :].astype(f32)
            for step in range(1, planes):
                total = total + rqp[block_rows((step - 1) * n + s, 2 * rq), :].astype(f32)
            gqb[rows, :] = total.astype(bf16)
            return carry

        lax.fori_loop(0, n, add_q, 0)
        for l in range(half):
            row = ((1 - at.team) * half + l) * m + 2 * at.plane
            send(gqb.at[block_rows(row, rq, 2)], rqh.at[block_rows(l, 2 * rq)], (m_s, m_r), 2, at.across())

        settle(smz, m_r.at[1])
        total = sm[:, block_rows(at.s, lanes_s)]
        for step in range(1, n):
            total = total + smz[step - 1]
        small_r[...] = total
        for step in range(1, planes):
            send(small_r, smp.at[step - 1], (m_s, m_r), 3, (at.s, 2 * at.beside(step) + core))

        settle(rqh, m_r.at[2])
        for l in range(half):
            rows = block_rows((at.team * half + l) * m + 2 * at.plane, rq, 2)
            gqb[rows, :] = (
                gqb[rows, :].astype(f32) + rqh[block_rows(l, 2 * rq), :].astype(f32)
            ).astype(bf16)

        def member_rows(r):
            return block_rows((at.team * half + lax.rem(r, half)) * m + 2 * at.plane + r // half, rq)

        for step in range(1, n):
            other = lax.rem(rank + step, n)
            send(gqb.at[member_rows(other)], gq_r.at[rank], (m_s, m_r), 4, at.member(other))
        pltpu.make_async_copy(gqb.at[member_rows(rank)], gq_r.at[rank], loc.at[0]).start()

        for c in range(nc):
            z_to_out(c)

        settle(smp, m_r.at[3])
        settle(smp, m_s.at[3])
        total = small_r[...]
        for step in range(1, planes):
            total = total + smp[step - 1]
        small_r[...] = total
        send(small_r, smc, (m_s, m_r), 5, at.partner())
        settle(smc, m_r.at[5])
        settle(smc, m_s.at[5])
        small_r[...] = small_r[...] + smc[...]

        settle(gq_r.at[pl.ds(0, n - 1)], m_r.at[4])
        settle(gq_r.at[0], loc.at[0])

        @pl.when(away)
        def _():
            settle(rg, x_r.at[1])
            settle(reso_r, x_r.at[0])
            settle(reso_r, x_s.at[0])
            settle(rg, x_s.at[1])

            def widen(t, carry):
                rows = pl.ds(pl.multiple_of(t * 128, 128), 128)
                gt_r[rows, :] = rg[rows, :].astype(f32)
                return carry

            lax.fori_loop(0, size // 128, widen, 0)

        @pl.when(jnp.logical_not(away))
        def _():
            settle(reso_r, loc.at[1])

        settle(do.at[pl.ds(0, (n - 1) * size)], d_s.at[0])
        for c in range(nc):
            settle(rc[c], c_s.at[c])
            settle(rp[c], p_s.at[c])
            settle(rz[c], z_s.at[c])
        for l in range(half):
            settle(rd.at[0], y_s.at[l])
        if half > 1:
            settle(rzd, e_s.at[0])
        settle(rqp, m_s.at[0])
        settle(smz, m_s.at[1])
        settle(rqh, m_s.at[2])
        settle(gq_r.at[pl.ds(0, n - 1)], m_s.at[4])

    def sds(shape, dtype=bf16):
        return jax.ShapeDtypeStruct(shape, dtype)

    def per_chunk(count, dtype=bf16):
        return [pltpu.VMEM((count * c[3], c[5]), dtype) for c in chunks]

    sems = pltpu.SemaphoreType.DMA
    return pl.pallas_call(
        kernel,
        name="attend_back_reduce",
        out_shape=(
            sds((size, d)),
            sds((size, d), f32),
            sds((n, rq, 3 * width)),
            sds((ro, gwo.shape[1]), f32),
            sds((ri, gwi.shape[1]), f32),
            sds((rb, gwb.shape[1]), f32),
            sds((16, lanes_s), f32),
        ),
        in_specs=[HB] * 3 + [VM] * 3 + [HB, VM, HB, VM, HB] + [VM] * 2 + [HB] * 3,
        out_specs=(HB,) + (VM,) * 6,
        scratch_shapes=[
            pltpu.VMEM((length, width), bf16),
            pltpu.VMEM((8, length), f32),
            pltpu.VMEM((length, width), f32),
            pltpu.VMEM((size, width), f32),
            pltpu.VMEM((size, width), f32),
            pltpu.VMEM((size, 3 * width), bf16),
            pltpu.VMEM((d, 3 * width), f32),
            pltpu.VMEM(((planes - 1) * n * 2 * rq, 3 * width), bf16),
            pltpu.VMEM((half * 2 * rq, 3 * width), bf16),
            pltpu.VMEM((size, d), f32),
            pltpu.VMEM((half, size, d), bf16),
            pltpu.VMEM((half, size, d), bf16),
            pltpu.VMEM((max(half - 1, 1), size, d), bf16),
            pltpu.VMEM((size, d), bf16),
            pltpu.VMEM((16, d), f32),
            pltpu.VMEM((n - 1, 16, lanes_s), f32),
            pltpu.VMEM((planes - 1, 16, lanes_s), f32),
            pltpu.VMEM((16, lanes_s), f32),
        ]
        + per_chunk(n * planes)
        + per_chunk(n * planes)
        + per_chunk((planes - 1) * n)
        + per_chunk(n - 1)
        + [
            sems((1,)), sems((1,)),
            sems((2,)), sems((2,)),
            sems((half,)), sems((half,)),
            sems((1,)), sems((1,)),
            sems((nc,)), sems((nc,)),
            sems((nc,)), sems((nc,)),
            sems((nc,)), sems((nc,)),
            sems((6,)), sems((6,)),
            sems((4 + nc,)),
        ],
        compiler_params=pltpu.CompilerParams(
            collective_id=1, has_side_effects=True, vmem_limit_bytes=67043328
        ),
    )(res, dat, dres, q, k, v, o, lse, h1, wq, tb, sv, gsm, gwo, gwi, gwb)


def solution(mesh):
    n, m = mesh.shape["seq"], mesh.shape["shard"]
    nd = n * m

    def per_device(
        tokens, ln1_gain, ln1_bias, w_qkv, bias_query, bias_value, w_out, bias_out,
        ln2_gain, ln2_bias, w_in, bias_in, w_back, bias_back, cotangent,
    ):
        d = tokens.shape[2]
        width = d // n
        index = lax.axis_index("seq") * m + lax.axis_index("shard")
        pack = small_pack(
            index,
            [ln1_gain, ln1_bias, bias_query, bias_value, bias_out, ln2_gain, ln2_bias, bias_back, bias_in],
        )
        rq = w_qkv.shape[0]
        by_rank = w_qkv.reshape(rq, 3, n, width).transpose(2, 0, 1, 3).reshape(n, rq, 3 * width)
        (full_out, full_in, full_back, q, k, v, o, lse, att_tok, h1, wq, tb, cot_b, sv) = forward_call(
            n, m, tokens[0], cotangent[0], by_rank, pack, w_out, w_in, w_back
        )
        per = d // nd
        parts = bias_in.shape[0] // per
        full_bin = sv[8 : 8 + parts].reshape(parts, nd, per).transpose(1, 0, 2).reshape(-1)
        g_two, s_two = sv[5], sv[6]

        x_f = tb.astype(f32)
        resid = x_f + dot(att_tok, full_out) + sv[4]
        normed2, scale2 = normalize(resid)
        h_two = (normed2 * g_two + s_two).astype(bf16)
        pre = dot(h_two, full_in) + full_bin
        act_val, slope = gelu_pair(pre)
        act = act_val.astype(bf16)
        result = (resid + dot(act, full_back) + sv[7]).astype(bf16)
        cot_f = cot_b.astype(f32)
        g_w_back = col_dot(act, cot_b).astype(bf16)
        g_b_back = jnp.sum(cot_f, axis=0)
        d_pre = (row_dot(cot_b, full_back) * slope).astype(bf16)
        g_w_in = col_dot(h_two, d_pre).astype(bf16)
        g_b_in = jnp.sum(d_pre.astype(f32), axis=0)
        d_h2 = row_dot(d_pre, full_in)
        g_g2 = jnp.sum(d_h2 * normed2, axis=0)
        g_s2 = jnp.sum(d_h2, axis=0)
        d_resid = cot_f + norm_back(d_h2 * g_two, normed2, scale2)
        d_resid_b = d_resid.astype(bf16)
        g_w_out = col_dot(att_tok, d_resid_b).astype(bf16)
        g_b_out = jnp.sum(d_resid, axis=0)
        d_att_tok = row_dot(d_resid_b, full_out).astype(bf16)
        bin_rows = g_b_in.reshape(nd, parts, per).transpose(1, 0, 2).reshape(parts, d)
        gsm = jnp.concatenate([jnp.stack([g_b_out, g_g2, g_s2, g_b_back]), bin_rows])

        (own_result, g_tok, gq, go, gi, gb, small) = backward_call(
            n, m, result, d_att_tok, d_resid, q, k, v, o, lse, h1, wq, tb, sv, gsm, g_w_out, g_w_in, g_w_back
        )
        g_qkv = gq.reshape(n, rq, 3, width).transpose(1, 2, 0, 3).reshape(rq, 3 * d).astype(f32)
        mine = lax.dynamic_slice_in_dim(small, lax.axis_index("shard") * per, per, 1)
        return (
            own_result[None], g_tok[None], mine[0], mine[1], g_qkv, mine[2], mine[3], go, mine[4],
            mine[5], mine[6], gi, mine[8 : 8 + parts].reshape(-1), gb, mine[7],
        )

    every = ("seq", "shard")
    whole, vector, matrix = P("shard", "seq", None), P(every), P(every, None)
    return jax.shard_map(
        per_device,
        mesh=mesh,
        in_specs=(
            whole, vector, vector, matrix, vector, vector, matrix, vector, vector, vector, matrix, vector,
            matrix, vector, whole,
        ),
        out_specs=(
            whole, whole, vector, vector, matrix, vector, vector, matrix, vector, vector, vector, matrix,
            vector, matrix, vector,
        ),
        check_vma=False,
    )
```

```python
import math

import jax
import jax.numpy as jnp
from jax import lax
from jax.experimental import pallas as pl
from jax.experimental.pallas import tpu as pltpu
from jax.sharding import PartitionSpec as P

HEAD_DIM = 64
PUMPS = ((('b', 0), ('b', 1)), (('z', 2),), ())
TAIL = (('a', 2), ('b', 2))
LANES = 128
PIECE = 128
MESH = pl.DeviceIdType.MESH
NT = (((1,), (1,)), ((), ()))
TN = (((0,), (0,)), ((), ()))
f32 = jnp.float32
bf16 = jnp.bfloat16

norm_eps = 1e-05
gelu_c = math.sqrt(2.0 / math.pi)
scale = 1.0 / math.sqrt(HEAD_DIM)

VM = pl.BlockSpec(memory_space=pltpu.VMEM)
HB = pl.BlockSpec(memory_space=pl.ANY)


def dot(a, b):
    return jnp.dot(a, b, preferred_element_type=f32)


def row_dot(a, b):
    return lax.dot_general(a, b, NT, preferred_element_type=f32)


def col_dot(a, b):
    return lax.dot_general(a, b, TN, preferred_element_type=f32)


def normalize(values):
    mean_row = jnp.mean(values, axis=-1, keepdims=True)
    centred = values - mean_row
    var_row = jnp.mean(centred * centred, axis=-1, keepdims=True)
    scale_row = lax.rsqrt(var_row + norm_eps)
    return (centred * scale_row, scale_row)


def norm_back(dnormed, normed, scale_row):
    return scale_row * (
        dnormed
        - jnp.mean(dnormed, axis=-1, keepdims=True)
        - normed * jnp.mean(dnormed * normed, axis=-1, keepdims=True)
    )


def gelu_pair(inputs):
    inner = gelu_c * (inputs + 0.044715 * inputs * inputs * inputs)
    tanh_val = jnp.tanh(inner)
    value = 0.5 * inputs * (1.0 + tanh_val)
    slope = 0.5 * (1.0 + tanh_val) + 0.5 * inputs * (1.0 - tanh_val * tanh_val) * gelu_c * (
        1.0 + 3.0 * 0.044715 * inputs * inputs
    )
    return (value, slope)


def block_rows(index, size, count=1):
    return pl.ds(pl.multiple_of(index * size, size), size * count)


def head_lanes(shape, head):
    return lax.broadcasted_iota(jnp.int32, shape, len(shape) - 1) // HEAD_DIM == head


def only_head(values, head):
    return jnp.where(head_lanes(values.shape, head), values, jnp.zeros_like(values))


def spread_heads(columns, rows, width):
    out = None
    for head in range(width // HEAD_DIM):
        one = jnp.broadcast_to(columns[:, head : head + 1], (rows, width))
        out = one if out is None else jnp.where(head_lanes((rows, width), head), one, out)
    return out


class Place:
    def __init__(self, n, m):
        self.n, self.m, self.half, self.planes = n, m, n // 2, m // 2
        self.s, self.k = lax.axis_index("seq"), lax.axis_index("shard")
        self.core, self.plane = lax.rem(self.k, 2), self.k // 2
        self.team, self.low = self.s // self.half, lax.rem(self.s, self.half)
        self.rank = self.low + self.half * self.core
        self.index = self.s * m + self.k
        self.odd = lax.rem(self.low, 2)

    def member(self, rank):
        return (self.team * self.half + lax.rem(rank, self.half), 2 * self.plane + rank // self.half)

    def across(self):
        return (lax.rem(self.s + self.half, self.n), self.k)

    def swap(self):
        return (lax.rem(self.s + self.half, self.n), 2 * self.plane + 1 - self.core)

    def partner(self):
        return (self.s, 2 * self.plane + 1 - self.core)

    def along(self, step):
        return lax.rem(self.s + step, self.n)

    def neighbour(self):
        return (self.team * self.half + self.low + 1 - 2 * lax.rem(self.low, 2), self.k)

    def beside(self, step):
        return lax.rem(self.plane + step, self.planes)

    def near_plane(self):
        return self.plane + 1 - 2 * lax.rem(self.plane, 2)

    def far_plane(self, step):
        return 2 * lax.rem(self.plane // 2 + step, self.planes // 2) + lax.rem(self.plane, 2)

    def greet(self):
        barrier = pltpu.get_barrier_semaphore()
        count = 0

        def signal(device):
            pl.semaphore_signal(barrier, inc=1, device_id=device, device_id_type=MESH)

        for step in range(1, self.n):
            signal((self.along(step), self.k))
            count += 1
        for step in range(self.n):
            signal((self.along(step), 2 * self.plane + 1 - self.core))
            count += 1
        for step in range(1, self.planes):
            signal((self.s, 2 * self.beside(step) + self.core))
            count += 1
        pl.semaphore_wait(barrier, count)


def send(src, dst, sems, at, device):
    pltpu.make_async_remote_copy(
        src_ref=src,
        dst_ref=dst,
        send_sem=sems[0].at[at],
        recv_sem=sems[1].at[at],
        device_id=device,
        device_id_type=MESH,
    ).start()


def settle(view, sem):
    pltpu.make_async_copy(view, view, sem).wait()


def attend_row(i, q_ref, k_ref, v_ref, o_ref, lse_ref, qm, m_s, l_s, acc, size):
    width = q_ref.shape[1]
    heads = width // HEAD_DIM
    rows = block_rows(i, size)
    q = q_ref[rows, :] * jnp.asarray(scale, bf16)
    for h in range(heads):
        qm[h] = only_head(q, h)

    def step(j, diagonal):
        at = block_rows(j, size)
        k = k_ref[at, :]
        v = v_ref[at, :]
        old = m_s[...]
        tops, sums, total = [], [], None
        for h in range(heads):
            s = row_dot(k, qm[h])
            if diagonal:
                k_pos = lax.broadcasted_iota(jnp.int32, (size, size), 0)
                q_pos = lax.broadcasted_iota(jnp.int32, (size, size), 1)
                s = jnp.where(k_pos <= q_pos, s, -1e30)
            top = jnp.max(s, axis=0, keepdims=True)
            if not diagonal:
                top = jnp.maximum(old[h : h + 1], top)
            p = jnp.exp(s - top)
            tops.append(top)
            sums.append(jnp.sum(p, axis=0, keepdims=True))
            part = col_dot(p.astype(bf16), only_head(v, h))
            total = part if total is None else total + part
        rest = [jnp.zeros((8 - heads, size), f32)] if heads < 8 else []
        top = jnp.concatenate(tops + rest, 0)
        add = jnp.concatenate(sums + rest, 0)
        if diagonal:
            l_s[...] = add
            acc[...] = total
        else:
            fade = jnp.exp(old - top)
            l_s[...] = l_s[...] * fade + add
            acc[...] = acc[...] * spread_heads(jnp.transpose(fade), size, width) + total
        m_s[...] = top

    step(i, True)

    def body(j, carry):
        step(j, False)
        return carry

    lax.fori_loop(0, i, body, 0)
    l = l_s[...]
    lse_ref[:, rows] = m_s[...] + jnp.log(l)
    o_ref[rows, :] = (acc[...] * spread_heads(jnp.transpose(1.0 / l), size, width)).astype(bf16)


def forward_call(n, m, tok, cot, wq_s, sm_s, wo_s, wi_s, wb_s):
    size, d = tok.shape
    nd = n * m
    length = n * size
    width = d // n
    half = n // 2
    rq = wq_s.shape[0]
    ff_half = wi_s.shape[1] // 2
    cells = (n, n, half)
    nc = len(cells)

    def kernel(
        tok_r, cot_r, wqs_r, sms_r, wos_r, wis_r, wbs_r,
        wo_r, wi_r, wb_r, q_r, k_r, v_r, o_r, lse_r, att_r, h1_r, wq_r, tb_r, cb_r, sv_r,
        q_v, k_v, v_v, h1_v, wq_v, tokf, sma, qm, m_s, l_s, acc, vec,
        t_send, t_recv, w_send, w_recv, a_send, a_recv, z_send, z_recv,
        lo_send, lo_recv, hi_send, hi_recv, b_send, b_recv, c_send, c_recv, loc,
    ):
        at = Place(n, m)
        planes, rank, core = at.planes, at.rank, at.core
        fulls, shards = (wo_r, wi_r, wb_r), (wos_r, wis_r, wbs_r)
        ts, ws, zs, cs = (t_send, t_recv), (w_send, w_recv), (z_send, z_recv), (c_send, c_recv)
        los, his, bs = (lo_send, lo_recv), (hi_send, hi_recv), (b_send, b_recv)
        rows_p = planes // 2
        near = 2 * at.near_plane() + core
        far = [2 * at.far_plane(step) + core for step in range(1, rows_p)]
        at.greet()
        away = core != at.team

        own = [(at.s, at.plane, core), (at.s, at.plane, core), (at.low, at.plane, core)]
        near_p = at.near_plane()
        far_p = [at.far_plane(step) for step in range(1, rows_p)]

        def half_of(odd):
            return wis_r.at[:, pl.ds(pl.multiple_of(odd * ff_half, ff_half), ff_half)]

        def start_z(c):
            dst = fulls[c].at[own[c]]
            if c < 2:
                for step in range(1, n):
                    s = at.along(step)
                    src = shards[c] if c == 0 else half_of(lax.rem(lax.rem(s, half), 2))
                    send(src, dst, zs, c, (s, at.k))
                src = shards[c] if c == 0 else half_of(at.odd)
                pltpu.make_async_copy(src, dst, loc.at[4 + c]).start()
                return
            for team in range(2):
                for pair in range(half // 2):
                    s = team * half + 2 * pair + at.team

                    @pl.when(s != at.s)
                    def _(s=s):
                        send(shards[c], dst, zs, c, (s, at.k))

            @pl.when(at.odd == at.team)
            def _():
                pltpu.make_async_copy(shards[c], dst, loc.at[4 + c]).start()

        def settle_z(c, sem):
            if c < 2:
                settle(fulls[c].at[pl.ds(0, n - 1), 0, 0], sem.at[c])
                return

            @pl.when(at.odd == at.team)
            def _():
                settle(fulls[c].at[pl.ds(0, half - 1), 0, 0], sem.at[c])

            @pl.when(at.odd != at.team)
            def _():
                settle(fulls[c].at[pl.ds(0, half), 0, 0], sem.at[c])

        def z_to_a(c):
            if c < 2:
                settle(fulls[c].at[own[c]], loc.at[4 + c])
            else:

                @pl.when(at.odd == at.team)
                def _():
                    settle(fulls[c].at[own[c]], loc.at[4 + c])

            settle_z(c, z_recv)
            part = fulls[c].at[:, at.plane, core]
            send(part, part, los, c, (at.s, near))
            for there in far:
                send(part, part, his, c, (at.s, there))

        def settle_far(c, sem):
            if far:
                settle(fulls[c].at[:, pl.ds(0, len(far)), 0], sem.at[c])

        def a_to_b(c):
            first = cells[c] // 2
            settle(fulls[c].at[:, 0, 0], lo_recv.at[c])
            part = fulls[c].at[pl.ds(0, first), near_p, core]
            for there in far:
                send(part, part, bs, c, (at.s, there))
            settle_far(c, hi_recv)
            for p in far_p:
                part = fulls[c].at[pl.ds(first, cells[c] - first), p, core]
                send(part, part, bs, c, (at.s, near))

        def b_to_c(c):
            settle_far(c, b_recv)
            part = fulls[c].at[:, :, core]
            send(part, part, cs, c, at.partner())

        def of_rank(r, part):
            return wqs_r.at[:, pl.ds(pl.multiple_of(part * d + r * width, width), width)]

        def to_part(part):
            return wq_v.at[block_rows(at.index, rq), pl.ds(part * width, width)]

        for part in range(3):
            pltpu.make_async_copy(of_rank(rank, part), to_part(part), loc.at[0]).start()
        own_s = pltpu.make_async_copy(sms_r, sma.at[at.index], loc.at[1])
        own_s.start()
        for step in range(1, n):
            other = lax.rem(rank + step, n)
            for part in range(3):
                send(of_rank(other, part), to_part(part), ws, 0, at.member(other))
            send(sms_r, sma.at[at.index], ws, 1, at.member(other))
        settle(wq_v.at[pl.ds(0, rq)], loc.at[0])
        own_s.wait()
        settle(wq_v.at[pl.ds(0, (n - 1) * rq)], w_recv.at[0])
        settle(sma.at[pl.ds(0, n - 1)], w_recv.at[1])
        for low in range(half):
            row = (at.team * half + low) * m + 2 * at.plane
            send(wq_v.at[block_rows(row, rq, 2)], wq_v.at[block_rows(row, rq, 2)], ws, 2, at.across())
            send(sma.at[pl.ds(row, 2)], sma.at[pl.ds(row, 2)], ws, 3, at.across())
        start_z(0)
        start_z(1)

        @pl.when(jnp.logical_not(away))
        def _():
            pltpu.make_async_copy(tok_r, tokf.at[rank], loc.at[2]).start()

        settle(wq_v.at[pl.ds(0, half * 2 * rq)], w_recv.at[2])
        settle(sma.at[pl.ds(0, half * 2)], w_recv.at[3])
        @pl.when(away)
        def _():
            send(tok_r, tokf.at[at.low + half * (1 - core)], ts, 0, at.swap())

        for step in range(1, planes):
            there = (at.s, 2 * at.beside(step) + core)
            for other in range(n):
                row = other * m + 2 * at.plane
                send(wq_v.at[block_rows(row, rq, 2)], wq_v.at[block_rows(row, rq, 2)], ws, 4, there)
                send(sma.at[pl.ds(row, 2)], sma.at[pl.ds(row, 2)], ws, 5, there)
        z_to_a(0)

        @pl.when(away)
        def _():
            settle(tokf.at[0], t_recv.at[0])

        @pl.when(jnp.logical_not(away))
        def _():
            settle(tokf.at[0], loc.at[2])

        for step in range(1, half):
            low = lax.rem(at.low + step, half)
            send(tokf.at[rank], tokf.at[rank], ts, 1, (at.team * half + low, at.k))
        send(tokf.at[rank], tokf.at[rank], ts, 2, at.partner())

        settle(wq_v.at[pl.ds(0, (planes - 1) * n * 2 * rq)], w_recv.at[4])
        settle(sma.at[pl.ds(0, (planes - 1) * n * 2)], w_recv.at[5])
        per = LANES // (d // nd)
        for group in range(d // LANES):
            total = sma[group * per].astype(f32)
            for other in range(1, per):
                total = total + sma[group * per + other].astype(f32)
            sv_r[:, group * LANES : (group + 1) * LANES] = total
            vec[0, group : group + 1, :] = total[2:3]
            vec[1, group : group + 1, :] = total[3:4]

        def norm_block(b):
            def body(t, carry):
                part = pl.ds(pl.multiple_of(t * 128, 128), 128)
                x = tokf[b, part, :].astype(f32)
                normed, _ = normalize(x)
                h1_v[pl.ds(pl.multiple_of(b * size + t * 128, 128), 128), :] = (
                    normed * sv_r[0:1, :] + sv_r[1:2, :]
                ).astype(bf16)
                return carry

            lax.fori_loop(0, size // 128, body, 0)

        groups = width // LANES
        bias_q = jnp.concatenate([vec[0, pl.ds(rank * groups + g, 1), :] for g in range(groups)], 1)
        bias_v = jnp.concatenate([vec[1, pl.ds(rank * groups + g, 1), :] for g in range(groups)], 1)

        def project_block(b):
            def body(t, carry):
                part = pl.ds(pl.multiple_of(b * size + t * 256, 256), 256)
                h = h1_v[part, :]
                q_v[part, :] = (dot(h, wq_v[:, 0:width]) + bias_q).astype(bf16)
                k_v[part, :] = dot(h, wq_v[:, width : 2 * width]).astype(bf16)
                v_v[part, :] = (dot(h, wq_v[:, 2 * width : 3 * width]) + bias_v).astype(bf16)
                return carry

            lax.fori_loop(0, size // 256, body, 0)

        def later_z():
            start_z(2)

            @pl.when(away)
            def _():
                send(cot_r, cb_r, ts, 4, at.swap())

            @pl.when(jnp.logical_not(away))
            def _():
                pltpu.make_async_copy(cot_r, cb_r, loc.at[3]).start()

        def take(t, carry):
            @pl.when(t == 1)
            def _():
                z_to_a(1)
                settle(tokf.at[0], t_recv.at[2])
                a_to_b(0)

            if half > 1:

                @pl.when(t == 2)
                def _():
                    a_to_b(1)
                    settle(tokf.at[pl.ds(0, half - 1)], t_recv.at[1])
                    for step in range(1, half):
                        b = lax.rem(at.low + step, half) + half * core
                        send(tokf.at[b], tokf.at[b], ts, 3, at.partner())

                @pl.when(t == 1 + half)
                def _():
                    settle(tokf.at[pl.ds(0, half - 1)], t_recv.at[3])
                    later_z()

            step = jnp.where(t < 2, 0, lax.rem(t - 2, max(half - 1, 1)) + 1)
            other_core = jnp.where(t < 2, t, (t - 2) // max(half - 1, 1))
            side = core + other_core - 2 * core * other_core
            b = lax.rem(at.low + step, half) + half * side
            norm_block(b)
            project_block(b)
            return carry

        lax.fori_loop(0, n, take, 0)
        beside = rank + 1 - 2 * lax.rem(rank, 2)
        leaving = [
            (tokf.at[rank], tb_r.at[0]), (tokf.at[beside], tb_r.at[1]),
            (q_v, q_r), (k_v, k_r), (v_v, v_r), (h1_v, h1_r), (wq_v, wq_r),
        ]
        for i, (src, dst) in enumerate(leaving):
            pltpu.make_async_copy(src, dst, loc.at[4 + nc + i]).start()

        pumps = PUMPS

        def row(i, carry):
            attend_row(i, q_v, k_v, v_v, o_r, lse_r, qm, m_s, l_s, acc, size)
            src = o_r.at[block_rows(i, size)]
            for which, owner in ((0, i), (1, i + 1 - 2 * lax.rem(i, 2))):
                dst = att_r.at[which, :, block_rows(rank, width)]

                @pl.when(owner != rank)
                def _(dst=dst, which=which, owner=owner):
                    send(src, dst, (a_send, a_recv), which, at.member(owner))

                @pl.when(owner == rank)
                def _(dst=dst, which=which):
                    pltpu.make_async_copy(src, dst, loc.at[which]).start()

            for when, todo in enumerate(pumps):

                @pl.when(i == n - len(pumps) + when)
                def _(todo=todo):
                    for what, c in todo:
                        {"z": z_to_a, "a": a_to_b, "b": b_to_c}[what](c)

            return carry

        lax.fori_loop(0, n, row, 0)
        for what, c in TAIL:
            {"z": z_to_a, "a": a_to_b, "b": b_to_c}[what](c)
        others = att_r.at[0, :, pl.ds(0, (n - 1) * width)]
        for which in range(2):
            settle(att_r.at[0, :, pl.ds(0, width)], loc.at[which])
            settle(others, a_recv.at[which])
        for i, (src, dst) in enumerate(leaving):
            settle(src, loc.at[4 + nc + i])
        for c in range(nc):
            settle(fulls[c].at[:, :, 0], c_recv.at[c])

        for which in range(2):
            settle(others, a_send.at[which])
        for c in range(nc):
            settle_z(c, z_send)
            settle(fulls[c].at[:, 0, 0], lo_send.at[c])
            settle_far(c, hi_send)
            settle_far(c, b_send)
            settle(fulls[c].at[:, :, 0], c_send.at[c])
        for at_sem, count in ((0, n - 1), (2, half * 2), (4, (planes - 1) * n * 2)):
            settle(wq_v.at[pl.ds(0, count * rq)], w_send.at[at_sem])
            settle(sma.at[pl.ds(0, count)], w_send.at[at_sem + 1])

        @pl.when(away)
        def _():
            settle(tokf.at[0], t_send.at[0])
            settle(cb_r, t_recv.at[4])
            settle(cb_r, t_send.at[4])

        @pl.when(jnp.logical_not(away))
        def _():
            settle(cb_r, loc.at[3])

        settle(tokf.at[0], t_send.at[2])
        if half > 1:
            settle(tokf.at[pl.ds(0, half - 1)], t_send.at[1])
            settle(tokf.at[pl.ds(0, half - 1)], t_send.at[3])

    def sds(shape, dtype=bf16):
        return jax.ShapeDtypeStruct(shape, dtype)

    sems = pltpu.SemaphoreType.DMA
    return pl.pallas_call(
        kernel,
        name="gather_attend",
        out_shape=(
            sds((n, m // 2, 2, *wo_s.shape)),
            sds((n, m // 2, 2, wi_s.shape[0], ff_half)),
            sds((half, m // 2, 2, *wb_s.shape)),
            sds((length, width)), sds((length, width)), sds((length, width)), sds((length, width)),
            sds((8, length), f32),
            sds((2, size, d)),
            sds((length, d)),
            sds((d, 3 * width)),
            sds((2, size, d)), sds((size, d)),
            sds((16, d), f32),
        ),
        in_specs=[HB] * 7,
        out_specs=(HB,) * 6 + (VM,) * 3 + (HB,) * 3 + (VM,) * 2,
        scratch_shapes=[
            pltpu.VMEM((length, width), bf16),
            pltpu.VMEM((length, width), bf16),
            pltpu.VMEM((length, width), bf16),
            pltpu.VMEM((length, d), bf16),
            pltpu.VMEM((d, 3 * width), bf16),
            pltpu.VMEM((n, size, d), bf16),
            pltpu.VMEM((nd, 16, LANES), bf16),
            pltpu.VMEM((width // HEAD_DIM, size, width), bf16),
            pltpu.VMEM((8, size), f32),
            pltpu.VMEM((8, size), f32),
            pltpu.VMEM((size, width), f32),
            pltpu.VMEM((2, max(8, d // LANES), LANES), f32),
            sems((6,)), sems((6,)),
            sems((6,)), sems((6,)),
            sems((2,)), sems((2,)),
            sems((nc,)), sems((nc,)),
            sems((nc,)), sems((nc,)),
            sems((nc,)), sems((nc,)),
            sems((nc,)), sems((nc,)),
            sems((nc,)), sems((nc,)),
            sems((11 + nc,)),
        ],
        compiler_params=pltpu.CompilerParams(
            collective_id=0, has_side_effects=True, vmem_limit_bytes=62 << 20
        ),
        cost_estimate=pl.CostEstimate(
            flops=6 * length * d * width + 2 * length * length * d // n, bytes_accessed=80 << 20, transcendentals=0
        ),
    )(tok, cot, wq_s, sm_s, wo_s, wi_s, wb_s)


def small_pack(index, vectors):
    per = vectors[0].shape[0]
    rows = [part for v in vectors for part in v.reshape(-1, per)]
    rows = jnp.stack(rows + [jnp.zeros_like(rows[0])] * (16 - len(rows)))
    lane = lax.broadcasted_iota(jnp.int32, (16, LANES), 1)
    spread = jnp.tile(rows, (1, LANES // per))
    return jnp.where(lane // per == lax.rem(index, LANES // per), spread, jnp.zeros_like(spread))


def backward_call(n, m, res, dat, dres, q, k, v, o, lse, h1, wq, tb, sv, gsm, gwo, gwi, gwb):
    size, d = dat.shape
    nd = n * m
    length = n * size
    width = d // n
    heads = width // HEAD_DIM
    half, planes = n // 2, m // 2
    rq = d // nd
    quarter = gwi.shape[4] // 2
    parts = [
        (half, *gwb.shape[3:]), (n, gwi.shape[3], quarter), (n, gwi.shape[3], quarter), (n, *gwo.shape[3:]),
    ]
    cells = [p[0] for p in parts]
    nc = len(cells)
    lanes_s = d // n

    def kernel(*refs):
        (res_r, dat_r, dres_r, q_h, k_h, v_h, o_r, lse_r, h1_r, wq_h, tb_r, sv_r, gsm_r, gwo_r, gwi_r, gwb_r) = refs[:16]
        (reso_r, gt_r, gq_r, go_r, gi_r, gb_r, small_r) = refs[16:23]
        (do, delta, dqa, dka, dva, dqkv, gacc, rqp, rqh, pf, sd, rd, rzd, rg, sm, smz, smp, smc) = refs[23:41]
        gqb, hb, sg, tb_v, o_v, q_r, k_r, v_r, wq_r = refs[41:50]
        rest = refs[50:]
        ga, rc, rp, rz = (rest[i * nc : (i + 1) * nc] for i in range(4))
        (d_s, d_r, x_s, x_r, y_s, y_r, e_s, e_r, c_s, c_r, p_s, p_r, z_s, z_r, m_s, m_r, yl_s, yl_r, el_s, el_r, loc) = rest[4 * nc :]
        at = Place(n, m)
        rank, core, low = at.rank, at.core, at.low
        left, right = (gwi_r.at[:, :, :, :, pl.ds(p * quarter, quarter)] for p in range(2))
        grads = (gwb_r, left, right, gwo_r)
        at.greet()
        away = core != at.team

        for step in range(1, n):
            other = lax.rem(rank + step, n)
            send(dat_r.at[:, block_rows(other, width)], do.at[block_rows(rank, size)], (d_s, d_r), 0, at.member(other))
        own_do = pltpu.make_async_copy(dat_r.at[:, block_rows(rank, width)], do.at[block_rows(rank, size)], loc.at[0])
        own_do.start()

        for c in range(nc):
            send(grads[c].at[:, :, 1 - core], rc[c], (c_s, c_r), c, at.partner())
            pltpu.make_async_copy(grads[c].at[:, :, core], ga[c], loc.at[6 + c]).start()
        fetch_tb = pltpu.make_async_copy(tb_r, tb_v, loc.at[4])
        fetch_tb.start()
        for i in range(n):
            pltpu.make_async_copy(o_r.at[pl.ds(i * size, size)], o_v.at[:, pl.ds(i * width, width)], loc.at[5]).start()

        arriving = [(q_h, q_r), (k_h, k_r), (v_h, v_r), (wq_h, wq_r)]
        for i, (src, dst) in enumerate(arriving):
            pltpu.make_async_copy(src, dst, loc.at[6 + nc + i]).start()

        own_dres = pltpu.make_async_copy(dres_r, gt_r, loc.at[2])
        own_dres.start()

        def fetch_h1(b):
            return pltpu.make_async_copy(h1_r.at[block_rows(b, size)], hb.at[block_rows(lax.rem(b, 2), size)], loc.at[3])

        def c_to_p(c):
            settle(ga[c], loc.at[6 + c])
            settle(rc[c], c_r.at[c])

            def add(t, carry):
                s, p = t // planes, lax.rem(t, planes)
                ga[c][s, p] = (ga[c][s, p].astype(f32) + rc[c][s, p].astype(f32)).astype(bf16)
                return carry

            lax.fori_loop(0, cells[c] * planes, add, 0)
            for step in range(1, planes):
                other = at.beside(step)
                send(ga[c].at[:, other], rp[c].at[step - 1], (p_s, p_r), c, (at.s, 2 * other + core))

        def p_to_z(c):
            settle(rp[c], p_r.at[c])

            def add(s, carry):
                total = ga[c][s, at.plane].astype(f32)
                for step in range(1, planes):
                    total = total + rp[c][step - 1, s].astype(f32)
                ga[c][s, at.plane] = total.astype(bf16)
                return carry

            lax.fori_loop(0, cells[c], add, 0)
            if c > 0:
                for step in range(1, n):
                    s = at.along(step)
                    send(ga[c].at[s, at.plane], rz[c].at[at.s], (z_s, z_r), c, (s, at.k))
                rz[c][at.s] = ga[c][at.s, at.plane]
                return
            source = at.team * (half // 2) + at.low // 2
            for place in range(half):
                s = at.odd * half + place

                @pl.when(s != at.s)
                def _(s=s, place=place):
                    send(ga[c].at[place, at.plane], rz[c].at[source], (z_s, z_r), c, (s, at.k))

                @pl.when(s == at.s)
                def _(place=place):
                    rz[c][source] = ga[c][place, at.plane]

        def settle_z(c, sem):
            if c > 0:
                settle(rz[c].at[pl.ds(0, n - 1)], sem.at[c])
                return

            @pl.when(at.odd == at.team)
            def _():
                settle(rz[c].at[pl.ds(0, half - 1)], sem.at[c])

            @pl.when(at.odd != at.team)
            def _():
                settle(rz[c].at[pl.ds(0, half)], sem.at[c])

        def z_to_out(c):
            settle_z(c, z_r)

            def total(sources):
                out = rz[c][sources[0]].astype(f32)
                for s in sources[1:]:
                    out = out + rz[c][s].astype(f32)
                return out

            if c == 0:
                gb_r[...] = total(range(half))
            elif c < 3:
                for odd in range(2):
                    first = (2 * odd + c - 1) * quarter
                    gi_r[:, first : first + quarter] = total([s for s in range(n) if s % half % 2 == odd])
            else:
                go_r[...] = total(range(n))

        for c in range(nc):
            c_to_p(c)
        fetch_h1(0).start()

        own_do.wait()
        settle(do.at[pl.ds(0, (n - 1) * size)], d_r.at[0])
        for i, (src, dst) in enumerate(arriving):
            settle(dst, loc.at[6 + nc + i])

        @pl.when(away)
        def _():
            send(res_r, reso_r, (x_s, x_r), 0, at.swap())

        @pl.when(jnp.logical_not(away))
        def _():
            pltpu.make_async_copy(res_r, reso_r, loc.at[1]).start()

        settle(o_v.at[:, pl.ds(0, n * width)], loc.at[5])
        pick = (
            lax.broadcasted_iota(jnp.int32, (8, width), 1) // HEAD_DIM
            == lax.broadcasted_iota(jnp.int32, (8, width), 0)
        ).astype(f32)

        def prepare(i, carry):
            rows = block_rows(i, size)
            product = do[rows, :].astype(f32) * o_v[:, block_rows(i, width)].astype(f32)
            delta[:, rows] = lax.dot_general(
                pick, product, NT, preferred_element_type=f32, precision=lax.Precision.HIGHEST
            )
            dqa[rows, :] = jnp.zeros((size, width), f32)
            return carry

        lax.fori_loop(0, n, prepare, 0)
        gacc[...] = jnp.zeros_like(gacc)
        sm[...] = jnp.zeros_like(sm)
        sm[4:12, :] = gsm_r[...]

        def pair(i, j, diagonal):
            rows, at_k = block_rows(i, size), block_rows(j, size)
            kk, vv = k_r[at_k, :], v_r[at_k, :]
            qs, dd = q_r[rows, :] * jnp.asarray(scale, bf16), do[rows, :]
            dq = dk = dv = None
            for h in range(heads):
                qh, dh_, kh = only_head(qs, h), only_head(dd, h), only_head(kk, h)
                p = jnp.exp(row_dot(kk, qh) - lse_r[h : h + 1, rows])
                if diagonal:
                    k_pos = lax.broadcasted_iota(jnp.int32, (size, size), 0)
                    q_pos = lax.broadcasted_iota(jnp.int32, (size, size), 1)
                    p = jnp.where(k_pos <= q_pos, p, 0.0)
                dp = row_dot(vv, dh_)
                ds = (p * (dp - delta[h : h + 1, rows])).astype(bf16)
                one, two, three = dot(p.astype(bf16), dh_), dot(ds, qh), col_dot(ds, kh)
                dv = one if dv is None else dv + one
                dk = two if dk is None else dk + two
                dq = three if dq is None else dq + three
            dva[...] += dv
            dka[...] += dk
            dqa[rows, :] += dq

        def owner(j):
            return j // half, lax.rem(j, half)

        def finish_block(j):
            core_j, low_j = owner(j)

            @pl.when(core_j == core)
            def _():
                settle(rd.at[0], y_r.at[low_j])

                def add(t, carry):
                    rows = pl.ds(pl.multiple_of(t * 128, 128), 128)
                    rd[low_j, rows, :] = (pf[rows, :] + rd[low_j, rows, :].astype(f32)).astype(bf16)
                    return carry

                lax.fori_loop(0, size // 128, add, 0)

                @pl.when(low_j != low)
                def _():
                    slot = lax.rem(low_j - low + half, half) - 1
                    send(rd.at[low_j], rzd.at[slot], (e_s, e_r), 0, (at.team * half + low_j, at.k))

        def column(j, carry):
            fetch_h1(j).wait()

            @pl.when(j + 1 < n)
            def _():
                fetch_h1(j + 1).start()

            dka[...] = jnp.zeros_like(dka)
            dva[...] = jnp.zeros_like(dva)
            pair(j, j, True)

            def inner(i, c2):
                pair(i, j, False)
                return c2

            lax.fori_loop(j + 1, n, inner, 0)
            dqb = (dqa[block_rows(j, size), :] * scale).astype(bf16)
            dkb, dvb = dka[...].astype(bf16), dva[...].astype(bf16)
            dqkv[:, 0:width] = dqb
            dqkv[:, width : 2 * width] = dkb
            dqkv[:, 2 * width : 3 * width] = dvb
            mine = block_rows(rank, width)
            sm[2:3, mine] += jnp.sum(dqb.astype(f32), axis=0, keepdims=True)
            sm[3:4, mine] += jnp.sum(dvb.astype(f32), axis=0, keepdims=True)

            @pl.when(j > 0)
            def _():
                finish_block(j - 1)

            core_j, low_j = owner(j)

            def project(t, c2):
                rows = pl.ds(pl.multiple_of(t * PIECE, PIECE), PIECE)
                part = row_dot(dqkv[rows, :], wq_r[...])

                @pl.when(core_j == core)
                def _():
                    pf[rows, :] = part

                @pl.when(core_j != core)
                def _():
                    sd[low_j, rows, :] = part.astype(bf16)

                    @pl.when(j == n - 1)
                    def _():
                        send(sd.at[low_j, rows], rd.at[low_j, rows], (yl_s, yl_r), t, at.partner())

                return c2

            lax.fori_loop(0, size // PIECE, project, 0)

            @pl.when(jnp.logical_and(core_j != core, j < n - 1))
            def _():
                send(sd.at[low_j], rd.at[low_j], (y_s, y_r), low_j, at.partner())

            slot = lax.rem(j, 2)
            for t in range(3):
                cols = slice(t * width, (t + 1) * width)
                gacc[:, cols] += col_dot(hb[block_rows(slot, size), :], dqkv[:, cols])
            for c in range(nc - 1):

                @pl.when(j == min(c, n - 2))
                def _(c=c):
                    p_to_z(c)

            return carry

        lax.fori_loop(0, n, column, 0)
        gqb[...] = gacc[...].astype(bf16)
        for step in range(1, planes):
            other = at.beside(step)
            for s in range(n):
                send(
                    gqb.at[block_rows(s * m + 2 * other, rq, 2)],
                    rqp.at[block_rows((step - 1) * n + s, 2 * rq)],
                    (m_s, m_r), 0, (at.s, 2 * other + core),
                )
        pieces = size // PIECE
        last = half - 1
        owner_last = (at.team * half + last, at.k)

        def pair_piece(rows):
            rd[last, rows, :] = (pf[rows, :] + rd[last, rows, :].astype(f32)).astype(bf16)

        @pl.when(jnp.logical_and(core == 1, low != last))
        def _():
            def pass_on(t, carry):
                rows = pl.ds(pl.multiple_of(t * PIECE, PIECE), PIECE)
                settle(rd.at[last, rows], yl_r.at[t])
                pair_piece(rows)
                send(rd.at[last, rows], rzd.at[last - low - 1, rows], (el_s, el_r), t, owner_last)
                return carry

            lax.fori_loop(0, pieces, pass_on, 0)

        own_dres.wait()
        fetch_tb.wait()
        if half > 1:

            @pl.when(rank != n - 1)
            def _():
                settle(rzd, e_r.at[0])

        def norm_step(t, carry):
            sum_g, sum_s = carry
            rows = pl.ds(pl.multiple_of(t * PIECE, PIECE), PIECE)

            @pl.when(rank == n - 1)
            def _():
                settle(rd.at[last, rows], yl_r.at[t])
                pair_piece(rows)
                if half > 1:
                    settle(rzd.at[:, rows], el_r.at[t])

            dh1 = rd[low, rows, :].astype(f32)
            for slot in range(half - 1):
                dh1 = dh1 + rzd[slot, rows, :].astype(f32)
            normed, inv = normalize(tb_v[rows, :].astype(f32))
            grad = gt_r[rows, :] + norm_back(dh1 * sv_r[0:1, :], normed, inv)
            gt_r[rows, :] = grad
            sg[rows, :] = grad.astype(bf16)

            @pl.when(away)
            def _():
                send(sg.at[rows], rg.at[rows], (x_s, x_r), 1, at.swap())

            return (
                sum_g + jnp.sum(dh1 * normed, axis=0, keepdims=True),
                sum_s + jnp.sum(dh1, axis=0, keepdims=True),
            )

        zero = jnp.zeros((1, d), f32)
        sum_g, sum_s = lax.fori_loop(0, pieces, norm_step, (zero, zero))
        sm[0:1, :] = sum_g
        sm[1:2, :] = sum_s

        settle(rqp, m_r.at[0])

        def add_q(s, carry):
            rows = block_rows(s * m + 2 * at.plane, rq, 2)
            total = gqb[rows, :].astype(f32)
            for step in range(1, planes):
                total = total + rqp[block_rows((step - 1) * n + s, 2 * rq), :].astype(f32)
            gqb[rows, :] = total.astype(bf16)
            return carry

        lax.fori_loop(0, n, add_q, 0)
        for l in range(half):
            row = ((1 - at.team) * half + l) * m + 2 * at.plane
            send(gqb.at[block_rows(row, rq, 2)], rqh.at[block_rows(l, 2 * rq)], (m_s, m_r), 2, at.across())

        p_to_z(nc - 1)
        send(sm, smc, (m_s, m_r), 1, at.partner())
        settle(rqh, m_r.at[2])
        for l in range(half):
            rows = block_rows((at.team * half + l) * m + 2 * at.plane, rq, 2)
            gqb[rows, :] = (
                gqb[rows, :].astype(f32) + rqh[block_rows(l, 2 * rq), :].astype(f32)
            ).astype(bf16)

        def member_rows(r):
            return block_rows((at.team * half + lax.rem(r, half)) * m + 2 * at.plane + r // half, rq)

        for step in range(1, n):
            other = lax.rem(rank + step, n)
            send(gqb.at[member_rows(other)], gq_r.at[rank], (m_s, m_r), 4, at.member(other))
        pltpu.make_async_copy(gqb.at[member_rows(rank)], gq_r.at[rank], loc.at[0]).start()

        settle(smc, m_r.at[1])
        settle(smc, m_s.at[1])
        sm[...] = sm[...] + smc[...]
        for step in range(1, planes):
            send(sm, smp.at[step - 1], (m_s, m_r), 3, (at.s, 2 * at.beside(step) + core))
        for c in range(nc):
            z_to_out(c)
        settle(smp, m_r.at[3])
        settle(smp, m_s.at[3])
        total = sm[...]
        for step in range(1, planes):
            total = total + smp[step - 1]
        sm[...] = total
        for step in range(1, n):
            s = at.along(step)
            send(sm.at[:, block_rows(s, lanes_s)], smz.at[step - 1], (m_s, m_r), 5, (s, at.k))
        settle(smz, m_r.at[5])
        total = sm[:, block_rows(at.s, lanes_s)]
        for step in range(1, n):
            total = total + smz[step - 1]
        small_r[...] = total

        settle(gq_r.at[pl.ds(0, n - 1)], m_r.at[4])
        settle(gq_r.at[0], loc.at[0])

        @pl.when(away)
        def _():
            settle(rg, x_r.at[1])
            settle(rg, x_s.at[1])
            settle(reso_r, x_r.at[0])
            settle(reso_r, x_s.at[0])

            def widen(t, carry):
                rows = pl.ds(pl.multiple_of(t * 128, 128), 128)
                gt_r[rows, :] = rg[rows, :].astype(f32)
                return carry

            lax.fori_loop(0, size // 128, widen, 0)

        @pl.when(jnp.logical_not(away))
        def _():
            settle(reso_r, loc.at[1])

        settle(do.at[pl.ds(0, (n - 1) * size)], d_s.at[0])
        for c in range(nc):
            settle(rc[c], c_s.at[c])
            settle(rp[c], p_s.at[c])
            settle_z(c, z_s)
        for l in range(half - 1):
            settle(rd.at[0], y_s.at[l])

        @pl.when(core == 1)
        def _():
            settle(rd.at[0], y_s.at[last])

        @pl.when(core == 0)
        def _():
            for t in range(pieces):
                settle(rd.at[0, pl.ds(0, PIECE)], yl_s.at[t])

        passes = jnp.logical_and(core == 1, low != last)

        @pl.when(passes)
        def _():
            for t in range(pieces):
                settle(rd.at[0, pl.ds(0, PIECE)], el_s.at[t])

        if half > 2:

            @pl.when(passes)
            def _():
                settle(rzd.at[pl.ds(0, half - 2)], e_s.at[0])

        if half > 1:

            @pl.when(jnp.logical_not(passes))
            def _():
                settle(rzd, e_s.at[0])

        settle(rqp, m_s.at[0])
        settle(smz, m_s.at[5])
        settle(rqh, m_s.at[2])
        settle(gq_r.at[pl.ds(0, n - 1)], m_s.at[4])

    def sds(shape, dtype=bf16):
        return jax.ShapeDtypeStruct(shape, dtype)

    sems = pltpu.SemaphoreType.DMA
    return pl.pallas_call(
        kernel,
        name="attend_back_reduce",
        out_shape=(
            sds((size, d)),
            sds((size, d), f32),
            sds((n, rq, 3 * width)),
            sds(gwo.shape[3:], f32),
            sds((gwi.shape[3], 2 * gwi.shape[4]), f32),
            sds(gwb.shape[3:], f32),
            sds((16, lanes_s), f32),
        ),
        in_specs=[HB] * 7 + [VM, HB, HB, HB] + [VM] * 2 + [HB] * 3,
        out_specs=(HB,) + (VM,) * 6,
        scratch_shapes=[
            pltpu.VMEM((length, width), bf16),
            pltpu.VMEM((8, length), f32),
            pltpu.VMEM((length, width), f32),
            pltpu.VMEM((size, width), f32),
            pltpu.VMEM((size, width), f32),
            pltpu.VMEM((size, 3 * width), bf16),
            pltpu.VMEM((d, 3 * width), f32),
            pltpu.VMEM(((planes - 1) * n * 2 * rq, 3 * width), bf16),
            pltpu.VMEM((half * 2 * rq, 3 * width), bf16),
            pltpu.VMEM((size, d), f32),
            pltpu.VMEM((half, size, d), bf16),
            pltpu.VMEM((half, size, d), bf16),
            pltpu.VMEM((max(half - 1, 1), size, d), bf16),
            pltpu.VMEM((size, d), bf16),
            pltpu.VMEM((16, d), f32),
            pltpu.VMEM((n - 1, 16, lanes_s), f32),
            pltpu.VMEM((planes - 1, 16, d), f32),
            pltpu.VMEM((16, d), f32),
        ]
        + [
            pltpu.VMEM((d, 3 * width), bf16),
            pltpu.VMEM((2 * size, d), bf16),
            pltpu.VMEM((size, d), bf16),
            pltpu.VMEM((size, d), bf16),
            pltpu.VMEM((size, d), bf16),
            pltpu.VMEM((length, width), bf16),
            pltpu.VMEM((length, width), bf16),
            pltpu.VMEM((length, width), bf16),
            pltpu.VMEM((d, 3 * width), bf16),
        ]
        + [pltpu.VMEM((count, planes, rows, cols), bf16) for count, rows, cols in parts] * 2
        + [pltpu.VMEM((planes - 1, *part), bf16) for part in parts]
        + [pltpu.VMEM(part, bf16) for part in parts]
        + [
            sems((1,)), sems((1,)),
            sems((2,)), sems((2,)),
            sems((half,)), sems((half,)),
            sems((1,)), sems((1,)),
            sems((nc,)), sems((nc,)),
            sems((nc,)), sems((nc,)),
            sems((nc,)), sems((nc,)),
            sems((6,)), sems((6,)),
            sems((size // PIECE,)), sems((size // PIECE,)),
            sems((size // PIECE,)), sems((size // PIECE,)),
            sems((10 + nc,)),
        ],
        compiler_params=pltpu.CompilerParams(
            collective_id=1, has_side_effects=True, vmem_limit_bytes=67043328
        ),
        cost_estimate=pl.CostEstimate(
            flops=12 * length * d * width + 5 * length * length * d // n, bytes_accessed=80 << 20, transcendentals=0
        ),
    )(res, dat, dres, q, k, v, o, lse, h1, wq, tb, sv, gsm, gwo, gwi, gwb)


def solution(mesh):
    n, m = mesh.shape["seq"], mesh.shape["shard"]
    nd = n * m
    every = ("seq", "shard")

    def per_device(
        tokens, ln1_gain, ln1_bias, w_qkv, bias_query, bias_value, w_out, bias_out,
        ln2_gain, ln2_bias, w_in, bias_in, w_back, bias_back, cotangent,
    ):
        d = tokens.shape[2]
        width = d // n
        index = lax.axis_index("seq") * m + lax.axis_index("shard")
        pack = small_pack(
            index,
            [ln1_gain, ln1_bias, bias_query, bias_value, bias_out, ln2_gain, ln2_bias, bias_back, bias_in],
        )
        rq = w_qkv.shape[0]
        ff = w_in.shape[1]
        rq = w_qkv.shape[0]
        (full_out, full_in, full_back, q, k, v, o, lse, att_two, h1, wq, tb, cot_own, sv) = forward_call(
            n, m, tokens[0], cotangent[0], w_qkv, pack, w_out, w_in, w_back
        )
        full_out = full_out.reshape(d, d)
        half_in = full_in.reshape(d, ff // 2)
        half_back = full_back.reshape(ff // 2, d)
        odd = lax.rem(lax.rem(lax.axis_index("seq"), n // 2), 2)
        per = d // nd
        parts = bias_in.shape[0] // per
        half_bin = lax.dynamic_slice_in_dim(sv[8 : 8 + parts], odd * (d // 2), d // 2, 1)
        half_bin = half_bin.reshape(parts, nd // 2, per).transpose(1, 0, 2).reshape(-1)
        g_two, s_two = sv[5], sv[6]

        def to_neighbour(values):
            pairs = []
            for s in range(n):
                there = s // 2 * 2 + 1 - s % 2
                pairs += [(s * m + k, there * m + k) for k in range(m)]
            return lax.ppermute(values.astype(bf16), every, pairs).astype(f32)

        size = tokens.shape[1]
        cot_two = jnp.concatenate([cot_own, to_neighbour(cot_own).astype(bf16)])
        x_f = tb.reshape(2 * size, d).astype(f32)
        att_two = att_two.reshape(2 * size, d)
        resid = x_f + dot(att_two, full_out) + sv[4]
        normed2, scale2 = normalize(resid)
        h_two = (normed2 * g_two + s_two).astype(bf16)
        pre = dot(h_two, half_in) + half_bin
        act = gelu_pair(pre)[0].astype(bf16)
        out_part = dot(act, half_back)
        leaves = out_part[size:].astype(bf16)
        others_out = to_neighbour(leaves)
        pre, leaves = lax.optimization_barrier((pre, leaves))
        d_pre = (row_dot(cot_two, half_back) * gelu_pair(pre)[1]).astype(bf16)
        g_b_in = jnp.sum(d_pre.astype(f32), axis=0)
        d_h2_part = row_dot(d_pre, half_in)
        leaves = d_h2_part[size:].astype(bf16)
        others_d = to_neighbour(leaves)
        pre, d_pre, leaves = lax.optimization_barrier((pre, d_pre, leaves))
        g_w_back = col_dot(gelu_pair(pre)[0].astype(bf16), cot_two).astype(bf16)
        g_w_in = col_dot(h_two, d_pre).astype(bf16)

        resid, normed2, scale2 = resid[:size], normed2[:size], scale2[:size]
        att_tok, cot_f = att_two[:size], cot_two[:size].astype(f32)
        result = (resid + out_part[:size] + others_out + sv[7]).astype(bf16)
        g_b_back = jnp.sum(cot_f, axis=0)
        d_h2 = d_h2_part[:size] + others_d
        g_g2 = jnp.sum(d_h2 * normed2, axis=0)
        g_s2 = jnp.sum(d_h2, axis=0)
        d_resid = cot_f + norm_back(d_h2 * g_two, normed2, scale2)
        d_resid_b = d_resid.astype(bf16)
        g_w_out = col_dot(att_tok, d_resid_b).astype(bf16)
        g_b_out = jnp.sum(d_resid, axis=0)
        d_att_tok = row_dot(d_resid_b, full_out).astype(bf16)
        bin_rows = g_b_in.reshape(nd // 2, parts, per).transpose(1, 0, 2).reshape(parts, d // 2)
        bin_rows = jnp.where(
            lax.broadcasted_iota(jnp.int32, (parts, d), 1) // (d // 2) == odd, jnp.tile(bin_rows, (1, 2)), 0.0
        )
        gsm = jnp.concatenate([jnp.stack([g_b_out, g_g2, g_s2, g_b_back]), bin_rows])

        (own_result, g_tok, gq, go, gi, gb, small) = backward_call(
            n, m, result, d_att_tok, d_resid, q, k, v, o, lse, h1, wq, tb[0], sv, gsm,
            g_w_out.reshape(n, m // 2, 2, d // nd, d),
            g_w_in.reshape(n, m // 2, 2, d // nd, ff // 2),
            g_w_back.reshape(n // 2, m // 2, 2, ff // nd, d),
        )
        g_qkv = gq.reshape(n, rq, 3, width).transpose(1, 2, 0, 3).reshape(rq, 3 * d).astype(f32)
        mine = lax.dynamic_slice_in_dim(small, lax.axis_index("shard") * per, per, 1)
        return (
            own_result[None], g_tok[None], mine[0], mine[1], g_qkv, mine[2], mine[3], go, mine[4],
            mine[5], mine[6], gi, mine[8 : 8 + parts].reshape(-1), gb, mine[7],
        )

    whole, vector, matrix = P("shard", "seq", None), P(every), P(every, None)
    return jax.shard_map(
        per_device,
        mesh=mesh,
        in_specs=(
            whole, vector, vector, matrix, vector, vector, matrix, vector, vector, vector, matrix, vector,
            matrix, vector, whole,
        ),
        out_specs=(
            whole, whole, vector, vector, matrix, vector, vector, matrix, vector, vector, vector, matrix,
            vector, matrix, vector,
        ),
        check_vma=False,
    )
```

```python
import math

import jax
import jax.numpy as jnp
from jax import lax
from jax.experimental import pallas as pl
from jax.experimental.pallas import tpu as pltpu
from jax.sharding import PartitionSpec as P

HEAD_DIM = 64
PUMPS = ((('b', 0), ('b', 1)), (('z', 2),), ())
TAIL = (('a', 2), ('b', 2))
LANES = 128
PIECE = 128
MESH = pl.DeviceIdType.MESH
NT = (((1,), (1,)), ((), ()))
TN = (((0,), (0,)), ((), ()))
f32 = jnp.float32
bf16 = jnp.bfloat16

norm_eps = 1e-05
gelu_c = math.sqrt(2.0 / math.pi)
scale = 1.0 / math.sqrt(HEAD_DIM)

VM = pl.BlockSpec(memory_space=pltpu.VMEM)
HB = pl.BlockSpec(memory_space=pl.ANY)


def dot(a, b):
    return jnp.dot(a, b, preferred_element_type=f32)


def row_dot(a, b):
    return lax.dot_general(a, b, NT, preferred_element_type=f32)


def col_dot(a, b):
    return lax.dot_general(a, b, TN, preferred_element_type=f32)


def normalize(values):
    mean_row = jnp.mean(values, axis=-1, keepdims=True)
    centred = values - mean_row
    var_row = jnp.mean(centred * centred, axis=-1, keepdims=True)
    scale_row = lax.rsqrt(var_row + norm_eps)
    return (centred * scale_row, scale_row)


def norm_back(dnormed, normed, scale_row):
    return scale_row * (
        dnormed
        - jnp.mean(dnormed, axis=-1, keepdims=True)
        - normed * jnp.mean(dnormed * normed, axis=-1, keepdims=True)
    )


def gelu_pair(inputs):
    inner = gelu_c * (inputs + 0.044715 * inputs * inputs * inputs)
    tanh_val = jnp.tanh(inner)
    value = 0.5 * inputs * (1.0 + tanh_val)
    slope = 0.5 * (1.0 + tanh_val) + 0.5 * inputs * (1.0 - tanh_val * tanh_val) * gelu_c * (
        1.0 + 3.0 * 0.044715 * inputs * inputs
    )
    return (value, slope)


def block_rows(index, size, count=1):
    return pl.ds(pl.multiple_of(index * size, size), size * count)


def head_lanes(shape, head):
    return lax.broadcasted_iota(jnp.int32, shape, len(shape) - 1) // HEAD_DIM == head


def only_head(values, head):
    return jnp.where(head_lanes(values.shape, head), values, jnp.zeros_like(values))


def spread_heads(columns, rows, width):
    out = None
    for head in range(width // HEAD_DIM):
        one = jnp.broadcast_to(columns[:, head : head + 1], (rows, width))
        out = one if out is None else jnp.where(head_lanes((rows, width), head), one, out)
    return out


class Place:
    def __init__(self, n, m):
        self.n, self.m, self.half, self.planes = n, m, n // 2, m // 2
        self.s, self.k = lax.axis_index("seq"), lax.axis_index("shard")
        self.core, self.plane = lax.rem(self.k, 2), self.k // 2
        self.team, self.low = self.s // self.half, lax.rem(self.s, self.half)
        self.rank = self.low + self.half * self.core
        self.index = self.s * m + self.k
        self.odd = lax.rem(self.low, 2)

    def member(self, rank):
        return (self.team * self.half + lax.rem(rank, self.half), 2 * self.plane + rank // self.half)

    def across(self):
        return (lax.rem(self.s + self.half, self.n), self.k)

    def swap(self):
        return (lax.rem(self.s + self.half, self.n), 2 * self.plane + 1 - self.core)

    def partner(self):
        return (self.s, 2 * self.plane + 1 - self.core)

    def along(self, step):
        return lax.rem(self.s + step, self.n)

    def neighbour(self):
        return (self.team * self.half + self.low + 1 - 2 * lax.rem(self.low, 2), self.k)

    def beside(self, step):
        return lax.rem(self.plane + step, self.planes)

    def near_plane(self):
        return self.plane + 1 - 2 * lax.rem(self.plane, 2)

    def far_plane(self, step):
        return 2 * lax.rem(self.plane // 2 + step, self.planes // 2) + lax.rem(self.plane, 2)

    def greet(self):
        barrier = pltpu.get_barrier_semaphore()
        count = 0

        def signal(device):
            pl.semaphore_signal(barrier, inc=1, device_id=device, device_id_type=MESH)

        for step in range(1, self.n):
            signal((self.along(step), self.k))
            count += 1
        for step in range(self.n):
            signal((self.along(step), 2 * self.plane + 1 - self.core))
            count += 1
        for step in range(1, self.planes):
            signal((self.s, 2 * self.beside(step) + self.core))
            count += 1
        pl.semaphore_wait(barrier, count)


def send(src, dst, sems, at, device):
    pltpu.make_async_remote_copy(
        src_ref=src,
        dst_ref=dst,
        send_sem=sems[0].at[at],
        recv_sem=sems[1].at[at],
        device_id=device,
        device_id_type=MESH,
    ).start()


def settle(view, sem):
    pltpu.make_async_copy(view, view, sem).wait()


def attend_row(i, q_ref, k_ref, v_ref, o_ref, lse_ref, qm, m_s, l_s, acc, size):
    width = q_ref.shape[1]
    heads = width // HEAD_DIM
    rows = block_rows(i, size)
    q = q_ref[rows, :] * jnp.asarray(scale, bf16)
    for h in range(heads):
        qm[h] = only_head(q, h)

    def step(j, diagonal):
        at = block_rows(j, size)
        k = k_ref[at, :]
        v = v_ref[at, :]
        old = m_s[...]
        tops, sums, total = [], [], None
        for h in range(heads):
            s = row_dot(k, qm[h])
            if diagonal:
                k_pos = lax.broadcasted_iota(jnp.int32, (size, size), 0)
                q_pos = lax.broadcasted_iota(jnp.int32, (size, size), 1)
                s = jnp.where(k_pos <= q_pos, s, -1e30)
            top = jnp.max(s, axis=0, keepdims=True)
            if not diagonal:
                top = jnp.maximum(old[h : h + 1], top)
            p = jnp.exp(s - top)
            tops.append(top)
            sums.append(jnp.sum(p, axis=0, keepdims=True))
            part = col_dot(p.astype(bf16), only_head(v, h))
            total = part if total is None else total + part
        rest = [jnp.zeros((8 - heads, size), f32)] if heads < 8 else []
        top = jnp.concatenate(tops + rest, 0)
        add = jnp.concatenate(sums + rest, 0)
        if diagonal:
            l_s[...] = add
            acc[...] = total
        else:
            fade = jnp.exp(old - top)
            l_s[...] = l_s[...] * fade + add
            acc[...] = acc[...] * spread_heads(jnp.transpose(fade), size, width) + total
        m_s[...] = top

    step(i, True)

    def body(j, carry):
        step(j, False)
        return carry

    lax.fori_loop(0, i, body, 0)
    l = l_s[...]
    lse_ref[:, rows] = m_s[...] + jnp.log(l)
    o_ref[rows, :] = (acc[...] * spread_heads(jnp.transpose(1.0 / l), size, width)).astype(bf16)


def forward_call(n, m, tok, cot, wq_s, sm_s, wo_s, wi_s, wb_s):
    size, d = tok.shape
    nd = n * m
    length = n * size
    width = d // n
    half = n // 2
    rq = wq_s.shape[0]
    ff_half = wi_s.shape[1] // 2
    cells = (n, n, half)
    nc = len(cells)

    def kernel(
        tok_r, cot_r, wqs_r, sms_r, wos_r, wis_r, wbs_r,
        wo_r, wi_r, wb_r, q_r, k_r, v_r, o_r, lse_r, att_r, h1_r, wq_r, tb_r, cb_r, sv_r,
        q_v, k_v, v_v, h1_v, wq_v, tokf, sma, qm, m_s, l_s, acc, vec,
        t_send, t_recv, w_send, w_recv, a_send, a_recv, z_send, z_recv,
        lo_send, lo_recv, hi_send, hi_recv, b_send, b_recv, c_send, c_recv, loc,
    ):
        at = Place(n, m)
        planes, rank, core = at.planes, at.rank, at.core
        fulls, shards = (wo_r, wi_r, wb_r), (wos_r, wis_r, wbs_r)
        ts, ws, zs, cs = (t_send, t_recv), (w_send, w_recv), (z_send, z_recv), (c_send, c_recv)
        los, his, bs = (lo_send, lo_recv), (hi_send, hi_recv), (b_send, b_recv)
        rows_p = planes // 2
        near = 2 * at.near_plane() + core
        far = [2 * at.far_plane(step) + core for step in range(1, rows_p)]
        at.greet()
        away = core != at.team

        own = [(at.s, at.plane, core), (at.s, at.plane, core), (at.low, at.plane, core)]
        near_p = at.near_plane()
        far_p = [at.far_plane(step) for step in range(1, rows_p)]

        def half_of(odd):
            return wis_r.at[:, pl.ds(pl.multiple_of(odd * ff_half, ff_half), ff_half)]

        def start_z(c):
            dst = fulls[c].at[own[c]]
            if c < 2:
                for step in range(1, n):
                    s = at.along(step)
                    src = shards[c] if c == 0 else half_of(lax.rem(lax.rem(s, half), 2))
                    send(src, dst, zs, c, (s, at.k))
                src = shards[c] if c == 0 else half_of(at.odd)
                pltpu.make_async_copy(src, dst, loc.at[4 + c]).start()
                return
            for team in range(2):
                for pair in range(half // 2):
                    s = team * half + 2 * pair + at.team

                    @pl.when(s != at.s)
                    def _(s=s):
                        send(shards[c], dst, zs, c, (s, at.k))

            @pl.when(at.odd == at.team)
            def _():
                pltpu.make_async_copy(shards[c], dst, loc.at[4 + c]).start()

        def settle_z(c, sem):
            if c < 2:
                settle(fulls[c].at[pl.ds(0, n - 1), 0, 0], sem.at[c])
                return

            @pl.when(at.odd == at.team)
            def _():
                settle(fulls[c].at[pl.ds(0, half - 1), 0, 0], sem.at[c])

            @pl.when(at.odd != at.team)
            def _():
                settle(fulls[c].at[pl.ds(0, half), 0, 0], sem.at[c])

        def z_to_a(c):
            if c < 2:
                settle(fulls[c].at[own[c]], loc.at[4 + c])
            else:

                @pl.when(at.odd == at.team)
                def _():
                    settle(fulls[c].at[own[c]], loc.at[4 + c])

            settle_z(c, z_recv)
            part = fulls[c].at[:, at.plane, core]
            send(part, part, los, c, (at.s, near))
            for there in far:
                send(part, part, his, c, (at.s, there))

        def settle_far(c, sem):
            if far:
                settle(fulls[c].at[:, pl.ds(0, len(far)), 0], sem.at[c])

        def a_to_b(c):
            first = cells[c] // 2
            settle(fulls[c].at[:, 0, 0], lo_recv.at[c])
            part = fulls[c].at[pl.ds(0, first), near_p, core]
            for there in far:
                send(part, part, bs, c, (at.s, there))
            settle_far(c, hi_recv)
            for p in far_p:
                part = fulls[c].at[pl.ds(first, cells[c] - first), p, core]
                send(part, part, bs, c, (at.s, near))

        def b_to_c(c):
            settle_far(c, b_recv)
            part = fulls[c].at[:, :, core]
            send(part, part, cs, c, at.partner())

        def of_rank(r, part):
            return wqs_r.at[:, pl.ds(pl.multiple_of(part * d + r * width, width), width)]

        def to_part(part):
            return wq_v.at[block_rows(at.index, rq), pl.ds(part * width, width)]

        for part in range(3):
            pltpu.make_async_copy(of_rank(rank, part), to_part(part), loc.at[0]).start()
        own_s = pltpu.make_async_copy(sms_r, sma.at[at.index], loc.at[1])
        own_s.start()
        for step in range(1, n):
            other = lax.rem(rank + step, n)
            for part in range(3):
                send(of_rank(other, part), to_part(part), ws, 0, at.member(other))
            send(sms_r, sma.at[at.index], ws, 1, at.member(other))
        settle(wq_v.at[pl.ds(0, rq)], loc.at[0])
        own_s.wait()
        settle(wq_v.at[pl.ds(0, (n - 1) * rq)], w_recv.at[0])
        settle(sma.at[pl.ds(0, n - 1)], w_recv.at[1])
        for low in range(half):
            row = (at.team * half + low) * m + 2 * at.plane
            send(wq_v.at[block_rows(row, rq, 2)], wq_v.at[block_rows(row, rq, 2)], ws, 2, at.across())
            send(sma.at[pl.ds(row, 2)], sma.at[pl.ds(row, 2)], ws, 3, at.across())
        start_z(0)
        start_z(1)

        @pl.when(jnp.logical_not(away))
        def _():
            pltpu.make_async_copy(tok_r, tokf.at[rank], loc.at[2]).start()

        settle(wq_v.at[pl.ds(0, half * 2 * rq)], w_recv.at[2])
        settle(sma.at[pl.ds(0, half * 2)], w_recv.at[3])
        def cut(block, h):
            return block.at[pl.ds(h * (size // 2), size // 2)]

        @pl.when(away)
        def _():
            for h in range(2):
                send(cut(tok_r, h), cut(tokf.at[at.low + half * (1 - core)], h), ts, h, at.swap())

        for step in range(1, planes):
            there = (at.s, 2 * at.beside(step) + core)
            for other in range(n):
                row = other * m + 2 * at.plane
                send(wq_v.at[block_rows(row, rq, 2)], wq_v.at[block_rows(row, rq, 2)], ws, 4, there)
                send(sma.at[pl.ds(row, 2)], sma.at[pl.ds(row, 2)], ws, 5, there)
        z_to_a(0)

        @pl.when(jnp.logical_not(away))
        def _():
            settle(tokf.at[0], loc.at[2])

        def own_half(h):
            @pl.when(away)
            def _():
                settle(cut(tokf.at[0], h), t_recv.at[h])

            part = cut(tokf.at[rank], h)
            for step in range(1, half):
                low = lax.rem(at.low + step, half)
                send(part, part, ts, 2 + h, (at.team * half + low, at.k))
            send(part, part, ts, 4, at.partner())

        own_half(0)

        settle(wq_v.at[pl.ds(0, (planes - 1) * n * 2 * rq)], w_recv.at[4])
        settle(sma.at[pl.ds(0, (planes - 1) * n * 2)], w_recv.at[5])
        per = LANES // (d // nd)
        for group in range(d // LANES):
            total = sma[group * per].astype(f32)
            for other in range(1, per):
                total = total + sma[group * per + other].astype(f32)
            sv_r[:, group * LANES : (group + 1) * LANES] = total
            vec[0, group : group + 1, :] = total[2:3]
            vec[1, group : group + 1, :] = total[3:4]

        def norm_block(b):
            def body(t, carry):
                part = pl.ds(pl.multiple_of(t * 128, 128), 128)
                x = tokf[b, part, :].astype(f32)
                normed, _ = normalize(x)
                h1_v[pl.ds(pl.multiple_of(b * size + t * 128, 128), 128), :] = (
                    normed * sv_r[0:1, :] + sv_r[1:2, :]
                ).astype(bf16)
                return carry

            lax.fori_loop(0, size // 128, body, 0)

        groups = width // LANES
        bias_q = jnp.concatenate([vec[0, pl.ds(rank * groups + g, 1), :] for g in range(groups)], 1)
        bias_v = jnp.concatenate([vec[1, pl.ds(rank * groups + g, 1), :] for g in range(groups)], 1)

        def project_block(b):
            def body(t, carry):
                part = pl.ds(pl.multiple_of(b * size + t * 256, 256), 256)
                h = h1_v[part, :]
                q_v[part, :] = (dot(h, wq_v[:, 0:width]) + bias_q).astype(bf16)
                k_v[part, :] = dot(h, wq_v[:, width : 2 * width]).astype(bf16)
                v_v[part, :] = (dot(h, wq_v[:, 2 * width : 3 * width]) + bias_v).astype(bf16)
                return carry

            lax.fori_loop(0, size // 256, body, 0)

        def later_z():
            start_z(2)

            @pl.when(away)
            def _():
                send(cot_r, cb_r, ts, 6, at.swap())

            @pl.when(jnp.logical_not(away))
            def _():
                pltpu.make_async_copy(cot_r, cb_r, loc.at[3]).start()

        own_half(1)

        def take(t, carry):
            @pl.when(t == 1)
            def _():
                z_to_a(1)
                settle(tokf.at[0], t_recv.at[4])
                a_to_b(0)

            if half > 1:

                @pl.when(t == 2)
                def _():
                    a_to_b(1)
                    for h in range(2):
                        settle(tokf.at[pl.ds(0, half - 1), pl.ds(0, size // 2)], t_recv.at[2 + h])
                        for step in range(1, half):
                            part = cut(tokf.at[lax.rem(at.low + step, half) + half * core], h)
                            send(part, part, ts, 5, at.partner())

                @pl.when(t == 1 + half)
                def _():
                    settle(tokf.at[pl.ds(0, half - 1)], t_recv.at[5])
                    later_z()

            step = jnp.where(t < 2, 0, lax.rem(t - 2, max(half - 1, 1)) + 1)
            other_core = jnp.where(t < 2, t, (t - 2) // max(half - 1, 1))
            side = core + other_core - 2 * core * other_core
            b = lax.rem(at.low + step, half) + half * side
            norm_block(b)
            project_block(b)
            return carry

        lax.fori_loop(0, n, take, 0)
        beside = rank + 1 - 2 * lax.rem(rank, 2)
        leaving = [
            (tokf.at[rank], tb_r.at[0]), (tokf.at[beside], tb_r.at[1]),
            (q_v, q_r), (k_v, k_r), (v_v, v_r), (h1_v, h1_r), (wq_v, wq_r),
        ]
        for i, (src, dst) in enumerate(leaving):
            pltpu.make_async_copy(src, dst, loc.at[4 + nc + i]).start()

        pumps = PUMPS

        def row(i, carry):
            attend_row(i, q_v, k_v, v_v, o_r, lse_r, qm, m_s, l_s, acc, size)
            src = o_r.at[block_rows(i, size)]
            for which, owner in ((0, i), (1, i + 1 - 2 * lax.rem(i, 2))):
                dst = att_r.at[which, :, block_rows(rank, width)]

                @pl.when(owner != rank)
                def _(dst=dst, which=which, owner=owner):
                    send(src, dst, (a_send, a_recv), which, at.member(owner))

                @pl.when(owner == rank)
                def _(dst=dst, which=which):
                    pltpu.make_async_copy(src, dst, loc.at[which]).start()

            for when, todo in enumerate(pumps):

                @pl.when(i == n - len(pumps) + when)
                def _(todo=todo):
                    for what, c in todo:
                        {"z": z_to_a, "a": a_to_b, "b": b_to_c}[what](c)

            return carry

        lax.fori_loop(0, n, row, 0)
        for what, c in TAIL:
            {"z": z_to_a, "a": a_to_b, "b": b_to_c}[what](c)
        others = att_r.at[0, :, pl.ds(0, (n - 1) * width)]
        for which in range(2):
            settle(att_r.at[0, :, pl.ds(0, width)], loc.at[which])
            settle(others, a_recv.at[which])
        for i, (src, dst) in enumerate(leaving):
            settle(src, loc.at[4 + nc + i])
        for c in range(nc):
            settle(fulls[c].at[:, :, 0], c_recv.at[c])

        for which in range(2):
            settle(others, a_send.at[which])
        for c in range(nc):
            settle_z(c, z_send)
            settle(fulls[c].at[:, 0, 0], lo_send.at[c])
            settle_far(c, hi_send)
            settle_far(c, b_send)
            settle(fulls[c].at[:, :, 0], c_send.at[c])
        for at_sem, count in ((0, n - 1), (2, half * 2), (4, (planes - 1) * n * 2)):
            settle(wq_v.at[pl.ds(0, count * rq)], w_send.at[at_sem])
            settle(sma.at[pl.ds(0, count)], w_send.at[at_sem + 1])

        @pl.when(away)
        def _():
            for h in range(2):
                settle(cut(tokf.at[0], h), t_send.at[h])
            settle(cb_r, t_recv.at[6])
            settle(cb_r, t_send.at[6])

        @pl.when(jnp.logical_not(away))
        def _():
            settle(cb_r, loc.at[3])

        settle(tokf.at[0], t_send.at[4])
        if half > 1:
            for h in range(2):
                settle(tokf.at[pl.ds(0, half - 1), pl.ds(0, size // 2)], t_send.at[2 + h])
            settle(tokf.at[pl.ds(0, half - 1)], t_send.at[5])

    def sds(shape, dtype=bf16):
        return jax.ShapeDtypeStruct(shape, dtype)

    sems = pltpu.SemaphoreType.DMA
    return pl.pallas_call(
        kernel,
        name="gather_attend",
        out_shape=(
            sds((n, m // 2, 2, *wo_s.shape)),
            sds((n, m // 2, 2, wi_s.shape[0], ff_half)),
            sds((half, m // 2, 2, *wb_s.shape)),
            sds((length, width)), sds((length, width)), sds((length, width)), sds((length, width)),
            sds((8, length), f32),
            sds((2, size, d)),
            sds((length, d)),
            sds((d, 3 * width)),
            sds((2, size, d)), sds((size, d)),
            sds((16, d), f32),
        ),
        in_specs=[HB] * 7,
        out_specs=(HB,) * 6 + (VM,) * 3 + (HB,) * 3 + (VM,) * 2,
        scratch_shapes=[
            pltpu.VMEM((length, width), bf16),
            pltpu.VMEM((length, width), bf16),
            pltpu.VMEM((length, width), bf16),
            pltpu.VMEM((length, d), bf16),
            pltpu.VMEM((d, 3 * width), bf16),
            pltpu.VMEM((n, size, d), bf16),
            pltpu.VMEM((nd, 16, LANES), bf16),
            pltpu.VMEM((width // HEAD_DIM, size, width), bf16),
            pltpu.VMEM((8, size), f32),
            pltpu.VMEM((8, size), f32),
            pltpu.VMEM((size, width), f32),
            pltpu.VMEM((2, max(8, d // LANES), LANES), f32),
            sems((7,)), sems((7,)),
            sems((6,)), sems((6,)),
            sems((2,)), sems((2,)),
            sems((nc,)), sems((nc,)),
            sems((nc,)), sems((nc,)),
            sems((nc,)), sems((nc,)),
            sems((nc,)), sems((nc,)),
            sems((nc,)), sems((nc,)),
            sems((11 + nc,)),
        ],
        compiler_params=pltpu.CompilerParams(
            collective_id=0, has_side_effects=True, vmem_limit_bytes=62 << 20
        ),
        cost_estimate=pl.CostEstimate(
            flops=6 * length * d * width + 2 * length * length * d // n, bytes_accessed=80 << 20, transcendentals=0
        ),
    )(tok, cot, wq_s, sm_s, wo_s, wi_s, wb_s)


def small_pack(index, vectors):
    per = vectors[0].shape[0]
    rows = [part for v in vectors for part in v.reshape(-1, per)]
    rows = jnp.stack(rows + [jnp.zeros_like(rows[0])] * (16 - len(rows)))
    lane = lax.broadcasted_iota(jnp.int32, (16, LANES), 1)
    spread = jnp.tile(rows, (1, LANES // per))
    return jnp.where(lane // per == lax.rem(index, LANES // per), spread, jnp.zeros_like(spread))


def backward_call(n, m, res, dat, dres, q, k, v, o, lse, h1, wq, tb, sv, gsm, gwo, gwi, gwb):
    size, d = dat.shape
    nd = n * m
    length = n * size
    width = d // n
    heads = width // HEAD_DIM
    half, planes = n // 2, m // 2
    rq = d // nd
    quarter = gwi.shape[4] // 2
    parts = [
        (half, *gwb.shape[3:]), (n, gwi.shape[3], quarter), (n, gwi.shape[3], quarter), (n, *gwo.shape[3:]),
    ]
    cells = [p[0] for p in parts]
    nc = len(cells)
    lanes_s = d // n

    def kernel(*refs):
        (res_r, dat_r, dres_r, q_h, k_h, v_h, o_r, lse_r, h1_r, wq_h, tb_r, sv_r, gsm_r, gwo_r, gwi_r, gwb_r) = refs[:16]
        (reso_r, gt_r, rg, gqo_r, go_r, gi_r, gb_r, small_r) = refs[16:24]
        (do, delta, dqa, dka, dva, dqkv, gacc, rqp, rqh, pf, sd, rd, rzd, sm, smz, smp, smc) = refs[24:41]
        gqb, hb, sg, tb_v, o_v, q_r, k_r, v_r, wq_r, gq_r = refs[41:51]
        rest = refs[51:]
        ga, rc, rp, rz = (rest[i * nc : (i + 1) * nc] for i in range(4))
        (d_s, d_r, x_s, x_r, y_s, y_r, e_s, e_r, c_s, c_r, p_s, p_r, z_s, z_r, m_s, m_r, yl_s, yl_r, el_s, el_r, loc) = rest[4 * nc :]
        at = Place(n, m)
        rank, core, low = at.rank, at.core, at.low
        left, right = (gwi_r.at[:, :, :, :, pl.ds(p * quarter, quarter)] for p in range(2))
        grads = (gwb_r, left, right, gwo_r)
        at.greet()
        away = core != at.team

        for step in range(1, n):
            other = lax.rem(rank + step, n)
            send(dat_r.at[:, block_rows(other, width)], do.at[block_rows(rank, size)], (d_s, d_r), 0, at.member(other))
        own_do = pltpu.make_async_copy(dat_r.at[:, block_rows(rank, width)], do.at[block_rows(rank, size)], loc.at[0])
        own_do.start()

        for c in range(nc):
            send(grads[c].at[:, :, 1 - core], rc[c], (c_s, c_r), c, at.partner())
            pltpu.make_async_copy(grads[c].at[:, :, core], ga[c], loc.at[6 + c]).start()
        fetch_tb = pltpu.make_async_copy(tb_r.at[0], tb_v, loc.at[4])
        fetch_tb.start()
        for i in range(n):
            pltpu.make_async_copy(o_r.at[pl.ds(i * size, size)], o_v.at[:, pl.ds(i * width, width)], loc.at[5]).start()

        arriving = [(q_h, q_r), (k_h, k_r), (v_h, v_r), (wq_h, wq_r)]
        for i, (src, dst) in enumerate(arriving):
            pltpu.make_async_copy(src, dst, loc.at[6 + nc + i]).start()

        own_dres = pltpu.make_async_copy(dres_r, gt_r, loc.at[2])
        own_dres.start()

        def fetch_h1(b):
            return pltpu.make_async_copy(h1_r.at[block_rows(b, size)], hb.at[block_rows(lax.rem(b, 2), size)], loc.at[3])

        def c_to_p(c):
            settle(ga[c], loc.at[6 + c])
            settle(rc[c], c_r.at[c])

            def add(t, carry):
                s, p = t // planes, lax.rem(t, planes)
                ga[c][s, p] = (ga[c][s, p].astype(f32) + rc[c][s, p].astype(f32)).astype(bf16)
                return carry

            lax.fori_loop(0, cells[c] * planes, add, 0)
            for step in range(1, planes):
                other = at.beside(step)
                send(ga[c].at[:, other], rp[c].at[step - 1], (p_s, p_r), c, (at.s, 2 * other + core))

        def p_to_z(c):
            settle(rp[c], p_r.at[c])

            def add(s, carry):
                total = ga[c][s, at.plane].astype(f32)
                for step in range(1, planes):
                    total = total + rp[c][step - 1, s].astype(f32)
                ga[c][s, at.plane] = total.astype(bf16)
                return carry

            lax.fori_loop(0, cells[c], add, 0)
            if c > 0:
                for step in range(1, n):
                    s = at.along(step)
                    send(ga[c].at[s, at.plane], rz[c].at[at.s], (z_s, z_r), c, (s, at.k))
                rz[c][at.s] = ga[c][at.s, at.plane]
                return
            source = at.team * (half // 2) + at.low // 2
            for place in range(half):
                s = at.odd * half + place

                @pl.when(s != at.s)
                def _(s=s, place=place):
                    send(ga[c].at[place, at.plane], rz[c].at[source], (z_s, z_r), c, (s, at.k))

                @pl.when(s == at.s)
                def _(place=place):
                    rz[c][source] = ga[c][place, at.plane]

        def settle_z(c, sem):
            if c > 0:
                settle(rz[c].at[pl.ds(0, n - 1)], sem.at[c])
                return

            @pl.when(at.odd == at.team)
            def _():
                settle(rz[c].at[pl.ds(0, half - 1)], sem.at[c])

            @pl.when(at.odd != at.team)
            def _():
                settle(rz[c].at[pl.ds(0, half)], sem.at[c])

        def z_to_out(c):
            settle_z(c, z_r)

            def total(sources):
                out = rz[c][sources[0]].astype(f32)
                for s in sources[1:]:
                    out = out + rz[c][s].astype(f32)
                return out

            if c == 0:
                gb_r[...] = total(range(half))
            elif c < 3:
                for odd in range(2):
                    first = (2 * odd + c - 1) * quarter
                    gi_r[:, first : first + quarter] = total([s for s in range(n) if s % half % 2 == odd])
            else:
                go_r[...] = total(range(n))

        for c in range(nc):
            c_to_p(c)
        fetch_h1(0).start()

        own_do.wait()
        settle(do.at[pl.ds(0, (n - 1) * size)], d_r.at[0])
        for i, (src, dst) in enumerate(arriving):
            settle(dst, loc.at[6 + nc + i])

        @pl.when(away)
        def _():
            send(res_r, reso_r, (x_s, x_r), 0, at.swap())

        @pl.when(jnp.logical_not(away))
        def _():
            pltpu.make_async_copy(res_r, reso_r, loc.at[1]).start()

        settle(o_v.at[:, pl.ds(0, n * width)], loc.at[5])
        pick = (
            lax.broadcasted_iota(jnp.int32, (8, width), 1) // HEAD_DIM
            == lax.broadcasted_iota(jnp.int32, (8, width), 0)
        ).astype(f32)

        def prepare(i, carry):
            rows = block_rows(i, size)
            product = do[rows, :].astype(f32) * o_v[:, block_rows(i, width)].astype(f32)
            delta[:, rows] = lax.dot_general(
                pick, product, NT, preferred_element_type=f32, precision=lax.Precision.HIGHEST
            )
            dqa[rows, :] = jnp.zeros((size, width), f32)
            return carry

        lax.fori_loop(0, n, prepare, 0)
        gacc[...] = jnp.zeros_like(gacc)
        sm[...] = jnp.zeros_like(sm)
        sm[4:12, :] = gsm_r[...]

        def pair(i, j, diagonal):
            rows, at_k = block_rows(i, size), block_rows(j, size)
            kk, vv = k_r[at_k, :], v_r[at_k, :]
            qs, dd = q_r[rows, :] * jnp.asarray(scale, bf16), do[rows, :]
            dq = dk = dv = None
            for h in range(heads):
                qh, dh_, kh = only_head(qs, h), only_head(dd, h), only_head(kk, h)
                p = jnp.exp(row_dot(kk, qh) - lse_r[h : h + 1, rows])
                if diagonal:
                    k_pos = lax.broadcasted_iota(jnp.int32, (size, size), 0)
                    q_pos = lax.broadcasted_iota(jnp.int32, (size, size), 1)
                    p = jnp.where(k_pos <= q_pos, p, 0.0)
                dp = row_dot(vv, dh_)
                ds = (p * (dp - delta[h : h + 1, rows])).astype(bf16)
                one, two, three = dot(p.astype(bf16), dh_), dot(ds, qh), col_dot(ds, kh)
                dv = one if dv is None else dv + one
                dk = two if dk is None else dk + two
                dq = three if dq is None else dq + three
            dva[...] += dv
            dka[...] += dk
            dqa[rows, :] += dq

        def owner(j):
            return j // half, lax.rem(j, half)

        def finish_block(j):
            core_j, low_j = owner(j)

            @pl.when(core_j == core)
            def _():
                settle(rd.at[0], y_r.at[low_j])

                def add(t, carry):
                    rows = pl.ds(pl.multiple_of(t * 128, 128), 128)
                    rd[low_j, rows, :] = (pf[rows, :] + rd[low_j, rows, :].astype(f32)).astype(bf16)
                    return carry

                lax.fori_loop(0, size // 128, add, 0)

                @pl.when(low_j != low)
                def _():
                    slot = lax.rem(low_j - low + half, half) - 1
                    send(rd.at[low_j], rzd.at[slot], (e_s, e_r), 0, (at.team * half + low_j, at.k))

        def column(j, carry):
            fetch_h1(j).wait()

            @pl.when(j + 1 < n)
            def _():
                fetch_h1(j + 1).start()

            dka[...] = jnp.zeros_like(dka)
            dva[...] = jnp.zeros_like(dva)
            pair(j, j, True)

            def inner(i, c2):
                pair(i, j, False)
                return c2

            lax.fori_loop(j + 1, n, inner, 0)
            dqb = (dqa[block_rows(j, size), :] * scale).astype(bf16)
            dkb, dvb = dka[...].astype(bf16), dva[...].astype(bf16)
            dqkv[:, 0:width] = dqb
            dqkv[:, width : 2 * width] = dkb
            dqkv[:, 2 * width : 3 * width] = dvb
            mine = block_rows(rank, width)
            sm[2:3, mine] += jnp.sum(dqb.astype(f32), axis=0, keepdims=True)
            sm[3:4, mine] += jnp.sum(dvb.astype(f32), axis=0, keepdims=True)

            @pl.when(j > 0)
            def _():
                finish_block(j - 1)

            core_j, low_j = owner(j)

            def project(t, c2):
                rows = pl.ds(pl.multiple_of(t * PIECE, PIECE), PIECE)
                part = row_dot(dqkv[rows, :], wq_r[...])

                @pl.when(core_j == core)
                def _():
                    pf[rows, :] = part

                @pl.when(core_j != core)
                def _():
                    sd[low_j, rows, :] = part.astype(bf16)

                    @pl.when(j == n - 1)
                    def _():
                        send(sd.at[low_j, rows], rd.at[low_j, rows], (yl_s, yl_r), t, at.partner())

                return c2

            lax.fori_loop(0, size // PIECE, project, 0)

            @pl.when(jnp.logical_and(core_j != core, j < n - 1))
            def _():
                send(sd.at[low_j], rd.at[low_j], (y_s, y_r), low_j, at.partner())

            slot = lax.rem(j, 2)
            for t in range(3):
                cols = slice(t * width, (t + 1) * width)
                gacc[:, cols] += col_dot(hb[block_rows(slot, size), :], dqkv[:, cols])
            for c in range(nc - 1):

                @pl.when(j == min(c, n - 2))
                def _(c=c):
                    p_to_z(c)

            return carry

        lax.fori_loop(0, n, column, 0)
        gqb[...] = gacc[...].astype(bf16)
        for step in range(1, planes):
            other = at.beside(step)
            for s in range(n):
                send(
                    gqb.at[block_rows(s * m + 2 * other, rq, 2)],
                    rqp.at[block_rows((step - 1) * n + s, 2 * rq)],
                    (m_s, m_r), 0, (at.s, 2 * other + core),
                )
        pieces = size // PIECE
        last = half - 1
        owner_last = (at.team * half + last, at.k)

        def pair_piece(rows):
            rd[last, rows, :] = (pf[rows, :] + rd[last, rows, :].astype(f32)).astype(bf16)

        @pl.when(jnp.logical_and(core == 1, low != last))
        def _():
            def pass_on(t, carry):
                rows = pl.ds(pl.multiple_of(t * PIECE, PIECE), PIECE)
                settle(rd.at[last, rows], yl_r.at[t])
                pair_piece(rows)
                send(rd.at[last, rows], rzd.at[last - low - 1, rows], (el_s, el_r), t, owner_last)
                return carry

            lax.fori_loop(0, pieces, pass_on, 0)

        own_dres.wait()
        fetch_tb.wait()
        if half > 1:

            @pl.when(rank != n - 1)
            def _():
                settle(rzd, e_r.at[0])

        def norm_step(t, carry):
            sum_g, sum_s = carry
            rows = pl.ds(pl.multiple_of(t * PIECE, PIECE), PIECE)

            @pl.when(rank == n - 1)
            def _():
                settle(rd.at[last, rows], yl_r.at[t])
                pair_piece(rows)
                if half > 1:
                    settle(rzd.at[:, rows], el_r.at[t])

            dh1 = rd[low, rows, :].astype(f32)
            for slot in range(half - 1):
                dh1 = dh1 + rzd[slot, rows, :].astype(f32)
            normed, inv = normalize(tb_v[rows, :].astype(f32))
            grad = gt_r[rows, :] + norm_back(dh1 * sv_r[0:1, :], normed, inv)
            gt_r[rows, :] = grad
            sg[rows, :] = grad.astype(bf16)

            @pl.when(away)
            def _():
                send(sg.at[rows], rg.at[rows], (x_s, x_r), 1, at.swap())

            return (
                sum_g + jnp.sum(dh1 * normed, axis=0, keepdims=True),
                sum_s + jnp.sum(dh1, axis=0, keepdims=True),
            )

        zero = jnp.zeros((1, d), f32)
        sum_g, sum_s = lax.fori_loop(0, pieces, norm_step, (zero, zero))
        sm[0:1, :] = sum_g
        sm[1:2, :] = sum_s

        settle(rqp, m_r.at[0])

        def add_q(s, carry):
            rows = block_rows(s * m + 2 * at.plane, rq, 2)
            total = gqb[rows, :].astype(f32)
            for step in range(1, planes):
                total = total + rqp[block_rows((step - 1) * n + s, 2 * rq), :].astype(f32)
            gqb[rows, :] = total.astype(bf16)
            return carry

        lax.fori_loop(0, n, add_q, 0)
        for l in range(half):
            row = ((1 - at.team) * half + l) * m + 2 * at.plane
            send(gqb.at[block_rows(row, rq, 2)], rqh.at[block_rows(l, 2 * rq)], (m_s, m_r), 2, at.across())

        p_to_z(nc - 1)
        send(sm, smc, (m_s, m_r), 1, at.partner())
        settle(rqh, m_r.at[2])
        for l in range(half):
            rows = block_rows((at.team * half + l) * m + 2 * at.plane, rq, 2)
            gqb[rows, :] = (
                gqb[rows, :].astype(f32) + rqh[block_rows(l, 2 * rq), :].astype(f32)
            ).astype(bf16)

        def member_rows(r):
            return block_rows((at.team * half + lax.rem(r, half)) * m + 2 * at.plane + r // half, rq)

        for step in range(1, n):
            other = lax.rem(rank + step, n)
            send(gqb.at[member_rows(other)], gq_r.at[rank], (m_s, m_r), 4, at.member(other))
        pltpu.make_async_copy(gqb.at[member_rows(rank)], gq_r.at[rank], loc.at[0]).start()

        settle(smc, m_r.at[1])
        settle(smc, m_s.at[1])
        sm[...] = sm[...] + smc[...]
        for step in range(1, planes):
            send(sm, smp.at[step - 1], (m_s, m_r), 3, (at.s, 2 * at.beside(step) + core))
        for c in range(nc):
            z_to_out(c)
        settle(smp, m_r.at[3])
        settle(smp, m_s.at[3])
        total = sm[...]
        for step in range(1, planes):
            total = total + smp[step - 1]
        sm[...] = total
        for step in range(1, n):
            s = at.along(step)
            send(sm.at[:, block_rows(s, lanes_s)], smz.at[step - 1], (m_s, m_r), 5, (s, at.k))
        settle(smz, m_r.at[5])
        total = sm[:, block_rows(at.s, lanes_s)]
        for step in range(1, n):
            total = total + smz[step - 1]
        small_r[...] = total

        settle(gq_r.at[pl.ds(0, n - 1)], m_r.at[4])
        settle(gq_r.at[0], loc.at[0])
        for r in range(n):
            for part in range(3):
                first = part * d + r * width
                gqo_r[:, first : first + width] = gq_r[r, :, part * width : (part + 1) * width].astype(f32)

        @pl.when(away)
        def _():
            settle(rg, x_r.at[1])
            settle(rg, x_s.at[1])
            settle(reso_r, x_r.at[0])
            settle(reso_r, x_s.at[0])

        @pl.when(jnp.logical_not(away))
        def _():
            settle(reso_r, loc.at[1])

        settle(do.at[pl.ds(0, (n - 1) * size)], d_s.at[0])
        for c in range(nc):
            settle(rc[c], c_s.at[c])
            settle(rp[c], p_s.at[c])
            settle_z(c, z_s)
        for l in range(half - 1):
            settle(rd.at[0], y_s.at[l])

        @pl.when(core == 1)
        def _():
            settle(rd.at[0], y_s.at[last])

        @pl.when(core == 0)
        def _():
            for t in range(pieces):
                settle(rd.at[0, pl.ds(0, PIECE)], yl_s.at[t])

        passes = jnp.logical_and(core == 1, low != last)

        @pl.when(passes)
        def _():
            for t in range(pieces):
                settle(rd.at[0, pl.ds(0, PIECE)], el_s.at[t])

        if half > 2:

            @pl.when(passes)
            def _():
                settle(rzd.at[pl.ds(0, half - 2)], e_s.at[0])

        if half > 1:

            @pl.when(jnp.logical_not(passes))
            def _():
                settle(rzd, e_s.at[0])

        settle(rqp, m_s.at[0])
        settle(smz, m_s.at[5])
        settle(rqh, m_s.at[2])
        settle(gq_r.at[pl.ds(0, n - 1)], m_s.at[4])

    def sds(shape, dtype=bf16):
        return jax.ShapeDtypeStruct(shape, dtype)

    sems = pltpu.SemaphoreType.DMA
    return pl.pallas_call(
        kernel,
        name="attend_back_reduce",
        out_shape=(
            sds((size, d)),
            sds((size, d), f32),
            sds((size, d)),
            sds((rq, 3 * d), f32),
            sds(gwo.shape[3:], f32),
            sds((gwi.shape[3], 2 * gwi.shape[4]), f32),
            sds(gwb.shape[3:], f32),
            sds((16, lanes_s), f32),
        ),
        in_specs=[HB] * 7 + [VM, HB, HB, HB] + [VM] * 2 + [HB] * 3,
        out_specs=(HB, VM, HB) + (VM,) * 5,
        scratch_shapes=[
            pltpu.VMEM((length, width), bf16),
            pltpu.VMEM((8, length), f32),
            pltpu.VMEM((length, width), f32),
            pltpu.VMEM((size, width), f32),
            pltpu.VMEM((size, width), f32),
            pltpu.VMEM((size, 3 * width), bf16),
            pltpu.VMEM((d, 3 * width), f32),
            pltpu.VMEM(((planes - 1) * n * 2 * rq, 3 * width), bf16),
            pltpu.VMEM((half * 2 * rq, 3 * width), bf16),
            pltpu.VMEM((size, d), f32),
            pltpu.VMEM((half, size, d), bf16),
            pltpu.VMEM((half, size, d), bf16),
            pltpu.VMEM((max(half - 1, 1), size, d), bf16),
            pltpu.VMEM((16, d), f32),
            pltpu.VMEM((n - 1, 16, lanes_s), f32),
            pltpu.VMEM((planes - 1, 16, d), f32),
            pltpu.VMEM((16, d), f32),
        ]
        + [
            pltpu.VMEM((d, 3 * width), bf16),
            pltpu.VMEM((2 * size, d), bf16),
            pltpu.VMEM((size, d), bf16),
            pltpu.VMEM((size, d), bf16),
            pltpu.VMEM((size, d), bf16),
            pltpu.VMEM((length, width), bf16),
            pltpu.VMEM((length, width), bf16),
            pltpu.VMEM((length, width), bf16),
            pltpu.VMEM((d, 3 * width), bf16),
            pltpu.VMEM((n, rq, 3 * width), bf16),
        ]
        + [pltpu.VMEM((count, planes, rows, cols), bf16) for count, rows, cols in parts] * 2
        + [pltpu.VMEM((planes - 1, *part), bf16) for part in parts]
        + [pltpu.VMEM(part, bf16) for part in parts]
        + [
            sems((1,)), sems((1,)),
            sems((2,)), sems((2,)),
            sems((half,)), sems((half,)),
            sems((1,)), sems((1,)),
            sems((nc,)), sems((nc,)),
            sems((nc,)), sems((nc,)),
            sems((nc,)), sems((nc,)),
            sems((6,)), sems((6,)),
            sems((size // PIECE,)), sems((size // PIECE,)),
            sems((size // PIECE,)), sems((size // PIECE,)),
            sems((10 + nc,)),
        ],
        compiler_params=pltpu.CompilerParams(
            collective_id=1, has_side_effects=True, vmem_limit_bytes=67043328
        ),
        cost_estimate=pl.CostEstimate(
            flops=12 * length * d * width + 5 * length * length * d // n, bytes_accessed=80 << 20, transcendentals=0
        ),
    )(res, dat, dres, q, k, v, o, lse, h1, wq, tb, sv, gsm, gwo, gwi, gwb)


def hidden_forward_call(att, tokens, wo, wi, wb, sv, bias):
    size, d = att.shape[1:]
    rows, hidden = 2 * size, wi.shape[1]
    some, columns = 512, hidden // 4
    blocks = size // some

    def kernel(
        att_h, tok_h, wo_h, wi_h, wb_h, sv_r, bias_r, norm_r, inv_r, h2_h, act_h, slope_h, own_r, other_r,
        att_v, tok_v, wo_v, wi_v, wb_v, h2_v, act_v, slope_v, loc,
    ):
        loads = ((att_h, att_v), (wo_h, wo_v), (tok_h, tok_v), (wi_h, wi_v), (wb_h, wb_v))
        for i, (src, dst) in enumerate(loads):
            pltpu.make_async_copy(src, dst, loc.at[i]).start()
        for i in range(3):
            settle(loads[i][1], loc.at[i])

        def first(t, carry):
            b = t // blocks
            part = pl.ds(pl.multiple_of(lax.rem(t, blocks) * some, some), some)
            resid = tok_v[b, part, :].astype(f32) + dot(att_v[b, part, :], wo_v[...]) + sv_r[4:5, :]

            normed, inv = normalize(resid)

            @pl.when(b == 0)
            def _():
                own_r[part, :] = resid + sv_r[7:8, :]
                norm_r[part, :] = normed
                inv_r[part, :] = jnp.broadcast_to(inv, (some, LANES))

            h2_v[pl.ds(pl.multiple_of(t * some, some), some), :] = (normed * sv_r[5:6, :] + sv_r[6:7, :]).astype(bf16)
            return carry

        lax.fori_loop(0, rows // some, first, 0)
        pltpu.make_async_copy(h2_v, h2_h, loc.at[5]).start()
        settle(wi_v, loc.at[3])

        def second(t, carry):
            part = pl.ds(pl.multiple_of(t * some, some), some)
            h = h2_v[part, :]
            for c in range(4):
                cols = slice(c * columns, (c + 1) * columns)
                act, slope = gelu_pair(dot(h, wi_v[:, cols]) + bias_r[:, cols])
                act_v[part, cols] = act.astype(bf16)
                slope_v[part, cols] = slope
            pltpu.make_async_copy(act_v.at[part], act_h.at[part], loc.at[6]).start()
            pltpu.make_async_copy(slope_v.at[part], slope_h.at[part], loc.at[7]).start()

            @pl.when(t == 0)
            def _():
                settle(wb_v, loc.at[4])

            out = dot(act_v[part, :], wb_v[...])

            @pl.when(t < blocks)
            def _():
                own_r[part, :] += out

            @pl.when(t >= blocks)
            def _():
                other_r[pl.ds(pl.multiple_of(t * some - size, some), some), :] = out.astype(bf16)

            return carry

        lax.fori_loop(0, rows // some, second, 0)
        settle(h2_v, loc.at[5])
        settle(act_v, loc.at[6])
        settle(slope_v, loc.at[7])

    def sds(shape, dtype=bf16):
        return jax.ShapeDtypeStruct(shape, dtype)

    return pl.pallas_call(
        kernel,
        name="hidden_forward",
        out_shape=(
            sds((size, d), f32), sds((size, LANES), f32), sds((rows, d)), sds((rows, hidden)), sds((rows, hidden), f32),
            sds((size, d), f32), sds((size, d)),
        ),
        in_specs=[HB] * 5 + [VM] * 2,
        out_specs=(VM,) * 2 + (HB,) * 3 + (VM,) * 2,
        scratch_shapes=[
            pltpu.VMEM(att.shape, bf16),
            pltpu.VMEM(tokens.shape, bf16),
            pltpu.VMEM(wo.shape, bf16),
            pltpu.VMEM(wi.shape, bf16),
            pltpu.VMEM(wb.shape, bf16),
            pltpu.VMEM((rows, d), bf16),
            pltpu.VMEM((rows, hidden), bf16),
            pltpu.VMEM((rows, hidden), f32),
            pltpu.SemaphoreType.DMA((8,)),
        ],
        compiler_params=pltpu.CompilerParams(vmem_limit_bytes=56 << 20),
        cost_estimate=pl.CostEstimate(
            flops=2 * rows * d * (d + 2 * hidden), bytes_accessed=40 << 20, transcendentals=rows * hidden
        ),
    )(att, tokens, wo, wi, wb, sv, bias)


def hidden_back_call(slopes, cot, wb, wi):
    rows, hidden = slopes.shape
    d = cot.shape[1]
    some, columns = 512, hidden // 4

    def kernel(slope_h, cot_h, wb_h, wi_h, dp_h, own_r, other_r, gb_r, slope_v, cot_v, wb_v, wi_v, dp_v, loc):
        steps = rows // some
        for i, (src, dst) in enumerate(((cot_h, cot_v), (wb_h, wb_v), (wi_h, wi_v))):
            pltpu.make_async_copy(src, dst, loc.at[i]).start()
        for t in range(steps):
            part = pl.ds(t * some, some)
            pltpu.make_async_copy(slope_h.at[part], slope_v.at[part], loc.at[5 + t]).start()
        gb_r[...] = jnp.zeros_like(gb_r)
        settle(cot_v, loc.at[0])
        settle(wb_v, loc.at[1])

        def body(t, carry):
            part = pl.ds(pl.multiple_of(t * some, some), some)
            settle(slope_v.at[part], loc.at[5 + t])
            c_rows = cot_v[part, :]
            for c in range(4):
                cols = slice(c * columns, (c + 1) * columns)
                grad = (row_dot(c_rows, wb_v[cols, :]) * slope_v[part, cols]).astype(bf16)
                dp_v[part, cols] = grad
                gb_r[:, cols] += jnp.sum(grad.astype(f32), axis=0, keepdims=True)
            pltpu.make_async_copy(dp_v.at[part], dp_h.at[part], loc.at[4]).start()

            @pl.when(t == 0)
            def _():
                settle(wi_v, loc.at[2])

            back = row_dot(dp_v[part, :], wi_v[...])

            @pl.when(t < steps // 2)
            def _():
                own_r[part, :] = back

            @pl.when(t >= steps // 2)
            def _():
                other_r[pl.ds(pl.multiple_of(t * some - rows // 2, some), some), :] = back.astype(bf16)

            return carry

        lax.fori_loop(0, steps, body, 0)
        settle(dp_v, loc.at[4])

    def sds(shape, dtype=bf16):
        return jax.ShapeDtypeStruct(shape, dtype)

    return pl.pallas_call(
        kernel,
        name="hidden_back",
        out_shape=(sds(slopes.shape), sds((rows // 2, d), f32), sds((rows // 2, d)), sds((1, hidden), f32)),
        in_specs=[HB] * 4,
        out_specs=(HB,) + (VM,) * 3,
        scratch_shapes=[
            pltpu.VMEM(slopes.shape, f32),
            pltpu.VMEM(cot.shape, bf16),
            pltpu.VMEM(wb.shape, bf16),
            pltpu.VMEM(wi.shape, bf16),
            pltpu.VMEM(slopes.shape, bf16),
            pltpu.SemaphoreType.DMA((5 + rows // some,)),
        ],
        compiler_params=pltpu.CompilerParams(vmem_limit_bytes=56 << 20),
        cost_estimate=pl.CostEstimate(flops=4 * rows * d * hidden, bytes_accessed=28 << 20, transcendentals=0),
    )(slopes, cot, wb, wi)


def solution(mesh):
    n, m = mesh.shape["seq"], mesh.shape["shard"]
    nd = n * m
    every = ("seq", "shard")

    def per_device(
        tokens, ln1_gain, ln1_bias, w_qkv, bias_query, bias_value, w_out, bias_out,
        ln2_gain, ln2_bias, w_in, bias_in, w_back, bias_back, cotangent,
    ):
        d = tokens.shape[2]
        width = d // n
        index = lax.axis_index("seq") * m + lax.axis_index("shard")
        pack = small_pack(
            index,
            [ln1_gain, ln1_bias, bias_query, bias_value, bias_out, ln2_gain, ln2_bias, bias_back, bias_in],
        )
        rq = w_qkv.shape[0]
        ff = w_in.shape[1]
        rq = w_qkv.shape[0]
        (full_out, full_in, full_back, q, k, v, o, lse, att_two, h1, wq, tb, cot_own, sv) = forward_call(
            n, m, tokens[0], cotangent[0], w_qkv, pack, w_out, w_in, w_back
        )
        full_out = full_out.reshape(d, d)
        half_in = full_in.reshape(d, ff // 2)
        half_back = full_back.reshape(ff // 2, d)
        odd = lax.rem(lax.rem(lax.axis_index("seq"), n // 2), 2)
        per = d // nd
        parts = bias_in.shape[0] // per
        half_bin = lax.dynamic_slice_in_dim(sv[8 : 8 + parts], odd * (d // 2), d // 2, 1)
        half_bin = half_bin.reshape(parts, nd // 2, per).transpose(1, 0, 2).reshape(-1)
        g_two = sv[5]

        def to_neighbour(values):
            pairs = []
            for s in range(n):
                there = s // 2 * 2 + 1 - s % 2
                pairs += [(s * m + k, there * m + k) for k in range(m)]
            return lax.ppermute(values.astype(bf16), every, pairs).astype(f32)

        size = tokens.shape[1]
        cot_two = jnp.concatenate([cot_own, to_neighbour(cot_own).astype(bf16)])
        normed2, scale2, h_two, act, slopes, own_out, leaves = hidden_forward_call(
            att_two, tb, full_out, half_in, half_back, sv, half_bin.reshape(1, -1)
        )
        others_out = to_neighbour(leaves)
        slopes, leaves = lax.optimization_barrier((slopes, leaves))
        d_pre, d_h2_own, leaves, g_b_in = hidden_back_call(slopes, cot_two, half_back, half_in)
        others_d = to_neighbour(leaves)
        act, d_pre, leaves = lax.optimization_barrier((act, d_pre, leaves))
        g_w_back = col_dot(act, cot_two).astype(bf16)
        g_w_in = col_dot(h_two, d_pre).astype(bf16)

        scale2 = scale2[:, :1]
        att_tok, cot_f = att_two[0], cot_own.astype(f32)
        result = (own_out + others_out).astype(bf16)
        g_b_back = jnp.sum(cot_f, axis=0)
        d_h2 = d_h2_own + others_d
        g_g2 = jnp.sum(d_h2 * normed2, axis=0)
        g_s2 = jnp.sum(d_h2, axis=0)
        d_resid = cot_f + norm_back(d_h2 * g_two, normed2, scale2)
        d_resid_b = d_resid.astype(bf16)
        g_w_out = col_dot(att_tok, d_resid_b).astype(bf16)
        g_b_out = jnp.sum(d_resid, axis=0)
        d_att_tok = row_dot(d_resid_b, full_out).astype(bf16)
        bin_rows = g_b_in.reshape(nd // 2, parts, per).transpose(1, 0, 2).reshape(parts, d // 2)
        bin_rows = jnp.where(
            lax.broadcasted_iota(jnp.int32, (parts, d), 1) // (d // 2) == odd, jnp.tile(bin_rows, (1, 2)), 0.0
        )
        gsm = jnp.concatenate([jnp.stack([g_b_out, g_g2, g_s2, g_b_back]), bin_rows])

        (own_result, g_tok, swapped, g_qkv, go, gi, gb, small) = backward_call(
            n, m, result, d_att_tok, d_resid, q, k, v, o, lse, h1, wq, tb, sv, gsm,
            g_w_out.reshape(n, m // 2, 2, d // nd, d),
            g_w_in.reshape(n, m // 2, 2, d // nd, ff // 2),
            g_w_back.reshape(n // 2, m // 2, 2, ff // nd, d),
        )
        away = lax.rem(lax.axis_index("shard"), 2) != lax.axis_index("seq") // (n // 2)
        g_tok = jnp.where(away, swapped.astype(f32), g_tok)
        mine = lax.dynamic_slice_in_dim(small, lax.axis_index("shard") * per, per, 1)
        return (
            own_result[None], g_tok[None], mine[0], mine[1], g_qkv, mine[2], mine[3], go, mine[4],
            mine[5], mine[6], gi, mine[8 : 8 + parts].reshape(-1), gb, mine[7],
        )

    whole, vector, matrix = P("shard", "seq", None), P(every), P(every, None)
    return jax.shard_map(
        per_device,
        mesh=mesh,
        in_specs=(
            whole, vector, vector, matrix, vector, vector, matrix, vector, vector, vector, matrix, vector,
            matrix, vector, whole,
        ),
        out_specs=(
            whole, whole, vector, vector, matrix, vector, vector, matrix, vector, vector, vector, matrix,
            vector, matrix, vector,
        ),
        check_vma=False,
    )
```

```python
import math

import jax
import jax.numpy as jnp
from jax import lax
from jax.experimental import pallas as pl
from jax.experimental.pallas import tpu as pltpu
from jax.sharding import PartitionSpec as P

HEAD_DIM = 64
PUMPS = ((('b', 0), ('b', 1)), (('z', 2),), ())
TAIL = (('a', 2), ('b', 2))
LANES = 128
PIECE = 128
MESH = pl.DeviceIdType.MESH
NT = (((1,), (1,)), ((), ()))
TN = (((0,), (0,)), ((), ()))
f32 = jnp.float32
bf16 = jnp.bfloat16

norm_eps = 1e-05
gelu_c = math.sqrt(2.0 / math.pi)
scale = 1.0 / math.sqrt(HEAD_DIM)

VM = pl.BlockSpec(memory_space=pltpu.VMEM)
HB = pl.BlockSpec(memory_space=pl.ANY)


def dot(a, b):
    return jnp.dot(a, b, preferred_element_type=f32)


def row_dot(a, b):
    return lax.dot_general(a, b, NT, preferred_element_type=f32)


def col_dot(a, b):
    return lax.dot_general(a, b, TN, preferred_element_type=f32)


def normalize(values):
    mean_row = jnp.mean(values, axis=-1, keepdims=True)
    centred = values - mean_row
    var_row = jnp.mean(centred * centred, axis=-1, keepdims=True)
    scale_row = lax.rsqrt(var_row + norm_eps)
    return (centred * scale_row, scale_row)


def norm_back(dnormed, normed, scale_row):
    return scale_row * (
        dnormed
        - jnp.mean(dnormed, axis=-1, keepdims=True)
        - normed * jnp.mean(dnormed * normed, axis=-1, keepdims=True)
    )


def gelu_pair(inputs):
    inner = gelu_c * (inputs + 0.044715 * inputs * inputs * inputs)
    tanh_val = jnp.tanh(inner)
    value = 0.5 * inputs * (1.0 + tanh_val)
    slope = 0.5 * (1.0 + tanh_val) + 0.5 * inputs * (1.0 - tanh_val * tanh_val) * gelu_c * (
        1.0 + 3.0 * 0.044715 * inputs * inputs
    )
    return (value, slope)


def block_rows(index, size, count=1):
    return pl.ds(pl.multiple_of(index * size, size), size * count)


def head_lanes(shape, head):
    return lax.broadcasted_iota(jnp.int32, shape, len(shape) - 1) // HEAD_DIM == head


def only_head(values, head):
    return jnp.where(head_lanes(values.shape, head), values, jnp.zeros_like(values))


def spread_heads(columns, rows, width):
    out = None
    for head in range(width // HEAD_DIM):
        one = jnp.broadcast_to(columns[:, head : head + 1], (rows, width))
        out = one if out is None else jnp.where(head_lanes((rows, width), head), one, out)
    return out


class Place:
    def __init__(self, n, m):
        self.n, self.m, self.half, self.planes = n, m, n // 2, m // 2
        self.s, self.k = lax.axis_index("seq"), lax.axis_index("shard")
        self.core, self.plane = lax.rem(self.k, 2), self.k // 2
        self.team, self.low = self.s // self.half, lax.rem(self.s, self.half)
        self.rank = self.low + self.half * self.core
        self.index = self.s * m + self.k
        self.odd = lax.rem(self.low, 2)

    def member(self, rank):
        return (self.team * self.half + lax.rem(rank, self.half), 2 * self.plane + rank // self.half)

    def across(self):
        return (lax.rem(self.s + self.half, self.n), self.k)

    def swap(self):
        return (lax.rem(self.s + self.half, self.n), 2 * self.plane + 1 - self.core)

    def partner(self):
        return (self.s, 2 * self.plane + 1 - self.core)

    def along(self, step):
        return lax.rem(self.s + step, self.n)

    def neighbour(self):
        return (self.team * self.half + self.low + 1 - 2 * lax.rem(self.low, 2), self.k)

    def beside(self, step):
        return lax.rem(self.plane + step, self.planes)

    def near_plane(self):
        return self.plane + 1 - 2 * lax.rem(self.plane, 2)

    def far_plane(self, step):
        return 2 * lax.rem(self.plane // 2 + step, self.planes // 2) + lax.rem(self.plane, 2)

    def greet(self):
        barrier = pltpu.get_barrier_semaphore()
        count = 0

        def signal(device):
            pl.semaphore_signal(barrier, inc=1, device_id=device, device_id_type=MESH)

        for step in range(1, self.n):
            signal((self.along(step), self.k))
            count += 1
        for step in range(self.n):
            signal((self.along(step), 2 * self.plane + 1 - self.core))
            count += 1
        for step in range(1, self.planes):
            signal((self.s, 2 * self.beside(step) + self.core))
            count += 1
        pl.semaphore_wait(barrier, count)


def send(src, dst, sems, at, device):
    pltpu.make_async_remote_copy(
        src_ref=src,
        dst_ref=dst,
        send_sem=sems[0].at[at],
        recv_sem=sems[1].at[at],
        device_id=device,
        device_id_type=MESH,
    ).start()


def settle(view, sem):
    pltpu.make_async_copy(view, view, sem).wait()


def attend_row(i, q_ref, k_ref, v_ref, o_ref, lse_ref, qm, m_s, l_s, acc, size):
    width = q_ref.shape[1]
    heads = width // HEAD_DIM
    rows = block_rows(i, size)
    q = q_ref[rows, :] * jnp.asarray(scale, bf16)
    for h in range(heads):
        qm[h] = only_head(q, h)

    def step(j, diagonal):
        at = block_rows(j, size)
        k = k_ref[at, :]
        v = v_ref[at, :]
        old = m_s[...]
        tops, sums, total = [], [], None
        for h in range(heads):
            s = row_dot(k, qm[h])
            if diagonal:
                k_pos = lax.broadcasted_iota(jnp.int32, (size, size), 0)
                q_pos = lax.broadcasted_iota(jnp.int32, (size, size), 1)
                s = jnp.where(k_pos <= q_pos, s, -1e30)
            top = jnp.max(s, axis=0, keepdims=True)
            if not diagonal:
                top = jnp.maximum(old[h : h + 1], top)
            p = jnp.exp(s - top)
            tops.append(top)
            sums.append(jnp.sum(p, axis=0, keepdims=True))
            part = col_dot(p.astype(bf16), only_head(v, h))
            total = part if total is None else total + part
        rest = [jnp.zeros((8 - heads, size), f32)] if heads < 8 else []
        top = jnp.concatenate(tops + rest, 0)
        add = jnp.concatenate(sums + rest, 0)
        if diagonal:
            l_s[...] = add
            acc[...] = total
        else:
            fade = jnp.exp(old - top)
            l_s[...] = l_s[...] * fade + add
            acc[...] = acc[...] * spread_heads(jnp.transpose(fade), size, width) + total
        m_s[...] = top

    step(i, True)

    def body(j, carry):
        step(j, False)
        return carry

    lax.fori_loop(0, i, body, 0)
    l = l_s[...]
    lse_ref[:, rows] = m_s[...] + jnp.log(l)
    o_ref[rows, :] = (acc[...] * spread_heads(jnp.transpose(1.0 / l), size, width)).astype(bf16)


def forward_call(n, m, tok, cot, wq_s, sm_s, wo_s, wi_s, wb_s):
    size, d = tok.shape
    nd = n * m
    length = n * size
    width = d // n
    half = n // 2
    rq = wq_s.shape[0]
    ff_half = wi_s.shape[1] // 2
    cells = (n, n, half)
    nc = len(cells)

    def kernel(
        tok_r, cot_r, wqs_r, sms_r, wos_r, wis_r, wbs_r,
        wo_r, wi_r, wb_r, q_r, k_r, v_r, o_r, lse_r, att_r, h1_r, wq_r, tb_r, cb_r, sv_r,
        q_v, k_v, v_v, h1_v, wq_v, tokf, sma, qm, m_s, l_s, acc, vec,
        t_send, t_recv, w_send, w_recv, a_send, a_recv, z_send, z_recv,
        lo_send, lo_recv, hi_send, hi_recv, b_send, b_recv, c_send, c_recv, loc,
    ):
        at = Place(n, m)
        planes, rank, core = at.planes, at.rank, at.core
        fulls, shards = (wo_r, wi_r, wb_r), (wos_r, wis_r, wbs_r)
        ts, ws, zs, cs = (t_send, t_recv), (w_send, w_recv), (z_send, z_recv), (c_send, c_recv)
        los, his, bs = (lo_send, lo_recv), (hi_send, hi_recv), (b_send, b_recv)
        rows_p = planes // 2
        near = 2 * at.near_plane() + core
        far = [2 * at.far_plane(step) + core for step in range(1, rows_p)]
        at.greet()
        away = core != at.team

        own = [(at.s, at.plane, core), (at.s, at.plane, core), (at.low, at.plane, core)]
        near_p = at.near_plane()
        far_p = [at.far_plane(step) for step in range(1, rows_p)]

        def half_of(odd):
            return wis_r.at[:, pl.ds(pl.multiple_of(odd * ff_half, ff_half), ff_half)]

        def start_z(c):
            dst = fulls[c].at[own[c]]
            if c < 2:
                for step in range(1, n):
                    s = at.along(step)
                    src = shards[c] if c == 0 else half_of(lax.rem(lax.rem(s, half), 2))
                    send(src, dst, zs, c, (s, at.k))
                src = shards[c] if c == 0 else half_of(at.odd)
                pltpu.make_async_copy(src, dst, loc.at[4 + c]).start()
                return
            for team in range(2):
                for pair in range(half // 2):
                    s = team * half + 2 * pair + at.team

                    @pl.when(s != at.s)
                    def _(s=s):
                        send(shards[c], dst, zs, c, (s, at.k))

            @pl.when(at.odd == at.team)
            def _():
                pltpu.make_async_copy(shards[c], dst, loc.at[4 + c]).start()

        def settle_z(c, sem):
            if c < 2:
                settle(fulls[c].at[pl.ds(0, n - 1), 0, 0], sem.at[c])
                return

            @pl.when(at.odd == at.team)
            def _():
                settle(fulls[c].at[pl.ds(0, half - 1), 0, 0], sem.at[c])

            @pl.when(at.odd != at.team)
            def _():
                settle(fulls[c].at[pl.ds(0, half), 0, 0], sem.at[c])

        def z_to_a(c):
            if c < 2:
                settle(fulls[c].at[own[c]], loc.at[4 + c])
            else:

                @pl.when(at.odd == at.team)
                def _():
                    settle(fulls[c].at[own[c]], loc.at[4 + c])

            settle_z(c, z_recv)
            part = fulls[c].at[:, at.plane, core]
            send(part, part, los, c, (at.s, near))
            for there in far:
                send(part, part, his, c, (at.s, there))

        def settle_far(c, sem):
            if far:
                settle(fulls[c].at[:, pl.ds(0, len(far)), 0], sem.at[c])

        def a_to_b(c):
            first = cells[c] // 2
            settle(fulls[c].at[:, 0, 0], lo_recv.at[c])
            part = fulls[c].at[pl.ds(0, first), near_p, core]
            for there in far:
                send(part, part, bs, c, (at.s, there))
            settle_far(c, hi_recv)
            for p in far_p:
                part = fulls[c].at[pl.ds(first, cells[c] - first), p, core]
                send(part, part, bs, c, (at.s, near))

        def b_to_c(c):
            settle_far(c, b_recv)
            part = fulls[c].at[:, :, core]
            send(part, part, cs, c, at.partner())

        def of_rank(r, part):
            return wqs_r.at[:, pl.ds(pl.multiple_of(part * d + r * width, width), width)]

        def to_part(part):
            return wq_v.at[block_rows(at.index, rq), pl.ds(part * width, width)]

        for part in range(3):
            pltpu.make_async_copy(of_rank(rank, part), to_part(part), loc.at[0]).start()
        own_s = pltpu.make_async_copy(sms_r, sma.at[at.index], loc.at[1])
        own_s.start()
        for step in range(1, n):
            other = lax.rem(rank + step, n)
            for part in range(3):
                send(of_rank(other, part), to_part(part), ws, 0, at.member(other))
            send(sms_r, sma.at[at.index], ws, 1, at.member(other))
        settle(wq_v.at[pl.ds(0, rq)], loc.at[0])
        own_s.wait()
        settle(wq_v.at[pl.ds(0, (n - 1) * rq)], w_recv.at[0])
        settle(sma.at[pl.ds(0, n - 1)], w_recv.at[1])
        for low in range(half):
            row = (at.team * half + low) * m + 2 * at.plane
            send(wq_v.at[block_rows(row, rq, 2)], wq_v.at[block_rows(row, rq, 2)], ws, 2, at.across())
            send(sma.at[pl.ds(row, 2)], sma.at[pl.ds(row, 2)], ws, 3, at.across())
        start_z(0)
        start_z(1)

        @pl.when(jnp.logical_not(away))
        def _():
            pltpu.make_async_copy(tok_r, tokf.at[rank], loc.at[2]).start()

        settle(wq_v.at[pl.ds(0, half * 2 * rq)], w_recv.at[2])
        settle(sma.at[pl.ds(0, half * 2)], w_recv.at[3])
        def cut(block, h):
            return block.at[pl.ds(h * (size // 2), size // 2)]

        @pl.when(away)
        def _():
            for h in range(2):
                send(cut(tok_r, h), cut(tokf.at[at.low + half * (1 - core)], h), ts, h, at.swap())

        for step in range(1, planes):
            there = (at.s, 2 * at.beside(step) + core)
            for other in range(n):
                row = other * m + 2 * at.plane
                send(wq_v.at[block_rows(row, rq, 2)], wq_v.at[block_rows(row, rq, 2)], ws, 4, there)
                send(sma.at[pl.ds(row, 2)], sma.at[pl.ds(row, 2)], ws, 5, there)
        z_to_a(0)

        @pl.when(jnp.logical_not(away))
        def _():
            settle(tokf.at[0], loc.at[2])

        def own_half(h):
            @pl.when(away)
            def _():
                settle(cut(tokf.at[0], h), t_recv.at[h])

            part = cut(tokf.at[rank], h)
            for step in range(1, half):
                low = lax.rem(at.low + step, half)
                send(part, part, ts, 2 + h, (at.team * half + low, at.k))
            send(part, part, ts, 4, at.partner())

        own_half(0)

        settle(wq_v.at[pl.ds(0, (planes - 1) * n * 2 * rq)], w_recv.at[4])
        settle(sma.at[pl.ds(0, (planes - 1) * n * 2)], w_recv.at[5])
        per = LANES // (d // nd)
        for group in range(d // LANES):
            total = sma[group * per].astype(f32)
            for other in range(1, per):
                total = total + sma[group * per + other].astype(f32)
            sv_r[:, group * LANES : (group + 1) * LANES] = total
            vec[0, group : group + 1, :] = total[2:3]
            vec[1, group : group + 1, :] = total[3:4]

        def norm_block(b):
            def body(t, carry):
                part = pl.ds(pl.multiple_of(t * 128, 128), 128)
                x = tokf[b, part, :].astype(f32)
                normed, _ = normalize(x)
                h1_v[pl.ds(pl.multiple_of(b * size + t * 128, 128), 128), :] = (
                    normed * sv_r[0:1, :] + sv_r[1:2, :]
                ).astype(bf16)
                return carry

            lax.fori_loop(0, size // 128, body, 0)

        groups = width // LANES
        bias_q = jnp.concatenate([vec[0, pl.ds(rank * groups + g, 1), :] for g in range(groups)], 1)
        bias_v = jnp.concatenate([vec[1, pl.ds(rank * groups + g, 1), :] for g in range(groups)], 1)

        def project_block(b):
            def body(t, carry):
                part = pl.ds(pl.multiple_of(b * size + t * 256, 256), 256)
                h = h1_v[part, :]
                q_v[part, :] = (dot(h, wq_v[:, 0:width]) + bias_q).astype(bf16)
                k_v[part, :] = dot(h, wq_v[:, width : 2 * width]).astype(bf16)
                v_v[part, :] = (dot(h, wq_v[:, 2 * width : 3 * width]) + bias_v).astype(bf16)
                return carry

            lax.fori_loop(0, size // 256, body, 0)

        def later_z():
            start_z(2)

            @pl.when(away)
            def _():
                send(cot_r, cb_r, ts, 6, at.swap())

            @pl.when(jnp.logical_not(away))
            def _():
                pltpu.make_async_copy(cot_r, cb_r, loc.at[3]).start()

        own_half(1)

        def take(t, carry):
            @pl.when(t == 1)
            def _():
                z_to_a(1)
                settle(tokf.at[0], t_recv.at[4])
                a_to_b(0)

            if half > 1:

                @pl.when(t == 2)
                def _():
                    a_to_b(1)
                    for h in range(2):
                        settle(tokf.at[pl.ds(0, half - 1), pl.ds(0, size // 2)], t_recv.at[2 + h])
                        for step in range(1, half):
                            part = cut(tokf.at[lax.rem(at.low + step, half) + half * core], h)
                            send(part, part, ts, 5, at.partner())

                @pl.when(t == 1 + half)
                def _():
                    settle(tokf.at[pl.ds(0, half - 1)], t_recv.at[5])
                    later_z()

            step = jnp.where(t < 2, 0, lax.rem(t - 2, max(half - 1, 1)) + 1)
            other_core = jnp.where(t < 2, t, (t - 2) // max(half - 1, 1))
            side = core + other_core - 2 * core * other_core
            b = lax.rem(at.low + step, half) + half * side
            norm_block(b)
            project_block(b)
            return carry

        lax.fori_loop(0, n, take, 0)
        beside = rank + 1 - 2 * lax.rem(rank, 2)
        leaving = [
            (tokf.at[rank], tb_r.at[0]), (tokf.at[beside], tb_r.at[1]),
            (q_v, q_r), (k_v, k_r), (v_v, v_r), (h1_v, h1_r), (wq_v, wq_r),
        ]
        for i, (src, dst) in enumerate(leaving):
            pltpu.make_async_copy(src, dst, loc.at[4 + nc + i]).start()

        pumps = PUMPS

        def row(i, carry):
            attend_row(i, q_v, k_v, v_v, o_r, lse_r, qm, m_s, l_s, acc, size)
            src = o_r.at[block_rows(i, size)]
            for which, owner in ((0, i), (1, i + 1 - 2 * lax.rem(i, 2))):
                dst = att_r.at[which, :, block_rows(rank, width)]

                @pl.when(owner != rank)
                def _(dst=dst, which=which, owner=owner):
                    send(src, dst, (a_send, a_recv), which, at.member(owner))

                @pl.when(owner == rank)
                def _(dst=dst, which=which):
                    pltpu.make_async_copy(src, dst, loc.at[which]).start()

            for when, todo in enumerate(pumps):

                @pl.when(i == n - len(pumps) + when)
                def _(todo=todo):
                    for what, c in todo:
                        {"z": z_to_a, "a": a_to_b, "b": b_to_c}[what](c)

            return carry

        lax.fori_loop(0, n, row, 0)
        for what, c in TAIL:
            {"z": z_to_a, "a": a_to_b, "b": b_to_c}[what](c)
        others = att_r.at[0, :, pl.ds(0, (n - 1) * width)]
        for which in range(2):
            settle(att_r.at[0, :, pl.ds(0, width)], loc.at[which])
            settle(others, a_recv.at[which])
        for i, (src, dst) in enumerate(leaving):
            settle(src, loc.at[4 + nc + i])
        for c in range(nc):
            settle(fulls[c].at[:, :, 0], c_recv.at[c])

        for which in range(2):
            settle(others, a_send.at[which])
        for c in range(nc):
            settle_z(c, z_send)
            settle(fulls[c].at[:, 0, 0], lo_send.at[c])
            settle_far(c, hi_send)
            settle_far(c, b_send)
            settle(fulls[c].at[:, :, 0], c_send.at[c])
        for at_sem, count in ((0, n - 1), (2, half * 2), (4, (planes - 1) * n * 2)):
            settle(wq_v.at[pl.ds(0, count * rq)], w_send.at[at_sem])
            settle(sma.at[pl.ds(0, count)], w_send.at[at_sem + 1])

        @pl.when(away)
        def _():
            for h in range(2):
                settle(cut(tokf.at[0], h), t_send.at[h])
            settle(cb_r, t_recv.at[6])
            settle(cb_r, t_send.at[6])

        @pl.when(jnp.logical_not(away))
        def _():
            settle(cb_r, loc.at[3])

        settle(tokf.at[0], t_send.at[4])
        if half > 1:
            for h in range(2):
                settle(tokf.at[pl.ds(0, half - 1), pl.ds(0, size // 2)], t_send.at[2 + h])
            settle(tokf.at[pl.ds(0, half - 1)], t_send.at[5])

    def sds(shape, dtype=bf16):
        return jax.ShapeDtypeStruct(shape, dtype)

    sems = pltpu.SemaphoreType.DMA
    return pl.pallas_call(
        kernel,
        name="gather_attend",
        out_shape=(
            sds((n, m // 2, 2, *wo_s.shape)),
            sds((n, m // 2, 2, wi_s.shape[0], ff_half)),
            sds((half, m // 2, 2, *wb_s.shape)),
            sds((length, width)), sds((length, width)), sds((length, width)), sds((length, width)),
            sds((8, length), f32),
            sds((2, size, d)),
            sds((length, d)),
            sds((d, 3 * width)),
            sds((2, size, d)), sds((size, d)),
            sds((16, d), f32),
        ),
        in_specs=[HB] * 7,
        out_specs=(HB,) * 6 + (VM,) * 3 + (HB,) * 3 + (VM,) * 2,
        scratch_shapes=[
            pltpu.VMEM((length, width), bf16),
            pltpu.VMEM((length, width), bf16),
            pltpu.VMEM((length, width), bf16),
            pltpu.VMEM((length, d), bf16),
            pltpu.VMEM((d, 3 * width), bf16),
            pltpu.VMEM((n, size, d), bf16),
            pltpu.VMEM((nd, 16, LANES), bf16),
            pltpu.VMEM((width // HEAD_DIM, size, width), bf16),
            pltpu.VMEM((8, size), f32),
            pltpu.VMEM((8, size), f32),
            pltpu.VMEM((size, width), f32),
            pltpu.VMEM((2, max(8, d // LANES), LANES), f32),
            sems((7,)), sems((7,)),
            sems((6,)), sems((6,)),
            sems((2,)), sems((2,)),
            sems((nc,)), sems((nc,)),
            sems((nc,)), sems((nc,)),
            sems((nc,)), sems((nc,)),
            sems((nc,)), sems((nc,)),
            sems((nc,)), sems((nc,)),
            sems((11 + nc,)),
        ],
        compiler_params=pltpu.CompilerParams(
            collective_id=0, has_side_effects=True, vmem_limit_bytes=62 << 20
        ),
        cost_estimate=pl.CostEstimate(
            flops=6 * length * d * width + 2 * length * length * d // n, bytes_accessed=80 << 20, transcendentals=0
        ),
    )(tok, cot, wq_s, sm_s, wo_s, wi_s, wb_s)


def small_pack(index, vectors):
    per = vectors[0].shape[0]
    rows = [part for v in vectors for part in v.reshape(-1, per)]
    rows = jnp.stack(rows + [jnp.zeros_like(rows[0])] * (16 - len(rows)))
    lane = lax.broadcasted_iota(jnp.int32, (16, LANES), 1)
    spread = jnp.tile(rows, (1, LANES // per))
    return jnp.where(lane // per == lax.rem(index, LANES // per), spread, jnp.zeros_like(spread))


def backward_call(n, m, res, dat, dres, q, k, v, o, lse, h1, wq, tb, sv, gsm, gwo, gwi, gwb):
    size, d = dat.shape
    nd = n * m
    length = n * size
    width = d // n
    heads = width // HEAD_DIM
    half, planes = n // 2, m // 2
    rq = d // nd
    quarter = gwi.shape[4] // 2
    parts = [
        (half, *gwb.shape[3:]), (n, gwi.shape[3], quarter), (n, gwi.shape[3], quarter), (n, *gwo.shape[3:]),
    ]
    cells = [p[0] for p in parts]
    nc = len(cells)
    lanes_s = d // n

    def kernel(*refs):
        (res_r, dat_r, dres_r, q_h, k_h, v_h, o_r, lse_r, h1_r, wq_h, tb_r, sv_r, gsm_r, gwo_r, gwi_r, gwb_r) = refs[:16]
        (reso_r, gt_r, rg, gqo_r, go_r, gi_r, gb_r, small_r) = refs[16:24]
        (do, delta, dqa, dka, dva, dqkv, gacc, rqp, rqh, pf, sd, rd, rzd, sm, smz, smp, smc) = refs[24:41]
        gqb, hb, sg, tb_v, o_v, q_r, k_r, v_r, wq_r, gq_r = refs[41:51]
        rest = refs[51:]
        ga, rc, rp, rz = (rest[i * nc : (i + 1) * nc] for i in range(4))
        (d_s, d_r, x_s, x_r, y_s, y_r, e_s, e_r, c_s, c_r, p_s, p_r, z_s, z_r, m_s, m_r, yl_s, yl_r, el_s, el_r, loc) = rest[4 * nc :]
        at = Place(n, m)
        rank, core, low = at.rank, at.core, at.low
        left, right = (gwi_r.at[:, :, :, :, pl.ds(p * quarter, quarter)] for p in range(2))
        grads = (gwb_r, left, right, gwo_r)
        at.greet()
        away = core != at.team

        for step in range(1, n):
            other = lax.rem(rank + step, n)
            send(dat_r.at[:, block_rows(other, width)], do.at[block_rows(rank, size)], (d_s, d_r), 0, at.member(other))
        own_do = pltpu.make_async_copy(dat_r.at[:, block_rows(rank, width)], do.at[block_rows(rank, size)], loc.at[0])
        own_do.start()

        for c in range(nc):
            send(grads[c].at[:, :, 1 - core], rc[c], (c_s, c_r), c, at.partner())
            pltpu.make_async_copy(grads[c].at[:, :, core], ga[c], loc.at[6 + c]).start()
        fetch_tb = pltpu.make_async_copy(tb_r.at[0], tb_v, loc.at[4])
        fetch_tb.start()
        for i in range(n):
            pltpu.make_async_copy(o_r.at[pl.ds(i * size, size)], o_v.at[:, pl.ds(i * width, width)], loc.at[5]).start()

        arriving = [(q_h, q_r), (k_h, k_r), (v_h, v_r), (wq_h, wq_r)]
        for i, (src, dst) in enumerate(arriving):
            pltpu.make_async_copy(src, dst, loc.at[6 + nc + i]).start()

        own_dres = pltpu.make_async_copy(dres_r, gt_r, loc.at[2])
        own_dres.start()

        def fetch_h1(b):
            return pltpu.make_async_copy(h1_r.at[block_rows(b, size)], hb.at[block_rows(lax.rem(b, 2), size)], loc.at[3])

        def c_to_p(c):
            settle(ga[c], loc.at[6 + c])
            settle(rc[c], c_r.at[c])

            def add(t, carry):
                s, p = t // planes, lax.rem(t, planes)
                ga[c][s, p] = (ga[c][s, p].astype(f32) + rc[c][s, p].astype(f32)).astype(bf16)
                return carry

            lax.fori_loop(0, cells[c] * planes, add, 0)
            for step in range(1, planes):
                other = at.beside(step)
                send(ga[c].at[:, other], rp[c].at[step - 1], (p_s, p_r), c, (at.s, 2 * other + core))

        def p_to_z(c):
            settle(rp[c], p_r.at[c])

            def add(s, carry):
                total = ga[c][s, at.plane].astype(f32)
                for step in range(1, planes):
                    total = total + rp[c][step - 1, s].astype(f32)
                ga[c][s, at.plane] = total.astype(bf16)
                return carry

            lax.fori_loop(0, cells[c], add, 0)
            if c > 0:
                for step in range(1, n):
                    s = at.along(step)
                    send(ga[c].at[s, at.plane], rz[c].at[at.s], (z_s, z_r), c, (s, at.k))
                rz[c][at.s] = ga[c][at.s, at.plane]
                return
            source = at.team * (half // 2) + at.low // 2
            for place in range(half):
                s = at.odd * half + place

                @pl.when(s != at.s)
                def _(s=s, place=place):
                    send(ga[c].at[place, at.plane], rz[c].at[source], (z_s, z_r), c, (s, at.k))

                @pl.when(s == at.s)
                def _(place=place):
                    rz[c][source] = ga[c][place, at.plane]

        def settle_z(c, sem):
            if c > 0:
                settle(rz[c].at[pl.ds(0, n - 1)], sem.at[c])
                return

            @pl.when(at.odd == at.team)
            def _():
                settle(rz[c].at[pl.ds(0, half - 1)], sem.at[c])

            @pl.when(at.odd != at.team)
            def _():
                settle(rz[c].at[pl.ds(0, half)], sem.at[c])

        def z_to_out(c):
            settle_z(c, z_r)

            def total(sources):
                out = rz[c][sources[0]].astype(f32)
                for s in sources[1:]:
                    out = out + rz[c][s].astype(f32)
                return out

            if c == 0:
                gb_r[...] = total(range(half))
            elif c < 3:
                for odd in range(2):
                    first = (2 * odd + c - 1) * quarter
                    gi_r[:, first : first + quarter] = total([s for s in range(n) if s % half % 2 == odd])
            else:
                go_r[...] = total(range(n))

        for c in range(nc):
            c_to_p(c)
        fetch_h1(0).start()

        own_do.wait()
        settle(do.at[pl.ds(0, (n - 1) * size)], d_r.at[0])
        for i, (src, dst) in enumerate(arriving):
            settle(dst, loc.at[6 + nc + i])

        @pl.when(away)
        def _():
            send(res_r, reso_r, (x_s, x_r), 0, at.swap())

        @pl.when(jnp.logical_not(away))
        def _():
            pltpu.make_async_copy(res_r, reso_r, loc.at[1]).start()

        settle(o_v.at[:, pl.ds(0, n * width)], loc.at[5])
        pick = (
            lax.broadcasted_iota(jnp.int32, (8, width), 1) // HEAD_DIM
            == lax.broadcasted_iota(jnp.int32, (8, width), 0)
        ).astype(f32)

        def prepare(i, carry):
            rows = block_rows(i, size)
            product = do[rows, :].astype(f32) * o_v[:, block_rows(i, width)].astype(f32)
            delta[:, rows] = lax.dot_general(
                pick, product, NT, preferred_element_type=f32, precision=lax.Precision.HIGHEST
            )
            dqa[rows, :] = jnp.zeros((size, width), f32)
            return carry

        lax.fori_loop(0, n, prepare, 0)
        gacc[...] = jnp.zeros_like(gacc)
        sm[...] = jnp.zeros_like(sm)
        sm[4:12, :] = gsm_r[...]

        def pair(i, j, diagonal):
            rows, at_k = block_rows(i, size), block_rows(j, size)
            kk, vv = k_r[at_k, :], v_r[at_k, :]
            qs, dd = q_r[rows, :] * jnp.asarray(scale, bf16), do[rows, :]
            dq = dk = dv = None
            for h in range(heads):
                qh, dh_, kh = only_head(qs, h), only_head(dd, h), only_head(kk, h)
                p = jnp.exp(row_dot(kk, qh) - lse_r[h : h + 1, rows])
                if diagonal:
                    k_pos = lax.broadcasted_iota(jnp.int32, (size, size), 0)
                    q_pos = lax.broadcasted_iota(jnp.int32, (size, size), 1)
                    p = jnp.where(k_pos <= q_pos, p, 0.0)
                dp = row_dot(vv, dh_)
                ds = (p * (dp - delta[h : h + 1, rows])).astype(bf16)
                one, two, three = dot(p.astype(bf16), dh_), dot(ds, qh), col_dot(ds, kh)
                dv = one if dv is None else dv + one
                dk = two if dk is None else dk + two
                dq = three if dq is None else dq + three
            dva[...] += dv
            dka[...] += dk
            dqa[rows, :] += dq

        def owner(j):
            return j // half, lax.rem(j, half)

        def finish_block(j):
            core_j, low_j = owner(j)

            @pl.when(core_j == core)
            def _():
                settle(rd.at[0], y_r.at[low_j])

                def add(t, carry):
                    rows = pl.ds(pl.multiple_of(t * 128, 128), 128)
                    rd[low_j, rows, :] = (pf[rows, :] + rd[low_j, rows, :].astype(f32)).astype(bf16)
                    return carry

                lax.fori_loop(0, size // 128, add, 0)

                @pl.when(low_j != low)
                def _():
                    slot = lax.rem(low_j - low + half, half) - 1
                    send(rd.at[low_j], rzd.at[slot], (e_s, e_r), 0, (at.team * half + low_j, at.k))

        def column(j, carry):
            fetch_h1(j).wait()

            @pl.when(j + 1 < n)
            def _():
                fetch_h1(j + 1).start()

            dka[...] = jnp.zeros_like(dka)
            dva[...] = jnp.zeros_like(dva)
            pair(j, j, True)

            def inner(i, c2):
                pair(i, j, False)
                return c2

            lax.fori_loop(j + 1, n, inner, 0)
            dqb = (dqa[block_rows(j, size), :] * scale).astype(bf16)
            dkb, dvb = dka[...].astype(bf16), dva[...].astype(bf16)
            dqkv[:, 0:width] = dqb
            dqkv[:, width : 2 * width] = dkb
            dqkv[:, 2 * width : 3 * width] = dvb
            mine = block_rows(rank, width)
            sm[2:3, mine] += jnp.sum(dqb.astype(f32), axis=0, keepdims=True)
            sm[3:4, mine] += jnp.sum(dvb.astype(f32), axis=0, keepdims=True)

            @pl.when(j > 0)
            def _():
                finish_block(j - 1)

            core_j, low_j = owner(j)

            def project(t, c2):
                rows = pl.ds(pl.multiple_of(t * PIECE, PIECE), PIECE)
                part = row_dot(dqkv[rows, :], wq_r[...])

                @pl.when(core_j == core)
                def _():
                    pf[rows, :] = part

                @pl.when(core_j != core)
                def _():
                    sd[low_j, rows, :] = part.astype(bf16)

                    @pl.when(j == n - 1)
                    def _():
                        send(sd.at[low_j, rows], rd.at[low_j, rows], (yl_s, yl_r), t, at.partner())

                return c2

            lax.fori_loop(0, size // PIECE, project, 0)

            @pl.when(jnp.logical_and(core_j != core, j < n - 1))
            def _():
                send(sd.at[low_j], rd.at[low_j], (y_s, y_r), low_j, at.partner())

            slot = lax.rem(j, 2)
            for t in range(3):
                cols = slice(t * width, (t + 1) * width)
                gacc[:, cols] += col_dot(hb[block_rows(slot, size), :], dqkv[:, cols])
            for c in range(nc - 1):

                @pl.when(j == min(c, n - 2))
                def _(c=c):
                    p_to_z(c)

            return carry

        lax.fori_loop(0, n, column, 0)
        gqb[...] = gacc[...].astype(bf16)
        for step in range(1, planes):
            other = at.beside(step)
            for s in range(n):
                send(
                    gqb.at[block_rows(s * m + 2 * other, rq, 2)],
                    rqp.at[block_rows((step - 1) * n + s, 2 * rq)],
                    (m_s, m_r), 0, (at.s, 2 * other + core),
                )
        pieces = size // PIECE
        last = half - 1
        owner_last = (at.team * half + last, at.k)

        def pair_piece(rows):
            rd[last, rows, :] = (pf[rows, :] + rd[last, rows, :].astype(f32)).astype(bf16)

        @pl.when(jnp.logical_and(core == 1, low != last))
        def _():
            def pass_on(t, carry):
                rows = pl.ds(pl.multiple_of(t * PIECE, PIECE), PIECE)
                settle(rd.at[last, rows], yl_r.at[t])
                pair_piece(rows)
                send(rd.at[last, rows], rzd.at[last - low - 1, rows], (el_s, el_r), t, owner_last)
                return carry

            lax.fori_loop(0, pieces, pass_on, 0)

        own_dres.wait()
        fetch_tb.wait()
        if half > 1:

            @pl.when(rank != n - 1)
            def _():
                settle(rzd, e_r.at[0])

        def norm_step(t, carry):
            sum_g, sum_s = carry
            rows = pl.ds(pl.multiple_of(t * PIECE, PIECE), PIECE)

            @pl.when(rank == n - 1)
            def _():
                settle(rd.at[last, rows], yl_r.at[t])
                pair_piece(rows)
                if half > 1:
                    settle(rzd.at[:, rows], el_r.at[t])

            dh1 = rd[low, rows, :].astype(f32)
            for slot in range(half - 1):
                dh1 = dh1 + rzd[slot, rows, :].astype(f32)
            normed, inv = normalize(tb_v[rows, :].astype(f32))
            grad = gt_r[rows, :] + norm_back(dh1 * sv_r[0:1, :], normed, inv)
            gt_r[rows, :] = grad
            sg[rows, :] = grad.astype(bf16)

            @pl.when(away)
            def _():
                send(sg.at[rows], rg.at[rows], (x_s, x_r), 1, at.swap())

            return (
                sum_g + jnp.sum(dh1 * normed, axis=0, keepdims=True),
                sum_s + jnp.sum(dh1, axis=0, keepdims=True),
            )

        zero = jnp.zeros((1, d), f32)
        sum_g, sum_s = lax.fori_loop(0, pieces, norm_step, (zero, zero))
        sm[0:1, :] = sum_g
        sm[1:2, :] = sum_s

        settle(rqp, m_r.at[0])

        def add_q(s, carry):
            rows = block_rows(s * m + 2 * at.plane, rq, 2)
            total = gqb[rows, :].astype(f32)
            for step in range(1, planes):
                total = total + rqp[block_rows((step - 1) * n + s, 2 * rq), :].astype(f32)
            gqb[rows, :] = total.astype(bf16)
            return carry

        lax.fori_loop(0, n, add_q, 0)
        for l in range(half):
            row = ((1 - at.team) * half + l) * m + 2 * at.plane
            send(gqb.at[block_rows(row, rq, 2)], rqh.at[block_rows(l, 2 * rq)], (m_s, m_r), 2, at.across())

        p_to_z(nc - 1)
        send(sm, smc, (m_s, m_r), 1, at.partner())
        settle(rqh, m_r.at[2])
        for l in range(half):
            rows = block_rows((at.team * half + l) * m + 2 * at.plane, rq, 2)
            gqb[rows, :] = (
                gqb[rows, :].astype(f32) + rqh[block_rows(l, 2 * rq), :].astype(f32)
            ).astype(bf16)

        def member_rows(r):
            return block_rows((at.team * half + lax.rem(r, half)) * m + 2 * at.plane + r // half, rq)

        for step in range(1, n):
            other = lax.rem(rank + step, n)
            send(gqb.at[member_rows(other)], gq_r.at[rank], (m_s, m_r), 4, at.member(other))
        pltpu.make_async_copy(gqb.at[member_rows(rank)], gq_r.at[rank], loc.at[0]).start()

        settle(smc, m_r.at[1])
        settle(smc, m_s.at[1])
        sm[...] = sm[...] + smc[...]
        for step in range(1, planes):
            send(sm, smp.at[step - 1], (m_s, m_r), 3, (at.s, 2 * at.beside(step) + core))
        for c in range(nc):
            z_to_out(c)
        settle(smp, m_r.at[3])
        settle(smp, m_s.at[3])
        total = sm[...]
        for step in range(1, planes):
            total = total + smp[step - 1]
        sm[...] = total
        for step in range(1, n):
            s = at.along(step)
            send(sm.at[:, block_rows(s, lanes_s)], smz.at[step - 1], (m_s, m_r), 5, (s, at.k))
        settle(smz, m_r.at[5])
        total = sm[:, block_rows(at.s, lanes_s)]
        for step in range(1, n):
            total = total + smz[step - 1]
        small_r[...] = total

        settle(gq_r.at[pl.ds(0, n - 1)], m_r.at[4])
        settle(gq_r.at[0], loc.at[0])
        for r in range(n):
            for part in range(3):
                first = part * d + r * width
                gqo_r[:, first : first + width] = gq_r[r, :, part * width : (part + 1) * width].astype(f32)

        @pl.when(away)
        def _():
            settle(rg, x_r.at[1])
            settle(rg, x_s.at[1])
            settle(reso_r, x_r.at[0])
            settle(reso_r, x_s.at[0])

        @pl.when(jnp.logical_not(away))
        def _():
            settle(reso_r, loc.at[1])

        settle(do.at[pl.ds(0, (n - 1) * size)], d_s.at[0])
        for c in range(nc):
            settle(rc[c], c_s.at[c])
            settle(rp[c], p_s.at[c])
            settle_z(c, z_s)
        for l in range(half - 1):
            settle(rd.at[0], y_s.at[l])

        @pl.when(core == 1)
        def _():
            settle(rd.at[0], y_s.at[last])

        @pl.when(core == 0)
        def _():
            for t in range(pieces):
                settle(rd.at[0, pl.ds(0, PIECE)], yl_s.at[t])

        passes = jnp.logical_and(core == 1, low != last)

        @pl.when(passes)
        def _():
            for t in range(pieces):
                settle(rd.at[0, pl.ds(0, PIECE)], el_s.at[t])

        if half > 2:

            @pl.when(passes)
            def _():
                settle(rzd.at[pl.ds(0, half - 2)], e_s.at[0])

        if half > 1:

            @pl.when(jnp.logical_not(passes))
            def _():
                settle(rzd, e_s.at[0])

        settle(rqp, m_s.at[0])
        settle(smz, m_s.at[5])
        settle(rqh, m_s.at[2])
        settle(gq_r.at[pl.ds(0, n - 1)], m_s.at[4])

    def sds(shape, dtype=bf16):
        return jax.ShapeDtypeStruct(shape, dtype)

    sems = pltpu.SemaphoreType.DMA
    return pl.pallas_call(
        kernel,
        name="attend_back_reduce",
        out_shape=(
            sds((size, d)),
            sds((size, d), f32),
            sds((size, d)),
            sds((rq, 3 * d), f32),
            sds(gwo.shape[3:], f32),
            sds((gwi.shape[3], 2 * gwi.shape[4]), f32),
            sds(gwb.shape[3:], f32),
            sds((16, lanes_s), f32),
        ),
        in_specs=[HB] * 7 + [VM, HB, HB, HB] + [VM] * 2 + [HB] * 3,
        out_specs=(HB, VM, HB) + (VM,) * 5,
        scratch_shapes=[
            pltpu.VMEM((length, width), bf16),
            pltpu.VMEM((8, length), f32),
            pltpu.VMEM((length, width), f32),
            pltpu.VMEM((size, width), f32),
            pltpu.VMEM((size, width), f32),
            pltpu.VMEM((size, 3 * width), bf16),
            pltpu.VMEM((d, 3 * width), f32),
            pltpu.VMEM(((planes - 1) * n * 2 * rq, 3 * width), bf16),
            pltpu.VMEM((half * 2 * rq, 3 * width), bf16),
            pltpu.VMEM((size, d), f32),
            pltpu.VMEM((half, size, d), bf16),
            pltpu.VMEM((half, size, d), bf16),
            pltpu.VMEM((max(half - 1, 1), size, d), bf16),
            pltpu.VMEM((16, d), f32),
            pltpu.VMEM((n - 1, 16, lanes_s), f32),
            pltpu.VMEM((planes - 1, 16, d), f32),
            pltpu.VMEM((16, d), f32),
        ]
        + [
            pltpu.VMEM((d, 3 * width), bf16),
            pltpu.VMEM((2 * size, d), bf16),
            pltpu.VMEM((size, d), bf16),
            pltpu.VMEM((size, d), bf16),
            pltpu.VMEM((size, d), bf16),
            pltpu.VMEM((length, width), bf16),
            pltpu.VMEM((length, width), bf16),
            pltpu.VMEM((length, width), bf16),
            pltpu.VMEM((d, 3 * width), bf16),
            pltpu.VMEM((n, rq, 3 * width), bf16),
        ]
        + [pltpu.VMEM((count, planes, rows, cols), bf16) for count, rows, cols in parts] * 2
        + [pltpu.VMEM((planes - 1, *part), bf16) for part in parts]
        + [pltpu.VMEM(part, bf16) for part in parts]
        + [
            sems((1,)), sems((1,)),
            sems((2,)), sems((2,)),
            sems((half,)), sems((half,)),
            sems((1,)), sems((1,)),
            sems((nc,)), sems((nc,)),
            sems((nc,)), sems((nc,)),
            sems((nc,)), sems((nc,)),
            sems((6,)), sems((6,)),
            sems((size // PIECE,)), sems((size // PIECE,)),
            sems((size // PIECE,)), sems((size // PIECE,)),
            sems((10 + nc,)),
        ],
        compiler_params=pltpu.CompilerParams(
            collective_id=1, has_side_effects=True, vmem_limit_bytes=67043328
        ),
        cost_estimate=pl.CostEstimate(
            flops=12 * length * d * width + 5 * length * length * d // n, bytes_accessed=80 << 20, transcendentals=0
        ),
    )(res, dat, dres, q, k, v, o, lse, h1, wq, tb, sv, gsm, gwo, gwi, gwb)


def hidden_forward_call(att, tokens, wo, wi, wb, sv, bias):
    size, d = att.shape[1:]
    rows, hidden = 2 * size, wi.shape[1]
    some, columns = 256, hidden // 4
    blocks = size // some

    def kernel(
        att_h, tok_h, wo_h, wi_h, wb_h, sv_r, bias_r, norm_r, inv_r, h2_h, act_h, slope_h, own_r, other_r,
        att_v, tok_v, wo_v, wi_v, wb_v, h2_v, act_v, slope_v, loc,
    ):
        loads = ((att_h, att_v), (wo_h, wo_v), (tok_h, tok_v), (wi_h, wi_v), (wb_h, wb_v))
        for i, (src, dst) in enumerate(loads):
            pltpu.make_async_copy(src, dst, loc.at[i]).start()
        for i in range(3):
            settle(loads[i][1], loc.at[i])

        def first(t, carry):
            b = t // blocks
            part = pl.ds(pl.multiple_of(lax.rem(t, blocks) * some, some), some)
            resid = tok_v[b, part, :].astype(f32) + dot(att_v[b, part, :], wo_v[...]) + sv_r[4:5, :]

            normed, inv = normalize(resid)

            @pl.when(b == 0)
            def _():
                own_r[part, :] = resid + sv_r[7:8, :]
                norm_r[part, :] = normed
                inv_r[part, :] = jnp.broadcast_to(inv, (some, LANES))

            h2_v[pl.ds(pl.multiple_of(t * some, some), some), :] = (normed * sv_r[5:6, :] + sv_r[6:7, :]).astype(bf16)
            return carry

        lax.fori_loop(0, rows // some, first, 0)
        pltpu.make_async_copy(h2_v, h2_h, loc.at[5]).start()
        settle(wi_v, loc.at[3])

        def second(t, carry):
            part = pl.ds(pl.multiple_of(t * some, some), some)
            h = h2_v[part, :]
            for c in range(4):
                cols = slice(c * columns, (c + 1) * columns)
                act, slope = gelu_pair(dot(h, wi_v[:, cols]) + bias_r[:, cols])
                act_v[part, cols] = act.astype(bf16)
                slope_v[part, cols] = slope
            pltpu.make_async_copy(act_v.at[part], act_h.at[part], loc.at[6]).start()
            pltpu.make_async_copy(slope_v.at[part], slope_h.at[part], loc.at[7]).start()

            @pl.when(t == 0)
            def _():
                settle(wb_v, loc.at[4])

            out = dot(act_v[part, :], wb_v[...])

            @pl.when(t < blocks)
            def _():
                own_r[part, :] += out

            @pl.when(t >= blocks)
            def _():
                other_r[pl.ds(pl.multiple_of(t * some - size, some), some), :] = out.astype(bf16)

            return carry

        lax.fori_loop(0, rows // some, second, 0)
        settle(h2_v, loc.at[5])
        settle(act_v, loc.at[6])
        settle(slope_v, loc.at[7])

    def sds(shape, dtype=bf16):
        return jax.ShapeDtypeStruct(shape, dtype)

    return pl.pallas_call(
        kernel,
        name="hidden_forward",
        out_shape=(
            sds((size, d), f32), sds((size, LANES), f32), sds((rows, d)), sds((rows, hidden)), sds((rows, hidden), f32),
            sds((size, d), f32), sds((size, d)),
        ),
        in_specs=[HB] * 5 + [VM] * 2,
        out_specs=(VM,) * 2 + (HB,) * 3 + (VM,) * 2,
        scratch_shapes=[
            pltpu.VMEM(att.shape, bf16),
            pltpu.VMEM(tokens.shape, bf16),
            pltpu.VMEM(wo.shape, bf16),
            pltpu.VMEM(wi.shape, bf16),
            pltpu.VMEM(wb.shape, bf16),
            pltpu.VMEM((rows, d), bf16),
            pltpu.VMEM((rows, hidden), bf16),
            pltpu.VMEM((rows, hidden), f32),
            pltpu.SemaphoreType.DMA((8,)),
        ],
        compiler_params=pltpu.CompilerParams(vmem_limit_bytes=56 << 20),
        cost_estimate=pl.CostEstimate(
            flops=2 * rows * d * (d + 2 * hidden), bytes_accessed=40 << 20, transcendentals=rows * hidden
        ),
    )(att, tokens, wo, wi, wb, sv, bias)


def hidden_back_call(slopes, cot, wb, wi):
    rows, hidden = slopes.shape
    d = cot.shape[1]
    some, columns = 256, hidden // 4

    def kernel(slope_h, cot_h, wb_h, wi_h, dp_h, own_r, other_r, gb_r, slope_v, cot_v, wb_v, wi_v, dp_v, loc):
        steps = rows // some
        for i, (src, dst) in enumerate(((cot_h, cot_v), (wb_h, wb_v), (wi_h, wi_v))):
            pltpu.make_async_copy(src, dst, loc.at[i]).start()
        for t in range(steps):
            part = pl.ds(t * some, some)
            pltpu.make_async_copy(slope_h.at[part], slope_v.at[part], loc.at[5 + t]).start()
        gb_r[...] = jnp.zeros_like(gb_r)
        settle(cot_v, loc.at[0])
        settle(wb_v, loc.at[1])

        def body(t, carry):
            part = pl.ds(pl.multiple_of(t * some, some), some)
            settle(slope_v.at[part], loc.at[5 + t])
            c_rows = cot_v[part, :]
            for c in range(4):
                cols = slice(c * columns, (c + 1) * columns)
                grad = (row_dot(c_rows, wb_v[cols, :]) * slope_v[part, cols]).astype(bf16)
                dp_v[part, cols] = grad
                gb_r[:, cols] += jnp.sum(grad.astype(f32), axis=0, keepdims=True)
            pltpu.make_async_copy(dp_v.at[part], dp_h.at[part], loc.at[4]).start()

            @pl.when(t == 0)
            def _():
                settle(wi_v, loc.at[2])

            back = row_dot(dp_v[part, :], wi_v[...])

            @pl.when(t < steps // 2)
            def _():
                own_r[part, :] = back

            @pl.when(t >= steps // 2)
            def _():
                other_r[pl.ds(pl.multiple_of(t * some - rows // 2, some), some), :] = back.astype(bf16)

            return carry

        lax.fori_loop(0, steps, body, 0)
        settle(dp_v, loc.at[4])

    def sds(shape, dtype=bf16):
        return jax.ShapeDtypeStruct(shape, dtype)

    return pl.pallas_call(
        kernel,
        name="hidden_back",
        out_shape=(sds(slopes.shape), sds((rows // 2, d), f32), sds((rows // 2, d)), sds((1, hidden), f32)),
        in_specs=[HB] * 4,
        out_specs=(HB,) + (VM,) * 3,
        scratch_shapes=[
            pltpu.VMEM(slopes.shape, f32),
            pltpu.VMEM(cot.shape, bf16),
            pltpu.VMEM(wb.shape, bf16),
            pltpu.VMEM(wi.shape, bf16),
            pltpu.VMEM(slopes.shape, bf16),
            pltpu.SemaphoreType.DMA((5 + rows // some,)),
        ],
        compiler_params=pltpu.CompilerParams(vmem_limit_bytes=56 << 20),
        cost_estimate=pl.CostEstimate(flops=4 * rows * d * hidden, bytes_accessed=28 << 20, transcendentals=0),
    )(slopes, cot, wb, wi)


def solution(mesh):
    n, m = mesh.shape["seq"], mesh.shape["shard"]
    nd = n * m
    every = ("seq", "shard")

    def per_device(
        tokens, ln1_gain, ln1_bias, w_qkv, bias_query, bias_value, w_out, bias_out,
        ln2_gain, ln2_bias, w_in, bias_in, w_back, bias_back, cotangent,
    ):
        d = tokens.shape[2]
        width = d // n
        index = lax.axis_index("seq") * m + lax.axis_index("shard")
        pack = small_pack(
            index,
            [ln1_gain, ln1_bias, bias_query, bias_value, bias_out, ln2_gain, ln2_bias, bias_back, bias_in],
        )
        rq = w_qkv.shape[0]
        ff = w_in.shape[1]
        rq = w_qkv.shape[0]
        (full_out, full_in, full_back, q, k, v, o, lse, att_two, h1, wq, tb, cot_own, sv) = forward_call(
            n, m, tokens[0], cotangent[0], w_qkv, pack, w_out, w_in, w_back
        )
        full_out = full_out.reshape(d, d)
        half_in = full_in.reshape(d, ff // 2)
        half_back = full_back.reshape(ff // 2, d)
        odd = lax.rem(lax.rem(lax.axis_index("seq"), n // 2), 2)
        per = d // nd
        parts = bias_in.shape[0] // per
        half_bin = lax.dynamic_slice_in_dim(sv[8 : 8 + parts], odd * (d // 2), d // 2, 1)
        half_bin = half_bin.reshape(parts, nd // 2, per).transpose(1, 0, 2).reshape(-1)
        g_two = sv[5]

        def to_neighbour(values):
            pairs = []
            for s in range(n):
                there = s // 2 * 2 + 1 - s % 2
                pairs += [(s * m + k, there * m + k) for k in range(m)]
            return lax.ppermute(values.astype(bf16), every, pairs).astype(f32)

        size = tokens.shape[1]
        cot_two = jnp.concatenate([cot_own, to_neighbour(cot_own).astype(bf16)])
        normed2, scale2, h_two, act, slopes, own_out, leaves = hidden_forward_call(
            att_two, tb, full_out, half_in, half_back, sv, half_bin.reshape(1, -1)
        )
        others_out = to_neighbour(leaves)
        slopes, leaves = lax.optimization_barrier((slopes, leaves))
        d_pre, d_h2_own, leaves, g_b_in = hidden_back_call(slopes, cot_two, half_back, half_in)
        others_d = to_neighbour(leaves)
        act, d_pre, leaves = lax.optimization_barrier((act, d_pre, leaves))
        g_w_back = col_dot(act, cot_two).astype(bf16)
        g_w_in = col_dot(h_two, d_pre).astype(bf16)

        scale2 = scale2[:, :1]
        att_tok, cot_f = att_two[0], cot_own.astype(f32)
        result = (own_out + others_out).astype(bf16)
        g_b_back = jnp.sum(cot_f, axis=0)
        d_h2 = d_h2_own + others_d
        g_g2 = jnp.sum(d_h2 * normed2, axis=0)
        g_s2 = jnp.sum(d_h2, axis=0)
        d_resid = cot_f + norm_back(d_h2 * g_two, normed2, scale2)
        d_resid_b = d_resid.astype(bf16)
        g_w_out = col_dot(att_tok, d_resid_b).astype(bf16)
        g_b_out = jnp.sum(d_resid, axis=0)
        d_att_tok = row_dot(d_resid_b, full_out).astype(bf16)
        bin_rows = g_b_in.reshape(nd // 2, parts, per).transpose(1, 0, 2).reshape(parts, d // 2)
        bin_rows = jnp.where(
            lax.broadcasted_iota(jnp.int32, (parts, d), 1) // (d // 2) == odd, jnp.tile(bin_rows, (1, 2)), 0.0
        )
        gsm = jnp.concatenate([jnp.stack([g_b_out, g_g2, g_s2, g_b_back]), bin_rows])

        (own_result, g_tok, swapped, g_qkv, go, gi, gb, small) = backward_call(
            n, m, result, d_att_tok, d_resid, q, k, v, o, lse, h1, wq, tb, sv, gsm,
            g_w_out.reshape(n, m // 2, 2, d // nd, d),
            g_w_in.reshape(n, m // 2, 2, d // nd, ff // 2),
            g_w_back.reshape(n // 2, m // 2, 2, ff // nd, d),
        )
        away = lax.rem(lax.axis_index("shard"), 2) != lax.axis_index("seq") // (n // 2)
        g_tok = jnp.where(away, swapped.astype(f32), g_tok)
        mine = lax.dynamic_slice_in_dim(small, lax.axis_index("shard") * per, per, 1)
        return (
            own_result[None], g_tok[None], mine[0], mine[1], g_qkv, mine[2], mine[3], go, mine[4],
            mine[5], mine[6], gi, mine[8 : 8 + parts].reshape(-1), gb, mine[7],
        )

    whole, vector, matrix = P("shard", "seq", None), P(every), P(every, None)
    return jax.shard_map(
        per_device,
        mesh=mesh,
        in_specs=(
            whole, vector, vector, matrix, vector, vector, matrix, vector, vector, vector, matrix, vector,
            matrix, vector, whole,
        ),
        out_specs=(
            whole, whole, vector, vector, matrix, vector, vector, matrix, vector, vector, vector, matrix,
            vector, matrix, vector,
        ),
        check_vma=False,
    )
```

```python
import math

import jax
import jax.numpy as jnp
from jax import lax
from jax.experimental import pallas as pl
from jax.experimental.pallas import tpu as pltpu
from jax.sharding import PartitionSpec as P

HEAD_DIM = 64
PUMPS = ((('b', 0), ('b', 1)), (('z', 2),), ())
TAIL = (('a', 2), ('b', 2))
LANES = 128
PIECE = 128
MESH = pl.DeviceIdType.MESH
NT = (((1,), (1,)), ((), ()))
TN = (((0,), (0,)), ((), ()))
f32 = jnp.float32
bf16 = jnp.bfloat16

norm_eps = 1e-05
gelu_c = math.sqrt(2.0 / math.pi)
scale = 1.0 / math.sqrt(HEAD_DIM)

VM = pl.BlockSpec(memory_space=pltpu.VMEM)
HB = pl.BlockSpec(memory_space=pl.ANY)


def dot(a, b):
    return jnp.dot(a, b, preferred_element_type=f32)


def row_dot(a, b):
    return lax.dot_general(a, b, NT, preferred_element_type=f32)


def col_dot(a, b):
    return lax.dot_general(a, b, TN, preferred_element_type=f32)


def normalize(values):
    mean_row = jnp.mean(values, axis=-1, keepdims=True)
    centred = values - mean_row
    var_row = jnp.mean(centred * centred, axis=-1, keepdims=True)
    scale_row = lax.rsqrt(var_row + norm_eps)
    return (centred * scale_row, scale_row)


def norm_back(dnormed, normed, scale_row):
    return scale_row * (
        dnormed
        - jnp.mean(dnormed, axis=-1, keepdims=True)
        - normed * jnp.mean(dnormed * normed, axis=-1, keepdims=True)
    )


def gelu_pair(inputs):
    inner = gelu_c * (inputs + 0.044715 * inputs * inputs * inputs)
    tanh_val = jnp.tanh(inner)
    value = 0.5 * inputs * (1.0 + tanh_val)
    slope = 0.5 * (1.0 + tanh_val) + 0.5 * inputs * (1.0 - tanh_val * tanh_val) * gelu_c * (
        1.0 + 3.0 * 0.044715 * inputs * inputs
    )
    return (value, slope)


def block_rows(index, size, count=1):
    return pl.ds(pl.multiple_of(index * size, size), size * count)


def head_lanes(shape, head):
    return lax.broadcasted_iota(jnp.int32, shape, len(shape) - 1) // HEAD_DIM == head


def only_head(values, head):
    return jnp.where(head_lanes(values.shape, head), values, jnp.zeros_like(values))


def spread_heads(columns, rows, width):
    out = None
    for head in range(width // HEAD_DIM):
        one = jnp.broadcast_to(columns[:, head : head + 1], (rows, width))
        out = one if out is None else jnp.where(head_lanes((rows, width), head), one, out)
    return out


class Place:
    def __init__(self, n, m):
        self.n, self.m, self.half, self.planes = n, m, n // 2, m // 2
        self.s, self.k = lax.axis_index("seq"), lax.axis_index("shard")
        self.core, self.plane = lax.rem(self.k, 2), self.k // 2
        self.team, self.low = self.s // self.half, lax.rem(self.s, self.half)
        self.rank = self.low + self.half * self.core
        self.index = self.s * m + self.k
        self.odd = lax.rem(self.low, 2)

    def member(self, rank):
        return (self.team * self.half + lax.rem(rank, self.half), 2 * self.plane + rank // self.half)

    def across(self):
        return (lax.rem(self.s + self.half, self.n), self.k)

    def swap(self):
        return (lax.rem(self.s + self.half, self.n), 2 * self.plane + 1 - self.core)

    def partner(self):
        return (self.s, 2 * self.plane + 1 - self.core)

    def along(self, step):
        return lax.rem(self.s + step, self.n)

    def neighbour(self):
        return (self.team * self.half + self.low + 1 - 2 * lax.rem(self.low, 2), self.k)

    def beside(self, step):
        return lax.rem(self.plane + step, self.planes)

    def near_plane(self):
        return self.plane + 1 - 2 * lax.rem(self.plane, 2)

    def far_plane(self, step):
        return 2 * lax.rem(self.plane // 2 + step, self.planes // 2) + lax.rem(self.plane, 2)

    def greet(self):
        barrier = pltpu.get_barrier_semaphore()
        count = 0

        def signal(device):
            pl.semaphore_signal(barrier, inc=1, device_id=device, device_id_type=MESH)

        for step in range(1, self.n):
            signal((self.along(step), self.k))
            count += 1
        for step in range(self.n):
            signal((self.along(step), 2 * self.plane + 1 - self.core))
            count += 1
        for step in range(1, self.planes):
            signal((self.s, 2 * self.beside(step) + self.core))
            count += 1
        pl.semaphore_wait(barrier, count)


def send(src, dst, sems, at, device):
    pltpu.make_async_remote_copy(
        src_ref=src,
        dst_ref=dst,
        send_sem=sems[0].at[at],
        recv_sem=sems[1].at[at],
        device_id=device,
        device_id_type=MESH,
    ).start()


def settle(view, sem):
    pltpu.make_async_copy(view, view, sem).wait()


def attend_row(i, q_ref, k_ref, v_ref, o_ref, lse_ref, qm, m_s, l_s, acc, size):
    width = q_ref.shape[1]
    heads = width // HEAD_DIM
    rows = block_rows(i, size)
    q = q_ref[rows, :] * jnp.asarray(scale, bf16)
    for h in range(heads):
        qm[h] = only_head(q, h)

    def step(j, diagonal):
        at = block_rows(j, size)
        k = k_ref[at, :]
        v = v_ref[at, :]
        old = m_s[...]
        tops, sums, total = [], [], None
        for h in range(heads):
            s = row_dot(k, qm[h])
            if diagonal:
                k_pos = lax.broadcasted_iota(jnp.int32, (size, size), 0)
                q_pos = lax.broadcasted_iota(jnp.int32, (size, size), 1)
                s = jnp.where(k_pos <= q_pos, s, -1e30)
            top = jnp.max(s, axis=0, keepdims=True)
            if not diagonal:
                top = jnp.maximum(old[h : h + 1], top)
            p = jnp.exp(s - top)
            tops.append(top)
            sums.append(jnp.sum(p, axis=0, keepdims=True))
            part = col_dot(p.astype(bf16), only_head(v, h))
            total = part if total is None else total + part
        rest = [jnp.zeros((8 - heads, size), f32)] if heads < 8 else []
        top = jnp.concatenate(tops + rest, 0)
        add = jnp.concatenate(sums + rest, 0)
        if diagonal:
            l_s[...] = add
            acc[...] = total
        else:
            fade = jnp.exp(old - top)
            l_s[...] = l_s[...] * fade + add
            acc[...] = acc[...] * spread_heads(jnp.transpose(fade), size, width) + total
        m_s[...] = top

    step(i, True)

    def body(j, carry):
        step(j, False)
        return carry

    lax.fori_loop(0, i, body, 0)
    l = l_s[...]
    lse_ref[:, rows] = m_s[...] + jnp.log(l)
    o_ref[rows, :] = (acc[...] * spread_heads(jnp.transpose(1.0 / l), size, width)).astype(bf16)


def forward_call(n, m, tok, cot, wq_s, sm_s, wo_s, wi_s, wb_s):
    size, d = tok.shape
    nd = n * m
    length = n * size
    width = d // n
    half = n // 2
    rq = wq_s.shape[0]
    ff_half = wi_s.shape[1] // 2
    cells = (n, n, half)
    nc = len(cells)

    def kernel(
        tok_r, cot_r, wqs_r, sms_r, wos_r, wis_r, wbs_r,
        wo_r, wi_r, wb_r, q_r, k_r, v_r, o_r, lse_r, att_r, h1_r, wq_r, tb_r, cb_r, sv_r,
        q_v, k_v, v_v, h1_v, wq_v, tokf, sma, qm, m_s, l_s, acc, vec,
        t_send, t_recv, w_send, w_recv, a_send, a_recv, z_send, z_recv,
        lo_send, lo_recv, hi_send, hi_recv, b_send, b_recv, c_send, c_recv, loc,
    ):
        at = Place(n, m)
        planes, rank, core = at.planes, at.rank, at.core
        fulls, shards = (wo_r, wi_r, wb_r), (wos_r, wis_r, wbs_r)
        ts, ws, zs, cs = (t_send, t_recv), (w_send, w_recv), (z_send, z_recv), (c_send, c_recv)
        los, his, bs = (lo_send, lo_recv), (hi_send, hi_recv), (b_send, b_recv)
        rows_p = planes // 2
        near = 2 * at.near_plane() + core
        far = [2 * at.far_plane(step) + core for step in range(1, rows_p)]
        at.greet()
        away = core != at.team

        own = [(at.s, at.plane, core), (at.s, at.plane, core), (at.low, at.plane, core)]
        near_p = at.near_plane()
        far_p = [at.far_plane(step) for step in range(1, rows_p)]

        def half_of(odd):
            return wis_r.at[:, pl.ds(pl.multiple_of(odd * ff_half, ff_half), ff_half)]

        def start_z(c):
            dst = fulls[c].at[own[c]]
            if c < 2:
                for step in range(1, n):
                    s = at.along(step)
                    src = shards[c] if c == 0 else half_of(lax.rem(lax.rem(s, half), 2))
                    send(src, dst, zs, c, (s, at.k))
                src = shards[c] if c == 0 else half_of(at.odd)
                pltpu.make_async_copy(src, dst, loc.at[4 + c]).start()
                return
            for team in range(2):
                for pair in range(half // 2):
                    s = team * half + 2 * pair + at.team

                    @pl.when(s != at.s)
                    def _(s=s):
                        send(shards[c], dst, zs, c, (s, at.k))

            @pl.when(at.odd == at.team)
            def _():
                pltpu.make_async_copy(shards[c], dst, loc.at[4 + c]).start()

        def settle_z(c, sem):
            if c < 2:
                settle(fulls[c].at[pl.ds(0, n - 1), 0, 0], sem.at[c])
                return

            @pl.when(at.odd == at.team)
            def _():
                settle(fulls[c].at[pl.ds(0, half - 1), 0, 0], sem.at[c])

            @pl.when(at.odd != at.team)
            def _():
                settle(fulls[c].at[pl.ds(0, half), 0, 0], sem.at[c])

        def z_to_a(c):
            if c < 2:
                settle(fulls[c].at[own[c]], loc.at[4 + c])
            else:

                @pl.when(at.odd == at.team)
                def _():
                    settle(fulls[c].at[own[c]], loc.at[4 + c])

            settle_z(c, z_recv)
            part = fulls[c].at[:, at.plane, core]
            send(part, part, los, c, (at.s, near))
            for there in far:
                send(part, part, his, c, (at.s, there))

        def settle_far(c, sem):
            if far:
                settle(fulls[c].at[:, pl.ds(0, len(far)), 0], sem.at[c])

        def a_to_b(c):
            first = cells[c] // 2
            settle(fulls[c].at[:, 0, 0], lo_recv.at[c])
            part = fulls[c].at[pl.ds(0, first), near_p, core]
            for there in far:
                send(part, part, bs, c, (at.s, there))
            settle_far(c, hi_recv)
            for p in far_p:
                part = fulls[c].at[pl.ds(first, cells[c] - first), p, core]
                send(part, part, bs, c, (at.s, near))

        def b_to_c(c):
            settle_far(c, b_recv)
            part = fulls[c].at[:, :, core]
            send(part, part, cs, c, at.partner())

        def of_rank(r, part):
            return wqs_r.at[:, pl.ds(pl.multiple_of(part * d + r * width, width), width)]

        def to_part(part):
            return wq_v.at[block_rows(at.index, rq), pl.ds(part * width, width)]

        for part in range(3):
            pltpu.make_async_copy(of_rank(rank, part), to_part(part), loc.at[0]).start()
        own_s = pltpu.make_async_copy(sms_r, sma.at[at.index], loc.at[1])
        own_s.start()
        for step in range(1, n):
            other = lax.rem(rank + step, n)
            for part in range(3):
                send(of_rank(other, part), to_part(part), ws, 0, at.member(other))
            send(sms_r, sma.at[at.index], ws, 1, at.member(other))
        settle(wq_v.at[pl.ds(0, rq)], loc.at[0])
        own_s.wait()
        settle(wq_v.at[pl.ds(0, (n - 1) * rq)], w_recv.at[0])
        settle(sma.at[pl.ds(0, n - 1)], w_recv.at[1])
        for low in range(half):
            row = (at.team * half + low) * m + 2 * at.plane
            send(wq_v.at[block_rows(row, rq, 2)], wq_v.at[block_rows(row, rq, 2)], ws, 2, at.across())
            send(sma.at[pl.ds(row, 2)], sma.at[pl.ds(row, 2)], ws, 3, at.across())
        start_z(0)
        start_z(1)

        @pl.when(jnp.logical_not(away))
        def _():
            pltpu.make_async_copy(tok_r, tokf.at[rank], loc.at[2]).start()

        settle(wq_v.at[pl.ds(0, half * 2 * rq)], w_recv.at[2])
        settle(sma.at[pl.ds(0, half * 2)], w_recv.at[3])
        def cut(block, h):
            return block.at[pl.ds(h * (size // 2), size // 2)]

        @pl.when(away)
        def _():
            for h in range(2):
                send(cut(tok_r, h), cut(tokf.at[at.low + half * (1 - core)], h), ts, h, at.swap())

        for step in range(1, planes):
            there = (at.s, 2 * at.beside(step) + core)
            for other in range(n):
                row = other * m + 2 * at.plane
                send(wq_v.at[block_rows(row, rq, 2)], wq_v.at[block_rows(row, rq, 2)], ws, 4, there)
                send(sma.at[pl.ds(row, 2)], sma.at[pl.ds(row, 2)], ws, 5, there)
        z_to_a(0)

        @pl.when(jnp.logical_not(away))
        def _():
            settle(tokf.at[0], loc.at[2])

        def own_half(h):
            @pl.when(away)
            def _():
                settle(cut(tokf.at[0], h), t_recv.at[h])

            part = cut(tokf.at[rank], h)
            for step in range(1, half):
                low = lax.rem(at.low + step, half)
                send(part, part, ts, 2 + h, (at.team * half + low, at.k))
            send(part, part, ts, 4, at.partner())

        own_half(0)

        settle(wq_v.at[pl.ds(0, (planes - 1) * n * 2 * rq)], w_recv.at[4])
        settle(sma.at[pl.ds(0, (planes - 1) * n * 2)], w_recv.at[5])
        per = LANES // (d // nd)
        for group in range(d // LANES):
            total = sma[group * per].astype(f32)
            for other in range(1, per):
                total = total + sma[group * per + other].astype(f32)
            sv_r[:, group * LANES : (group + 1) * LANES] = total
            vec[0, group : group + 1, :] = total[2:3]
            vec[1, group : group + 1, :] = total[3:4]

        def norm_block(b):
            def body(t, carry):
                part = pl.ds(pl.multiple_of(t * 128, 128), 128)
                x = tokf[b, part, :].astype(f32)
                normed, _ = normalize(x)
                h1_v[pl.ds(pl.multiple_of(b * size + t * 128, 128), 128), :] = (
                    normed * sv_r[0:1, :] + sv_r[1:2, :]
                ).astype(bf16)
                return carry

            lax.fori_loop(0, size // 128, body, 0)

        groups = width // LANES
        bias_q = jnp.concatenate([vec[0, pl.ds(rank * groups + g, 1), :] for g in range(groups)], 1)
        bias_v = jnp.concatenate([vec[1, pl.ds(rank * groups + g, 1), :] for g in range(groups)], 1)

        def project_block(b):
            def body(t, carry):
                part = pl.ds(pl.multiple_of(b * size + t * 256, 256), 256)
                h = h1_v[part, :]
                q_v[part, :] = (dot(h, wq_v[:, 0:width]) + bias_q).astype(bf16)
                k_v[part, :] = dot(h, wq_v[:, width : 2 * width]).astype(bf16)
                v_v[part, :] = (dot(h, wq_v[:, 2 * width : 3 * width]) + bias_v).astype(bf16)
                return carry

            lax.fori_loop(0, size // 256, body, 0)

        def later_z():
            start_z(2)

            @pl.when(away)
            def _():
                send(cot_r, cb_r, ts, 6, at.swap())

            @pl.when(jnp.logical_not(away))
            def _():
                pltpu.make_async_copy(cot_r, cb_r, loc.at[3]).start()

        own_half(1)

        def take(t, carry):
            @pl.when(t == 1)
            def _():
                z_to_a(1)
                settle(tokf.at[0], t_recv.at[4])
                a_to_b(0)

            if half > 1:

                @pl.when(t == 2)
                def _():
                    a_to_b(1)
                    for h in range(2):
                        settle(tokf.at[pl.ds(0, half - 1), pl.ds(0, size // 2)], t_recv.at[2 + h])
                        for step in range(1, half):
                            part = cut(tokf.at[lax.rem(at.low + step, half) + half * core], h)
                            send(part, part, ts, 5, at.partner())

                @pl.when(t == 1 + half)
                def _():
                    settle(tokf.at[pl.ds(0, half - 1)], t_recv.at[5])
                    later_z()

            step = jnp.where(t < 2, 0, lax.rem(t - 2, max(half - 1, 1)) + 1)
            other_core = jnp.where(t < 2, t, (t - 2) // max(half - 1, 1))
            side = core + other_core - 2 * core * other_core
            b = lax.rem(at.low + step, half) + half * side
            norm_block(b)
            project_block(b)
            return carry

        lax.fori_loop(0, n, take, 0)
        beside = rank + 1 - 2 * lax.rem(rank, 2)
        leaving = [
            (tokf.at[rank], tb_r.at[0]), (tokf.at[beside], tb_r.at[1]),
            (q_v, q_r), (k_v, k_r), (v_v, v_r), (h1_v, h1_r), (wq_v, wq_r),
        ]
        for i, (src, dst) in enumerate(leaving):
            pltpu.make_async_copy(src, dst, loc.at[4 + nc + i]).start()

        pumps = PUMPS

        def row(i, carry):
            attend_row(i, q_v, k_v, v_v, o_r, lse_r, qm, m_s, l_s, acc, size)
            src = o_r.at[block_rows(i, size)]
            for which, owner in ((0, i), (1, i + 1 - 2 * lax.rem(i, 2))):
                dst = att_r.at[which, :, block_rows(rank, width)]

                @pl.when(owner != rank)
                def _(dst=dst, which=which, owner=owner):
                    send(src, dst, (a_send, a_recv), which, at.member(owner))

                @pl.when(owner == rank)
                def _(dst=dst, which=which):
                    pltpu.make_async_copy(src, dst, loc.at[which]).start()

            for when, todo in enumerate(pumps):

                @pl.when(i == n - len(pumps) + when)
                def _(todo=todo):
                    for what, c in todo:
                        {"z": z_to_a, "a": a_to_b, "b": b_to_c}[what](c)

            return carry

        lax.fori_loop(0, n, row, 0)
        for what, c in TAIL:
            {"z": z_to_a, "a": a_to_b, "b": b_to_c}[what](c)
        others = att_r.at[0, :, pl.ds(0, (n - 1) * width)]
        for which in range(2):
            settle(att_r.at[0, :, pl.ds(0, width)], loc.at[which])
            settle(others, a_recv.at[which])
        for i, (src, dst) in enumerate(leaving):
            settle(src, loc.at[4 + nc + i])
        for c in range(nc):
            settle(fulls[c].at[:, :, 0], c_recv.at[c])

        for which in range(2):
            settle(others, a_send.at[which])
        for c in range(nc):
            settle_z(c, z_send)
            settle(fulls[c].at[:, 0, 0], lo_send.at[c])
            settle_far(c, hi_send)
            settle_far(c, b_send)
            settle(fulls[c].at[:, :, 0], c_send.at[c])
        for at_sem, count in ((0, n - 1), (2, half * 2), (4, (planes - 1) * n * 2)):
            settle(wq_v.at[pl.ds(0, count * rq)], w_send.at[at_sem])
            settle(sma.at[pl.ds(0, count)], w_send.at[at_sem + 1])

        @pl.when(away)
        def _():
            for h in range(2):
                settle(cut(tokf.at[0], h), t_send.at[h])
            settle(cb_r, t_recv.at[6])
            settle(cb_r, t_send.at[6])

        @pl.when(jnp.logical_not(away))
        def _():
            settle(cb_r, loc.at[3])

        settle(tokf.at[0], t_send.at[4])
        if half > 1:
            for h in range(2):
                settle(tokf.at[pl.ds(0, half - 1), pl.ds(0, size // 2)], t_send.at[2 + h])
            settle(tokf.at[pl.ds(0, half - 1)], t_send.at[5])

    def sds(shape, dtype=bf16):
        return jax.ShapeDtypeStruct(shape, dtype)

    sems = pltpu.SemaphoreType.DMA
    return pl.pallas_call(
        kernel,
        name="gather_attend",
        out_shape=(
            sds((n, m // 2, 2, *wo_s.shape)),
            sds((n, m // 2, 2, wi_s.shape[0], ff_half)),
            sds((half, m // 2, 2, *wb_s.shape)),
            sds((length, width)), sds((length, width)), sds((length, width)), sds((length, width)),
            sds((8, length), f32),
            sds((2, size, d)),
            sds((length, d)),
            sds((d, 3 * width)),
            sds((2, size, d)), sds((size, d)),
            sds((16, d), f32),
        ),
        in_specs=[HB] * 7,
        out_specs=(HB,) * 6 + (VM,) * 3 + (HB,) * 3 + (VM,) * 2,
        scratch_shapes=[
            pltpu.VMEM((length, width), bf16),
            pltpu.VMEM((length, width), bf16),
            pltpu.VMEM((length, width), bf16),
            pltpu.VMEM((length, d), bf16),
            pltpu.VMEM((d, 3 * width), bf16),
            pltpu.VMEM((n, size, d), bf16),
            pltpu.VMEM((nd, 16, LANES), bf16),
            pltpu.VMEM((width // HEAD_DIM, size, width), bf16),
            pltpu.VMEM((8, size), f32),
            pltpu.VMEM((8, size), f32),
            pltpu.VMEM((size, width), f32),
            pltpu.VMEM((2, max(8, d // LANES), LANES), f32),
            sems((7,)), sems((7,)),
            sems((6,)), sems((6,)),
            sems((2,)), sems((2,)),
            sems((nc,)), sems((nc,)),
            sems((nc,)), sems((nc,)),
            sems((nc,)), sems((nc,)),
            sems((nc,)), sems((nc,)),
            sems((nc,)), sems((nc,)),
            sems((11 + nc,)),
        ],
        compiler_params=pltpu.CompilerParams(
            collective_id=0, has_side_effects=True, vmem_limit_bytes=62 << 20
        ),
        cost_estimate=pl.CostEstimate(
            flops=6 * length * d * width + 2 * length * length * d // n, bytes_accessed=80 << 20, transcendentals=0
        ),
    )(tok, cot, wq_s, sm_s, wo_s, wi_s, wb_s)


def small_pack(index, vectors):
    per = vectors[0].shape[0]
    rows = [part for v in vectors for part in v.reshape(-1, per)]
    rows = jnp.stack(rows + [jnp.zeros_like(rows[0])] * (16 - len(rows)))
    lane = lax.broadcasted_iota(jnp.int32, (16, LANES), 1)
    spread = jnp.tile(rows, (1, LANES // per))
    return jnp.where(lane // per == lax.rem(index, LANES // per), spread, jnp.zeros_like(spread))


def backward_call(n, m, res, dat, dres, q, k, v, o, lse, h1, wq, tb, sv, gsm, gwo, gwi, gwb):
    size, d = dat.shape
    nd = n * m
    length = n * size
    width = d // n
    heads = width // HEAD_DIM
    half, planes = n // 2, m // 2
    rq = d // nd
    quarter = gwi.shape[4] // 2
    parts = [
        (half, *gwb.shape[3:]), (n, gwi.shape[3], quarter), (n, gwi.shape[3], quarter), (n, *gwo.shape[3:]),
    ]
    cells = [p[0] for p in parts]
    nc = len(cells)
    lanes_s = d // n

    def kernel(*refs):
        (res_r, dat_r, dres_r, q_h, k_h, v_h, o_r, lse_r, h1_r, wq_h, tb_r, sv_r, gsm_r, gwo_r, gwi_r, gwb_r) = refs[:16]
        (reso_r, gt_r, rg, gqo_r, go_r, gi_r, gb_r, small_r) = refs[16:24]
        (do, delta, dqa, dka, dva, dqkv, gacc, rqp, rqh, pf, sd, rd, rzd, sm, smz, smp, smc) = refs[24:41]
        gqb, hb, sg, tb_v, o_v, q_r, k_r, v_r, wq_r, gq_r = refs[41:51]
        rest = refs[51:]
        ga, rc, rp, rz = (rest[i * nc : (i + 1) * nc] for i in range(4))
        (d_s, d_r, x_s, x_r, y_s, y_r, e_s, e_r, c_s, c_r, p_s, p_r, z_s, z_r, m_s, m_r, yl_s, yl_r, el_s, el_r, loc) = rest[4 * nc :]
        at = Place(n, m)
        rank, core, low = at.rank, at.core, at.low
        left, right = (gwi_r.at[:, :, :, :, pl.ds(p * quarter, quarter)] for p in range(2))
        grads = (gwb_r, left, right, gwo_r)
        at.greet()
        away = core != at.team

        for step in range(1, n):
            other = lax.rem(rank + step, n)
            send(dat_r.at[:, block_rows(other, width)], do.at[block_rows(rank, size)], (d_s, d_r), 0, at.member(other))
        own_do = pltpu.make_async_copy(dat_r.at[:, block_rows(rank, width)], do.at[block_rows(rank, size)], loc.at[0])
        own_do.start()

        for c in range(nc):
            send(grads[c].at[:, :, 1 - core], rc[c], (c_s, c_r), c, at.partner())
            pltpu.make_async_copy(grads[c].at[:, :, core], ga[c], loc.at[6 + c]).start()
        fetch_tb = pltpu.make_async_copy(tb_r.at[0], tb_v, loc.at[4])
        fetch_tb.start()
        for i in range(n):
            pltpu.make_async_copy(o_r.at[pl.ds(i * size, size)], o_v.at[:, pl.ds(i * width, width)], loc.at[5]).start()

        arriving = [(q_h, q_r), (k_h, k_r), (v_h, v_r), (wq_h, wq_r)]
        for i, (src, dst) in enumerate(arriving):
            pltpu.make_async_copy(src, dst, loc.at[6 + nc + i]).start()

        own_dres = pltpu.make_async_copy(dres_r, gt_r, loc.at[2])
        own_dres.start()

        def fetch_h1(b):
            return pltpu.make_async_copy(h1_r.at[block_rows(b, size)], hb.at[block_rows(lax.rem(b, 2), size)], loc.at[3])

        def c_to_p(c):
            settle(ga[c], loc.at[6 + c])
            settle(rc[c], c_r.at[c])

            def add(t, carry):
                s, p = t // planes, lax.rem(t, planes)
                ga[c][s, p] = (ga[c][s, p].astype(f32) + rc[c][s, p].astype(f32)).astype(bf16)
                return carry

            lax.fori_loop(0, cells[c] * planes, add, 0)
            for step in range(1, planes):
                other = at.beside(step)
                send(ga[c].at[:, other], rp[c].at[step - 1], (p_s, p_r), c, (at.s, 2 * other + core))

        def p_to_z(c):
            settle(rp[c], p_r.at[c])

            def add(s, carry):
                total = ga[c][s, at.plane].astype(f32)
                for step in range(1, planes):
                    total = total + rp[c][step - 1, s].astype(f32)
                ga[c][s, at.plane] = total.astype(bf16)
                return carry

            lax.fori_loop(0, cells[c], add, 0)
            if c > 0:
                for step in range(1, n):
                    s = at.along(step)
                    send(ga[c].at[s, at.plane], rz[c].at[at.s], (z_s, z_r), c, (s, at.k))
                rz[c][at.s] = ga[c][at.s, at.plane]
                return
            source = at.team * (half // 2) + at.low // 2
            for place in range(half):
                s = at.odd * half + place

                @pl.when(s != at.s)
                def _(s=s, place=place):
                    send(ga[c].at[place, at.plane], rz[c].at[source], (z_s, z_r), c, (s, at.k))

                @pl.when(s == at.s)
                def _(place=place):
                    rz[c][source] = ga[c][place, at.plane]

        def settle_z(c, sem):
            if c > 0:
                settle(rz[c].at[pl.ds(0, n - 1)], sem.at[c])
                return

            @pl.when(at.odd == at.team)
            def _():
                settle(rz[c].at[pl.ds(0, half - 1)], sem.at[c])

            @pl.when(at.odd != at.team)
            def _():
                settle(rz[c].at[pl.ds(0, half)], sem.at[c])

        def z_to_out(c):
            settle_z(c, z_r)

            def total(sources):
                out = rz[c][sources[0]].astype(f32)
                for s in sources[1:]:
                    out = out + rz[c][s].astype(f32)
                return out

            if c == 0:
                gb_r[...] = total(range(half))
            elif c < 3:
                for odd in range(2):
                    first = (2 * odd + c - 1) * quarter
                    gi_r[:, first : first + quarter] = total([s for s in range(n) if s % half % 2 == odd])
            else:
                go_r[...] = total(range(n))

        for c in range(nc):
            c_to_p(c)
        fetch_h1(0).start()

        own_do.wait()
        settle(do.at[pl.ds(0, (n - 1) * size)], d_r.at[0])
        for i, (src, dst) in enumerate(arriving):
            settle(dst, loc.at[6 + nc + i])

        @pl.when(away)
        def _():
            send(res_r, reso_r, (x_s, x_r), 0, at.swap())

        @pl.when(jnp.logical_not(away))
        def _():
            pltpu.make_async_copy(res_r, reso_r, loc.at[1]).start()

        settle(o_v.at[:, pl.ds(0, n * width)], loc.at[5])
        pick = (
            lax.broadcasted_iota(jnp.int32, (8, width), 1) // HEAD_DIM
            == lax.broadcasted_iota(jnp.int32, (8, width), 0)
        ).astype(f32)

        def prepare(i, carry):
            rows = block_rows(i, size)
            product = do[rows, :].astype(f32) * o_v[:, block_rows(i, width)].astype(f32)
            delta[:, rows] = lax.dot_general(
                pick, product, NT, preferred_element_type=f32, precision=lax.Precision.HIGHEST
            )
            dqa[rows, :] = jnp.zeros((size, width), f32)
            return carry

        lax.fori_loop(0, n, prepare, 0)
        gacc[...] = jnp.zeros_like(gacc)
        sm[...] = jnp.zeros_like(sm)
        sm[4:12, :] = gsm_r[...]

        def pair(i, j, diagonal):
            rows, at_k = block_rows(i, size), block_rows(j, size)
            kk, vv = k_r[at_k, :], v_r[at_k, :]
            qs, dd = q_r[rows, :] * jnp.asarray(scale, bf16), do[rows, :]
            dq = dk = dv = None
            for h in range(heads):
                qh, dh_, kh = only_head(qs, h), only_head(dd, h), only_head(kk, h)
                p = jnp.exp(row_dot(kk, qh) - lse_r[h : h + 1, rows])
                if diagonal:
                    k_pos = lax.broadcasted_iota(jnp.int32, (size, size), 0)
                    q_pos = lax.broadcasted_iota(jnp.int32, (size, size), 1)
                    p = jnp.where(k_pos <= q_pos, p, 0.0)
                dp = row_dot(vv, dh_)
                ds = (p * (dp - delta[h : h + 1, rows])).astype(bf16)
                one, two, three = dot(p.astype(bf16), dh_), dot(ds, qh), col_dot(ds, kh)
                dv = one if dv is None else dv + one
                dk = two if dk is None else dk + two
                dq = three if dq is None else dq + three
            dva[...] += dv
            dka[...] += dk
            dqa[rows, :] += dq

        def owner(j):
            return j // half, lax.rem(j, half)

        def finish_block(j):
            core_j, low_j = owner(j)

            @pl.when(core_j == core)
            def _():
                settle(rd.at[0], y_r.at[low_j])

                def add(t, carry):
                    rows = pl.ds(pl.multiple_of(t * 128, 128), 128)
                    rd[low_j, rows, :] = (pf[rows, :] + rd[low_j, rows, :].astype(f32)).astype(bf16)
                    return carry

                lax.fori_loop(0, size // 128, add, 0)

                @pl.when(low_j != low)
                def _():
                    slot = lax.rem(low_j - low + half, half) - 1
                    send(rd.at[low_j], rzd.at[slot], (e_s, e_r), 0, (at.team * half + low_j, at.k))

        def column(j, carry):
            fetch_h1(j).wait()

            @pl.when(j + 1 < n)
            def _():
                fetch_h1(j + 1).start()

            dka[...] = jnp.zeros_like(dka)
            dva[...] = jnp.zeros_like(dva)
            pair(j, j, True)

            def inner(i, c2):
                pair(i, j, False)
                return c2

            lax.fori_loop(j + 1, n, inner, 0)
            dqb = (dqa[block_rows(j, size), :] * scale).astype(bf16)
            dkb, dvb = dka[...].astype(bf16), dva[...].astype(bf16)
            dqkv[:, 0:width] = dqb
            dqkv[:, width : 2 * width] = dkb
            dqkv[:, 2 * width : 3 * width] = dvb
            mine = block_rows(rank, width)
            sm[2:3, mine] += jnp.sum(dqb.astype(f32), axis=0, keepdims=True)
            sm[3:4, mine] += jnp.sum(dvb.astype(f32), axis=0, keepdims=True)

            @pl.when(j > 0)
            def _():
                finish_block(j - 1)

            core_j, low_j = owner(j)

            def project(t, c2):
                rows = pl.ds(pl.multiple_of(t * PIECE, PIECE), PIECE)
                part = row_dot(dqkv[rows, :], wq_r[...])

                @pl.when(core_j == core)
                def _():
                    pf[rows, :] = part

                @pl.when(core_j != core)
                def _():
                    sd[low_j, rows, :] = part.astype(bf16)

                    @pl.when(j == n - 1)
                    def _():
                        send(sd.at[low_j, rows], rd.at[low_j, rows], (yl_s, yl_r), t, at.partner())

                return c2

            lax.fori_loop(0, size // PIECE, project, 0)

            @pl.when(jnp.logical_and(core_j != core, j < n - 1))
            def _():
                send(sd.at[low_j], rd.at[low_j], (y_s, y_r), low_j, at.partner())

            slot = lax.rem(j, 2)
            for t in range(3):
                cols = slice(t * width, (t + 1) * width)
                gacc[:, cols] += col_dot(hb[block_rows(slot, size), :], dqkv[:, cols])
            for c in range(nc - 1):

                @pl.when(j == min(c, n - 2))
                def _(c=c):
                    p_to_z(c)

            return carry

        lax.fori_loop(0, n, column, 0)
        gqb[...] = gacc[...].astype(bf16)
        for step in range(1, planes):
            other = at.beside(step)
            for s in range(n):
                send(
                    gqb.at[block_rows(s * m + 2 * other, rq, 2)],
                    rqp.at[block_rows((step - 1) * n + s, 2 * rq)],
                    (m_s, m_r), 0, (at.s, 2 * other + core),
                )
        pieces = size // PIECE
        last = half - 1
        owner_last = (at.team * half + last, at.k)

        def pair_piece(rows):
            rd[last, rows, :] = (pf[rows, :] + rd[last, rows, :].astype(f32)).astype(bf16)

        @pl.when(jnp.logical_and(core == 1, low != last))
        def _():
            def pass_on(t, carry):
                rows = pl.ds(pl.multiple_of(t * PIECE, PIECE), PIECE)
                settle(rd.at[last, rows], yl_r.at[t])
                pair_piece(rows)
                send(rd.at[last, rows], rzd.at[last - low - 1, rows], (el_s, el_r), t, owner_last)
                return carry

            lax.fori_loop(0, pieces, pass_on, 0)

        own_dres.wait()
        fetch_tb.wait()
        if half > 1:

            @pl.when(rank != n - 1)
            def _():
                settle(rzd, e_r.at[0])

        def norm_step(t, carry):
            sum_g, sum_s = carry
            rows = pl.ds(pl.multiple_of(t * PIECE, PIECE), PIECE)

            @pl.when(rank == n - 1)
            def _():
                settle(rd.at[last, rows], yl_r.at[t])
                pair_piece(rows)
                if half > 1:
                    settle(rzd.at[:, rows], el_r.at[t])

            dh1 = rd[low, rows, :].astype(f32)
            for slot in range(half - 1):
                dh1 = dh1 + rzd[slot, rows, :].astype(f32)
            normed, inv = normalize(tb_v[rows, :].astype(f32))
            grad = gt_r[rows, :] + norm_back(dh1 * sv_r[0:1, :], normed, inv)
            gt_r[rows, :] = grad
            sg[rows, :] = grad.astype(bf16)

            @pl.when(away)
            def _():
                send(sg.at[rows], rg.at[rows], (x_s, x_r), 1, at.swap())

            return (
                sum_g + jnp.sum(dh1 * normed, axis=0, keepdims=True),
                sum_s + jnp.sum(dh1, axis=0, keepdims=True),
            )

        zero = jnp.zeros((1, d), f32)
        sum_g, sum_s = lax.fori_loop(0, pieces, norm_step, (zero, zero))
        sm[0:1, :] = sum_g
        sm[1:2, :] = sum_s

        settle(rqp, m_r.at[0])

        def add_q(s, carry):
            rows = block_rows(s * m + 2 * at.plane, rq, 2)
            total = gqb[rows, :].astype(f32)
            for step in range(1, planes):
                total = total + rqp[block_rows((step - 1) * n + s, 2 * rq), :].astype(f32)
            gqb[rows, :] = total.astype(bf16)
            return carry

        lax.fori_loop(0, n, add_q, 0)
        for l in range(half):
            row = ((1 - at.team) * half + l) * m + 2 * at.plane
            send(gqb.at[block_rows(row, rq, 2)], rqh.at[block_rows(l, 2 * rq)], (m_s, m_r), 2, at.across())

        p_to_z(nc - 1)
        send(sm, smc, (m_s, m_r), 1, at.partner())
        settle(rqh, m_r.at[2])
        for l in range(half):
            rows = block_rows((at.team * half + l) * m + 2 * at.plane, rq, 2)
            gqb[rows, :] = (
                gqb[rows, :].astype(f32) + rqh[block_rows(l, 2 * rq), :].astype(f32)
            ).astype(bf16)

        def member_rows(r):
            return block_rows((at.team * half + lax.rem(r, half)) * m + 2 * at.plane + r // half, rq)

        for step in range(1, n):
            other = lax.rem(rank + step, n)
            send(gqb.at[member_rows(other)], gq_r.at[rank], (m_s, m_r), 4, at.member(other))
        pltpu.make_async_copy(gqb.at[member_rows(rank)], gq_r.at[rank], loc.at[0]).start()

        settle(smc, m_r.at[1])
        settle(smc, m_s.at[1])
        sm[...] = sm[...] + smc[...]
        for step in range(1, planes):
            send(sm, smp.at[step - 1], (m_s, m_r), 3, (at.s, 2 * at.beside(step) + core))
        for c in range(nc):
            z_to_out(c)
        settle(smp, m_r.at[3])
        settle(smp, m_s.at[3])
        total = sm[...]
        for step in range(1, planes):
            total = total + smp[step - 1]
        sm[...] = total
        for step in range(1, n):
            s = at.along(step)
            send(sm.at[:, block_rows(s, lanes_s)], smz.at[step - 1], (m_s, m_r), 5, (s, at.k))
        settle(smz, m_r.at[5])
        total = sm[:, block_rows(at.s, lanes_s)]
        for step in range(1, n):
            total = total + smz[step - 1]
        small_r[...] = total

        settle(gq_r.at[pl.ds(0, n - 1)], m_r.at[4])
        settle(gq_r.at[0], loc.at[0])
        for r in range(n):
            for part in range(3):
                first = part * d + r * width
                gqo_r[:, first : first + width] = gq_r[r, :, part * width : (part + 1) * width].astype(f32)

        @pl.when(away)
        def _():
            settle(rg, x_r.at[1])
            settle(rg, x_s.at[1])
            settle(reso_r, x_r.at[0])
            settle(reso_r, x_s.at[0])

        @pl.when(jnp.logical_not(away))
        def _():
            settle(reso_r, loc.at[1])

        settle(do.at[pl.ds(0, (n - 1) * size)], d_s.at[0])
        for c in range(nc):
            settle(rc[c], c_s.at[c])
            settle(rp[c], p_s.at[c])
            settle_z(c, z_s)
        for l in range(half - 1):
            settle(rd.at[0], y_s.at[l])

        @pl.when(core == 1)
        def _():
            settle(rd.at[0], y_s.at[last])

        @pl.when(core == 0)
        def _():
            for t in range(pieces):
                settle(rd.at[0, pl.ds(0, PIECE)], yl_s.at[t])

        passes = jnp.logical_and(core == 1, low != last)

        @pl.when(passes)
        def _():
            for t in range(pieces):
                settle(rd.at[0, pl.ds(0, PIECE)], el_s.at[t])

        if half > 2:

            @pl.when(passes)
            def _():
                settle(rzd.at[pl.ds(0, half - 2)], e_s.at[0])

        if half > 1:

            @pl.when(jnp.logical_not(passes))
            def _():
                settle(rzd, e_s.at[0])

        settle(rqp, m_s.at[0])
        settle(smz, m_s.at[5])
        settle(rqh, m_s.at[2])
        settle(gq_r.at[pl.ds(0, n - 1)], m_s.at[4])

    def sds(shape, dtype=bf16):
        return jax.ShapeDtypeStruct(shape, dtype)

    sems = pltpu.SemaphoreType.DMA
    return pl.pallas_call(
        kernel,
        name="attend_back_reduce",
        out_shape=(
            sds((size, d)),
            sds((size, d), f32),
            sds((size, d)),
            sds((rq, 3 * d), f32),
            sds(gwo.shape[3:], f32),
            sds((gwi.shape[3], 2 * gwi.shape[4]), f32),
            sds(gwb.shape[3:], f32),
            sds((16, lanes_s), f32),
        ),
        in_specs=[HB] * 7 + [VM, HB, HB, HB] + [VM] * 2 + [HB] * 3,
        out_specs=(HB, VM, HB) + (VM,) * 5,
        scratch_shapes=[
            pltpu.VMEM((length, width), bf16),
            pltpu.VMEM((8, length), f32),
            pltpu.VMEM((length, width), f32),
            pltpu.VMEM((size, width), f32),
            pltpu.VMEM((size, width), f32),
            pltpu.VMEM((size, 3 * width), bf16),
            pltpu.VMEM((d, 3 * width), f32),
            pltpu.VMEM(((planes - 1) * n * 2 * rq, 3 * width), bf16),
            pltpu.VMEM((half * 2 * rq, 3 * width), bf16),
            pltpu.VMEM((size, d), f32),
            pltpu.VMEM((half, size, d), bf16),
            pltpu.VMEM((half, size, d), bf16),
            pltpu.VMEM((max(half - 1, 1), size, d), bf16),
            pltpu.VMEM((16, d), f32),
            pltpu.VMEM((n - 1, 16, lanes_s), f32),
            pltpu.VMEM((planes - 1, 16, d), f32),
            pltpu.VMEM((16, d), f32),
        ]
        + [
            pltpu.VMEM((d, 3 * width), bf16),
            pltpu.VMEM((2 * size, d), bf16),
            pltpu.VMEM((size, d), bf16),
            pltpu.VMEM((size, d), bf16),
            pltpu.VMEM((size, d), bf16),
            pltpu.VMEM((length, width), bf16),
            pltpu.VMEM((length, width), bf16),
            pltpu.VMEM((length, width), bf16),
            pltpu.VMEM((d, 3 * width), bf16),
            pltpu.VMEM((n, rq, 3 * width), bf16),
        ]
        + [pltpu.VMEM((count, planes, rows, cols), bf16) for count, rows, cols in parts] * 2
        + [pltpu.VMEM((planes - 1, *part), bf16) for part in parts]
        + [pltpu.VMEM(part, bf16) for part in parts]
        + [
            sems((1,)), sems((1,)),
            sems((2,)), sems((2,)),
            sems((half,)), sems((half,)),
            sems((1,)), sems((1,)),
            sems((nc,)), sems((nc,)),
            sems((nc,)), sems((nc,)),
            sems((nc,)), sems((nc,)),
            sems((6,)), sems((6,)),
            sems((size // PIECE,)), sems((size // PIECE,)),
            sems((size // PIECE,)), sems((size // PIECE,)),
            sems((10 + nc,)),
        ],
        compiler_params=pltpu.CompilerParams(
            collective_id=1, has_side_effects=True, vmem_limit_bytes=67043328
        ),
        cost_estimate=pl.CostEstimate(
            flops=12 * length * d * width + 5 * length * length * d // n, bytes_accessed=80 << 20, transcendentals=0
        ),
    )(res, dat, dres, q, k, v, o, lse, h1, wq, tb, sv, gsm, gwo, gwi, gwb)


def solution(mesh):
    n, m = mesh.shape["seq"], mesh.shape["shard"]
    nd = n * m
    every = ("seq", "shard")

    def per_device(
        tokens, ln1_gain, ln1_bias, w_qkv, bias_query, bias_value, w_out, bias_out,
        ln2_gain, ln2_bias, w_in, bias_in, w_back, bias_back, cotangent,
    ):
        d = tokens.shape[2]
        width = d // n
        index = lax.axis_index("seq") * m + lax.axis_index("shard")
        pack = small_pack(
            index,
            [ln1_gain, ln1_bias, bias_query, bias_value, bias_out, ln2_gain, ln2_bias, bias_back, bias_in],
        )
        rq = w_qkv.shape[0]
        ff = w_in.shape[1]
        rq = w_qkv.shape[0]
        (full_out, full_in, full_back, q, k, v, o, lse, att_two, h1, wq, tb, cot_own, sv) = forward_call(
            n, m, tokens[0], cotangent[0], w_qkv, pack, w_out, w_in, w_back
        )
        full_out = full_out.reshape(d, d)
        half_in = full_in.reshape(d, ff // 2)
        half_back = full_back.reshape(ff // 2, d)
        odd = lax.rem(lax.rem(lax.axis_index("seq"), n // 2), 2)
        per = d // nd
        parts = bias_in.shape[0] // per
        half_bin = lax.dynamic_slice_in_dim(sv[8 : 8 + parts], odd * (d // 2), d // 2, 1)
        half_bin = half_bin.reshape(parts, nd // 2, per).transpose(1, 0, 2).reshape(-1)
        g_two, s_two = sv[5], sv[6]

        def to_neighbour(values):
            pairs = []
            for s in range(n):
                there = s // 2 * 2 + 1 - s % 2
                pairs += [(s * m + k, there * m + k) for k in range(m)]
            return lax.ppermute(values.astype(bf16), every, pairs).astype(f32)

        size = tokens.shape[1]
        cot_two = jnp.concatenate([cot_own, to_neighbour(cot_own).astype(bf16)])
        x_f = tb.reshape(2 * size, d).astype(f32)
        att_two = att_two.reshape(2 * size, d)
        resid = x_f + dot(att_two, full_out) + sv[4]
        normed2, scale2 = normalize(resid)
        h_two = (normed2 * g_two + s_two).astype(bf16)
        pre = dot(h_two, half_in) + half_bin
        act = gelu_pair(pre)[0].astype(bf16)
        out_part = dot(act, half_back)
        leaves = out_part[size:].astype(bf16)
        others_out = to_neighbour(leaves)
        pre, leaves = lax.optimization_barrier((pre, leaves))
        d_pre = (row_dot(cot_two, half_back) * gelu_pair(pre)[1]).astype(bf16)
        g_b_in = jnp.sum(d_pre.astype(f32), axis=0)
        d_h2_part = row_dot(d_pre, half_in)
        leaves = d_h2_part[size:].astype(bf16)
        others_d = to_neighbour(leaves)
        pre, d_pre, leaves = lax.optimization_barrier((pre, d_pre, leaves))
        g_w_back = col_dot(gelu_pair(pre)[0].astype(bf16), cot_two).astype(bf16)
        g_w_in = col_dot(h_two, d_pre).astype(bf16)

        resid, normed2, scale2 = resid[:size], normed2[:size], scale2[:size]
        att_tok, cot_f = att_two[:size], cot_two[:size].astype(f32)
        result = (resid + out_part[:size] + others_out + sv[7]).astype(bf16)
        g_b_back = jnp.sum(cot_f, axis=0)
        d_h2 = d_h2_part[:size] + others_d
        g_g2 = jnp.sum(d_h2 * normed2, axis=0)
        g_s2 = jnp.sum(d_h2, axis=0)
        d_resid = cot_f + norm_back(d_h2 * g_two, normed2, scale2)
        d_resid_b = d_resid.astype(bf16)
        g_w_out = col_dot(att_tok, d_resid_b).astype(bf16)
        g_b_out = jnp.sum(d_resid, axis=0)
        d_att_tok = row_dot(d_resid_b, full_out).astype(bf16)
        bin_rows = g_b_in.reshape(nd // 2, parts, per).transpose(1, 0, 2).reshape(parts, d // 2)
        bin_rows = jnp.where(
            lax.broadcasted_iota(jnp.int32, (parts, d), 1) // (d // 2) == odd, jnp.tile(bin_rows, (1, 2)), 0.0
        )
        gsm = jnp.concatenate([jnp.stack([g_b_out, g_g2, g_s2, g_b_back]), bin_rows])

        (own_result, g_tok, swapped, g_qkv, go, gi, gb, small) = backward_call(
            n, m, result, d_att_tok, d_resid, q, k, v, o, lse, h1, wq, tb, sv, gsm,
            g_w_out.reshape(n, m // 2, 2, d // nd, d),
            g_w_in.reshape(n, m // 2, 2, d // nd, ff // 2),
            g_w_back.reshape(n // 2, m // 2, 2, ff // nd, d),
        )
        away = lax.rem(lax.axis_index("shard"), 2) != lax.axis_index("seq") // (n // 2)
        g_tok = jnp.where(away, swapped.astype(f32), g_tok)
        mine = lax.dynamic_slice_in_dim(small, lax.axis_index("shard") * per, per, 1)
        return (
            own_result[None], g_tok[None], mine[0], mine[1], g_qkv, mine[2], mine[3], go, mine[4],
            mine[5], mine[6], gi, mine[8 : 8 + parts].reshape(-1), gb, mine[7],
        )

    whole, vector, matrix = P("shard", "seq", None), P(every), P(every, None)
    return jax.shard_map(
        per_device,
        mesh=mesh,
        in_specs=(
            whole, vector, vector, matrix, vector, vector, matrix, vector, vector, vector, matrix, vector,
            matrix, vector, whole,
        ),
        out_specs=(
            whole, whole, vector, vector, matrix, vector, vector, matrix, vector, vector, vector, matrix,
            vector, matrix, vector,
        ),
        check_vma=False,
    )
```
